512 devices in a mesh: section: 4 (over x), shard: 128 (over y, z, core).
Axes of the slice: x: 4, y: 8, z: 8, core: 2. Of those that a mesh axis runs over, the one named last changes fastest.
Arguments:
- user_dense: bfloat16 [128, 1024], P('shard'), may hold values from -6 to 6
- tables: bfloat16 [4, 262144, 128], P('section', 'shard'), may hold values from -3 to 3
- feat_owner: int32 [4, 128, 1024, 1], P('section', 'shard'), may hold values from 0 to 127; in each aligned block of 1024 rows (0 to 1023, 1024 to 2047, ..., all dimensions but the last counted through in order) at most 16 rows name the same one
- feat_row: int32 [4, 128, 1024], P('section', 'shard'), may hold values from 0 to 2047
- keep_first: int32 [128, 256], P('shard'), may hold values from 0 to 1023, all different within a row
- keep_second: int32 [128, 32], P('shard'), may hold values from 0 to 255, all different within a row
- section_weight: bfloat16 [4, 1024, 1024], P('section'), may hold values from -0.1875 to 0.1875
- section_head: float32 [4, 1024], P('section'), may hold values from -5 to 5
- user_proj: bfloat16 [1024, 128], replicated, may hold values from -0.1875 to 0.1875
- item_in: bfloat16 [128, 512], replicated, may hold values from -0.5 to 0.5
- item_out: bfloat16 [512, 128], replicated, may hold values from -0.25 to 0.25
- prerank_feat: bfloat16 [512, 1024], replicated, may hold values from -0.25 to 0.25
- prerank_item: bfloat16 [128, 1024], replicated, may hold values from -0.5 to 0.5
Outputs:
- section_scores: float32 [4, 128, 32], P('section', 'shard')
The draws below stay inside these ranges and needn't reach their ends.
Inputs may be any that keep to these rules, and one draw needn't show every extreme that they name: `feat_owner`: among the 1024 requests of one user in one section, no shard index occurs more than 16 times, and 16 times in some of them. `keep_first`: the 256 entries of a row are distinct. `keep_second`: the 32 entries of a row are distinct.
All inputs are finite; a program needn't handle non-finite values.
Results may differ from the reference program's by a relative error of at most 0.007.
Values may be sent and summed in bfloat16 or wider, within the bound.
No kernel may reach another device: no remote copies, remote signals or barrier semaphores. Data moves between devices by JAX's collectives and lax.ppermute only.
A program may use at most 64 MiB of HBM per device.

```python
import math
import jax
import jax.numpy as jnp
import numpy as np
from jax import lax

CANDS = 1024
F1 = 4
F2 = 32
EMB = 128
HID = 1024
TOWER = 512
ROWS_DEV = 2048
KEEP1 = 256
KEEP2 = 32
U = 128
ROWS = 262144
CAP = 16
N_SHARD = 128


def touch_ends(values, stream_key, least, high):
    index_at = [jax.random.randint(jax.random.fold_in(stream_key, axis), (), 0, length) for axis, length in enumerate(values.shape)]
    main_axis = values.shape.index(max(values.shape))
    neighbour = index_at[:main_axis] + [(index_at[main_axis] + 1) % values.shape[main_axis]] + index_at[main_axis + 1:]
    return values.at[tuple(index_at)].set(least).at[tuple(neighbour)].set(high)


def shard_levels(own_key, shape, split, low, high):
    def one(axis_at, blocks):
        heights = jax.random.uniform(jax.random.fold_in(jax.random.fold_in(own_key, 6), axis_at), (blocks,), jnp.float32, low / len(split), high / len(split))
        return jnp.repeat(jnp.exp(heights), shape[axis_at] // blocks).reshape((-1,) + (1,) * (len(shape) - axis_at - 1))

    gain = one(*split[0])
    for cut in split[1:]:
        gain = gain * one(*cut)
    return gain


def cumulative_ranks(number_of, lean):
    loads = [(1 << 20) // math.isqrt(standing ** lean) + 1 for standing in range(1, number_of + 1)]
    spread = 1 + sum(loads) // (1 << 30)
    return np.cumsum(np.array([max(1, weight // spread) for weight in loads]))


def skewed_ids(own_key, extent, number_of, skew):
    table = cumulative_ranks(number_of, skew)
    ticket = jax.random.randint(jax.random.fold_in(own_key, 1), extent, 0, int(table[number_of - 1]))
    rank = jnp.searchsorted(jnp.asarray(table, jnp.int32), ticket, side="right")
    return jax.random.permutation(jax.random.fold_in(own_key, 2), number_of)[rank].astype(jnp.int32)


def different_ones(own_key, rows, number_of, top, lift):
    sequence = jax.random.permutation(jax.random.fold_in(own_key, 1), number_of)
    boost = sequence
    for power in range(3):
        boost = boost * boost // number_of
    boost = boost * lift // number_of
    lots = jax.random.randint(jax.random.fold_in(own_key, 2), (rows, number_of), 0, 4096) + boost
    sure = jax.random.permutation(jax.random.fold_in(own_key, 3), rows)[jnp.arange(number_of) % rows]
    lots = jnp.where(jnp.arange(rows)[:, None] == sure[None, :], 1 << 14, lots)
    priority = lots * number_of + jnp.arange(number_of)
    return lax.top_k(priority.astype(jnp.int32), top)[1].astype(jnp.int32)


def deal_out(stream_key, own, number, rows, number_of, top, limit, skew):
    order = jax.random.permutation(stream_key, number_of)
    heavy_load, ordinary = load_shares(number_of, rows * top, limit, skew, True), load_shares(number_of, rows * top, limit, skew, False)
    places = jnp.arange(number_of)

    def named(tallies, offset_by):
        used = int((tallies > 0).sum())
        fixed = max(1, used // 4)
        moved = fixed + (places - fixed + offset_by * (used - fixed)) % max(1, number_of - fixed)
        return jnp.zeros((number_of,), jnp.int32).at[order[jnp.where(places < fixed, places, moved)]].set(jnp.asarray(tallies, jnp.int32))

    tallies = jnp.where(number % 4 == 0, named(heavy_load, number // 4), named(ordinary, number - number // 4 - 1))
    mixed = jax.random.permutation(jax.random.fold_in(own, 3), number_of)
    donor, sink = mixed[0:number_of // 2 * 2:2], mixed[1:number_of // 2 * 2:2]
    slack = jnp.minimum(tallies[donor] - 1, limit - tallies[sink]) // 2
    slack = jnp.where((donor == order[0]) | (sink == order[0]) | (tallies[sink] == 0), 0, jnp.maximum(slack, 0))
    moved = jax.random.randint(jax.random.fold_in(own, 4), (number_of // 2,), 0, 1 << 20) % (slack + 1)
    tallies = tallies.at[donor].add(-moved).at[sink].add(moved)
    items = jnp.searchsorted(jnp.cumsum(tallies), jnp.arange(rows * top), side="right").astype(jnp.int32)
    listing = items.reshape(top, rows).T
    listing = listing[jax.random.permutation(jax.random.fold_in(own, 1), rows)]
    offset_by = jax.random.randint(jax.random.fold_in(own, 2), (rows, 1), 0, top)
    return jnp.take_along_axis(listing, (jnp.arange(top)[None, :] + offset_by) % top, axis=1)


def load_shares(amount, total, most, slope, full):
    weights = [(1 << 20) // math.isqrt(grade ** slope) + 1 for grade in range(1, amount + 1)]
    largest = most if full else min(most, max(-(-total // amount), total * weights[0] // sum(weights)))
    least = 1 if total - largest >= amount - 1 else 0
    counts, rest = [largest] + [least] * (amount - 1), total - largest - least * (amount - 1)
    while rest > 0:
        free = [i for i in range(1, amount) if counts[i] < largest] or [i for i in range(1, amount) if counts[i] < most]
        whole, left = sum([weights[i] for i in free]), rest
        for i in free:
            more = min(most - counts[i], max(1, left * weights[i] // whole), rest)
            counts[i] = counts[i] + more
            rest = rest - more
    return np.array(counts)


def normal_values(own_key, extent, spread, bound, split=(), kind=jnp.bfloat16):
    array = jax.random.normal(own_key, extent, jnp.float32) * spread
    if len(split) > 0:
        array = shard_levels(own_key, extent, split, -0.22, 0.18) * array
    return jnp.clip(array, min=-bound, max=bound).astype(kind)


def setup_inputs(seed: int = 0) -> dict:
    splits = jax.random.split(jax.random.key(seed), 14)
    user_dense = normal_values(splits[0], (U, HID), 1.0, 6.0, ((0, 128),))
    tables = normal_values(splits[1], (4, ROWS, EMB), 0.5, 3.0, ((0, 4), (1, 128)))
    feat_owner_keys = jax.random.split(jax.random.fold_in(splits[2], 1), 4 * U * CANDS // CANDS)
    feat_owner_turns = jax.random.permutation(jax.random.fold_in(splits[2], 3), 4 * U * CANDS // CANDS)
    feat_owner = jax.vmap(lambda own, number: deal_out(jax.random.fold_in(splits[2], 2), own, number, CANDS, N_SHARD, 1, CAP, 2))(feat_owner_keys, feat_owner_turns).reshape((4, U, CANDS, 1))
    feat_row = touch_ends(skewed_ids(splits[3], (4, U, CANDS), ROWS_DEV, 2), jax.random.fold_in(splits[3], 3), 0, ROWS_DEV - 1).astype(jnp.int32)
    keep_first = different_ones(splits[4], U, CANDS, KEEP1, 0)
    keep_second = different_ones(splits[5], U, KEEP1, KEEP2, 0)
    section_weight = normal_values(splits[6], (4, HID, HID), HID ** -0.5, 0.1875, ((0, 4),))
    section_head = normal_values(splits[7], (4, HID), 1.0, 5.0, ((0, 4),), jnp.float32)
    user_proj = normal_values(splits[8], (HID, EMB), HID ** -0.5, 0.1875)
    item_in = normal_values(splits[9], (EMB, TOWER), EMB ** -0.5, 0.5)
    item_out = normal_values(splits[10], (TOWER, EMB), TOWER ** -0.5, 0.25)
    prerank_feat = normal_values(splits[11], (F1 * EMB, HID), (F1 * EMB) ** -0.5, 0.25)
    prerank_item = normal_values(splits[12], (EMB, HID), EMB ** -0.5, 0.5)
    return dict(user_dense=user_dense, tables=tables, feat_owner=feat_owner, feat_row=feat_row, keep_first=keep_first, keep_second=keep_second, section_weight=section_weight, section_head=section_head, user_proj=user_proj, item_in=item_in, item_out=item_out, prerank_feat=prerank_feat, prerank_item=prerank_item)


highest = lax.Precision.HIGHEST

def carry_round(values):
    return lax.optimization_barrier(values.astype(jnp.bfloat16)).astype(jnp.float32)

def section_zero(embedded, user_part, first_keep, second_keep, main_weight, head_vec, user_proj, item_in, item_out):
    users_here = user_part.shape[0]
    active = jax.nn.relu(jnp.dot(user_part, main_weight, preferred_element_type=jnp.float32))
    user_query = (active * head_vec).astype(jnp.bfloat16)
    user_vec = jnp.dot(user_query, user_proj, preferred_element_type=jnp.float32)
    hidden = jax.nn.relu(jnp.dot(embedded.reshape(-1, EMB), item_in, preferred_element_type=jnp.float32)).astype(jnp.bfloat16)
    tower_out = jnp.dot(hidden, item_out, preferred_element_type=jnp.float32).astype(jnp.bfloat16).reshape(users_here, CANDS, EMB)
    logits = jnp.einsum('bcd,bd->bc', tower_out.astype(jnp.float32), user_vec, precision=highest)
    kept_rows = jnp.take_along_axis(tower_out, first_keep[:, :, None], axis=1)
    kept_logits = jnp.take_along_axis(logits, first_keep, axis=1)
    scored = jnp.take_along_axis(kept_logits, second_keep, axis=1)
    return (kept_rows, carry_round(kept_logits), scored)

def section_one(embedded, tower_rows, prior, second_keep, main_weight, head_vec, prerank_feat, prerank_item):
    users_here = tower_rows.shape[0]
    features = embedded.reshape(users_here * KEEP1, F1 * EMB)
    pre_act = jnp.dot(features, prerank_feat, preferred_element_type=jnp.float32)
    pre_act = pre_act + jnp.dot(tower_rows.reshape(-1, EMB), prerank_item, preferred_element_type=jnp.float32)
    inner_act = jax.nn.relu(pre_act).astype(jnp.bfloat16)
    hidden = jax.nn.relu(jnp.dot(inner_act, main_weight, preferred_element_type=jnp.float32))
    logits = lax.optimization_barrier(jnp.sum(hidden * head_vec, axis=1)).reshape(users_here, KEEP1) / math.sqrt(HID) + prior
    carried = hidden.astype(jnp.bfloat16).reshape(users_here, KEEP1, HID)
    kept_rows = jnp.take_along_axis(carried, second_keep[:, :, None], axis=1)
    kept_logits = jnp.take_along_axis(logits, second_keep, axis=1)
    return (kept_rows, carry_round(kept_logits), kept_logits)

def section_rank(embedded, carried, prior, main_weight, head_vec):
    users_here = carried.shape[0]
    features = embedded.reshape(users_here, KEEP2, F2, EMB).astype(jnp.float32)
    gram_flat = jnp.einsum('bkfd,bkgd->bkfg', features, features, precision=highest) / math.sqrt(EMB)
    gram_flat = gram_flat.astype(jnp.bfloat16).reshape(users_here * KEEP2, F2 * F2)
    hidden = jax.nn.relu(jnp.dot(gram_flat, main_weight, preferred_element_type=jnp.float32) + carried.reshape(-1, HID).astype(jnp.float32))
    logits = lax.optimization_barrier(jnp.sum(hidden * head_vec, axis=1)).reshape(users_here, KEEP2) / math.sqrt(HID) + prior
    return (hidden.astype(jnp.bfloat16).reshape(users_here, KEEP2, HID), carry_round(logits), logits)

def reference(user_dense, tables, feat_owner, feat_row, keep_first, keep_second, section_weight, section_head, user_proj, item_in, item_out, prerank_feat, prerank_item):
    block_users = 8
    total_users = user_dense.shape[0]
    block_count = total_users // block_users
    row_index = (feat_owner[..., 0] * ROWS_DEV + feat_row).astype(jnp.int32)

    def per_block(pieces):
        user_part, row_ids, first_keep, second_keep = pieces
        embedded = [tables[level][row_ids[level]] for level in range(4)]
        tower_rows, prior_one, score_zero = section_zero(embedded[0], user_part, first_keep, second_keep, section_weight[0], section_head[0], user_proj, item_in, item_out)
        carry_one, prior_two, score_one = section_one(embedded[1], tower_rows, prior_one, second_keep, section_weight[1], section_head[1], prerank_feat, prerank_item)
        carry_two, prior_three, score_two = section_rank(embedded[2], carry_one, prior_two, section_weight[2], section_head[2])
        carry_three, unused_prior, score_three = section_rank(embedded[3], carry_two, prior_three, section_weight[3], section_head[3])
        return jnp.stack([score_zero, score_one, score_two, score_three])
    pieces = (user_dense.reshape(block_count, block_users, HID), jnp.moveaxis(row_index.reshape(4, block_count, block_users, CANDS), 1, 0), keep_first.reshape(block_count, block_users, KEEP1), keep_second.reshape(block_count, block_users, KEEP2))
    scored = lax.map(per_block, pieces)
    return jnp.moveaxis(scored, 1, 0).reshape(4, total_users, KEEP2)
```

```python
import math

import jax
import jax.numpy as jnp
from jax import lax
from jax.experimental import pallas as pl
from jax.experimental.pallas import tpu as pltpu
from jax.sharding import PartitionSpec as P

F32 = jnp.float32
BF16 = jnp.bfloat16
NT = (((1,), (1,)), ((), ()))


def call(kernel, out_shape, *operands, smem=0):
    specs = [pl.BlockSpec(memory_space=pltpu.SMEM)] * smem
    specs += [pl.BlockSpec(memory_space=pltpu.VMEM)] * (len(operands) - smem)
    return pl.pallas_call(kernel, out_shape=out_shape, in_specs=specs)(*operands)


def iota(shape, axis):
    return lax.broadcasted_iota(jnp.int32, shape, axis)


def ones_where(mask):
    return jnp.where(mask, 1.0, 0.0).astype(BF16)


def dot(a, b):
    return jnp.dot(a, b, preferred_element_type=F32)


def dot_nt(a, b):
    return lax.dot_general(a, b, NT, preferred_element_type=F32)


def column(row):
    return jnp.broadcast_to(row, (128, 128)).T


def request_kernel(owner_ref, row_ref, req_ref, slot_ref):
    shards, slots = req_ref.shape
    cands = owner_ref.shape[1]
    owner = owner_ref[...]
    hits = owner == iota((shards, cands), 0)
    hot = ones_where(hits)
    earlier = ones_where((iota((128, 256), 0) < iota((128, 256), 1)) | (iota((128, 256), 1) >= 128))
    seen = jnp.zeros((shards, 128), F32)
    ranks = []
    for b in range(cands // 128):
        part = slice(b * 128, b * 128 + 128)
        counts = dot(hot[:, part], earlier)
        ranks.append(jnp.sum(jnp.where(hits[:, part], counts[:, :128] + seen, 0.0), axis=0, keepdims=True))
        seen = seen + counts[:, 128:]
    rank = jnp.concatenate(ranks, axis=1).astype(jnp.int32)
    slot_ref[...] = owner * slots + rank
    row = row_ref[...]
    at_slot = rank == iota((slots, cands), 0)
    high = jnp.where(at_slot, (row >> 4).astype(F32), 0.0).astype(BF16)
    low = jnp.where(at_slot, (row & 15).astype(F32), 0.0).astype(BF16)
    req_ref[...] = (dot_nt(hot, high) * 16.0 + dot_nt(hot, low)).astype(jnp.int32)


def serve_kernel(ids_ref, table_ref, out_ref):
    blocks = ids_ref.shape[0]
    rows = table_ref.shape[0]
    step = 4
    ids = ids_ref[...].astype(F32)
    lanes = iota((128, 128), 1).astype(F32)
    table = table_ref[...]
    for first in range(0, blocks, step):
        tall = []
        for b in range(first, first + step):
            col = column(ids[b:b + 1, :])
            tall.append(jnp.concatenate(
                [ones_where(col - 128.0 * r == lanes) for r in range(rows // 128)], axis=1))
        hot = jnp.concatenate(tall, axis=0)
        out_ref[first * 128:(first + step) * 128, :] = dot(hot, table).astype(BF16)


def prepare_kernel(sec_ref, slot_ref, first_ref, second_ref, dense_ref, weight_ref, head_ref, proj_ref,
                   pick_ref, vec_ref):
    sec = sec_ref[0]
    slot = slot_ref[...].astype(F32)
    cands = slot.shape[1]
    spots = pick_ref.shape[1]
    final = second_ref.shape[1]

    def second_column():
        wide = jnp.concatenate([second_ref[...].astype(F32), jnp.zeros((1, 128 - final), F32)], axis=1)
        return column(wide)[:final, :1]

    def lookup(at, row):
        lanes = iota((at.shape[0], row.shape[1]), 1).astype(F32)
        return jnp.sum(jnp.where(lanes == at, row, 0.0), axis=1, keepdims=True)

    @pl.when(sec == 0)
    def _():
        at = lookup(second_column(), first_ref[...].astype(F32))
        where = lookup(at, slot)
        pick_ref[:final, :] = ones_where(iota((final, spots), 1).astype(F32) == where)
        active = jax.nn.relu(dot(dense_ref[...], weight_ref[...]))
        query = (active * head_ref[...]).astype(BF16)
        vec_ref[...] = dot(query, proj_ref[...])

    @pl.when(sec == 1)
    def _():
        at = second_column() * 4.0
        where = jnp.concatenate([lookup(at + float(f), slot) for f in range(4)], axis=0)
        pick_ref[:4 * final, :] = ones_where(iota((4 * final, spots), 1).astype(F32) == where)

    @pl.when(sec >= 2)
    def _():
        lanes = iota((128, 128), 1).astype(F32)
        for b in range(cands // 128):
            col = column(slot[:, b * 128:b * 128 + 128])
            for s in range(spots // 128):
                pick_ref[b * 128:b * 128 + 128, s * 128:s * 128 + 128] = ones_where(col - 128.0 * s == lanes)


def as_row(col, lanes):
    n = col.shape[0]
    return jnp.sum(jnp.where(iota((n, lanes), 0) == iota((n, lanes), 1), col, 0.0), axis=0, keepdims=True)


def tower_kernel(sec_ref, pick_ref, rows_ref, vec_ref, in_ref, out_ref, packet_ref, score_ref):
    @pl.when(sec_ref[0] == 0)
    def _():
        n = packet_ref.shape[0] // 2
        embed = dot(pick_ref[:n, :], rows_ref[...]).astype(BF16)
        hidden = jax.nn.relu(dot(embed, in_ref[...])).astype(BF16)
        tower = dot(hidden, out_ref[...]).astype(BF16)
        logit = jnp.sum(tower.astype(F32) * vec_ref[...], axis=1, keepdims=True)
        packet_ref[:n, :] = tower
        packet_ref[n:, :] = jnp.broadcast_to(logit, (n, 128)).astype(BF16)
        score_ref[...] = as_row(logit, 128)


def features_kernel(sec_ref, pick_ref, rows_ref, feat_ref, weight_ref, part_ref):
    sec = sec_ref[0]
    n = part_ref.shape[0]
    width = rows_ref.shape[1]

    @pl.when(sec == 1)
    def _():
        embed = dot(pick_ref[:4 * n, :], rows_ref[...]).astype(BF16)
        wide = jnp.concatenate([embed[f * n:(f + 1) * n, :] for f in range(4)], axis=1)
        part_ref[...] = dot(wide, feat_ref[...])

    @pl.when(sec >= 2)
    def _():
        embed = dot(pick_ref[...], rows_ref[...]).astype(BF16)
        r, c = iota((128, 128), 0), iota((128, 128), 1)
        same_item = (r // 32) == (c // 32)
        spread = ones_where((r % 32) == (c % 32))
        own_lanes = (r % 4) == (c // 32)
        grams = []
        for b in range(embed.shape[0] // 128):
            block = embed[b * 128:b * 128 + 128, :]
            gram = dot_nt(block, block) * (1.0 / math.sqrt(width))
            gram = jnp.where(same_item, gram, 0.0).astype(BF16)
            grams.append(jnp.where(own_lanes, dot(gram, spread), 0.0).astype(BF16))
        tall = jnp.concatenate(grams, axis=0)
        i, k = iota((8 * n, 32 * n), 0), iota((8 * n, 32 * n), 1)
        choose = ones_where(((k // 32) == (i % n)) & (((k % 32) // 4) == (i // n)))
        flat = dot(choose, tall).astype(BF16)
        flat = jnp.concatenate([flat[q * n:(q + 1) * n, :] for q in range(8)], axis=1)
        part_ref[...] = dot(flat, weight_ref[...])


def prerank_kernel(sec_ref, packet_ref, part_ref, item_ref, weight_ref, head_ref, carry_ref, score_ref):
    @pl.when(sec_ref[0] == 1)
    def _():
        n, hid = part_ref.shape
        pre = part_ref[...] + dot(packet_ref[:n, :], item_ref[...])
        inner = jax.nn.relu(pre).astype(BF16)
        hidden = jax.nn.relu(dot(inner, weight_ref[...]))
        prior = packet_ref[n:, :].astype(F32)[:, :1]
        logit = jnp.sum(hidden * head_ref[...], axis=1, keepdims=True) / math.sqrt(hid) + prior
        carry_ref[:, :hid] = hidden.astype(BF16)
        carry_ref[:, hid:] = jnp.broadcast_to(logit, (n, 128)).astype(BF16)
        score_ref[...] = as_row(logit, 128)


def final_kernel(sec_ref, near_ref, far_ref, part_ref, before_ref, head_ref, head_before_ref,
                 score0_ref, score1_ref, score_ref):
    sec = sec_ref[0]
    n, hid = part_ref.shape
    scale = 1.0 / math.sqrt(hid)

    def rank(part, carry, prior, head):
        hidden = jax.nn.relu(part + carry)
        return hidden, jnp.sum(hidden * head, axis=1, keepdims=True) * scale + prior

    @pl.when(sec == 0)
    def _():
        score_ref[...] = score0_ref[...]

    @pl.when(sec == 1)
    def _():
        score_ref[...] = score1_ref[...]

    @pl.when(sec == 2)
    def _():
        near = near_ref[...].astype(F32)
        _, logit = rank(part_ref[...], near[:, :hid], near[:, hid:hid + 1], head_ref[...])
        score_ref[...] = as_row(logit, 128)

    @pl.when(sec == 3)
    def _():
        far = far_ref[...].astype(F32)
        hidden, logit = rank(before_ref[...], far[:, :hid], far[:, hid:hid + 1], head_before_ref[...])
        prior = logit.astype(BF16).astype(F32)
        _, logit = rank(part_ref[...], hidden.astype(BF16).astype(F32), prior, head_ref[...])
        score_ref[...] = as_row(logit, 128)


def per_device(
    user_dense,
    tables,
    feat_owner,
    feat_row,
    keep_first,
    keep_second,
    section_weight,
    section_head,
    user_proj,
    item_in,
    item_out,
    prerank_feat,
    prerank_item,
):
    shape = jax.ShapeDtypeStruct
    shards = lax.axis_size("shard")
    cands = feat_row.shape[2]
    slots = 2 * cands // shards
    spots = shards * slots
    width = tables.shape[2]
    hid = section_weight.shape[1]
    final = keep_second.shape[1]
    sec = lax.axis_index("section").reshape(1).astype(jnp.int32)
    weight = section_weight[0]

    head_before = lax.ppermute(section_head, "section", [(2, 3)])

    request, slot = call(
        request_kernel,
        (shape((shards, slots), jnp.int32), shape((1, cands), jnp.int32)),
        feat_owner.reshape(1, cands),
        feat_row.reshape(1, cands),
    )
    asked = lax.all_to_all(request, "shard", 0, 0, tiled=True)
    pick, user_vec = call(
        prepare_kernel,
        (shape((cands, spots), BF16), shape((1, width), F32)),
        sec, slot, keep_first, keep_second, user_dense, weight, section_head, user_proj,
        smem=1,
    )
    served = call(
        serve_kernel,
        shape((spots, width), BF16),
        asked.reshape(spots // 128, 128),
        tables[0],
    )
    rows = lax.all_to_all(served.reshape(shards, slots, width), "shard", 0, 0, tiled=True)
    rows = rows.reshape(spots, width)
    packet, score0 = call(
        tower_kernel,
        (shape((2 * final, width), BF16), shape((1, 128), F32)),
        sec, pick, rows, user_vec, item_in, item_out,
        smem=1,
    )
    packet = lax.ppermute(packet, "section", [(0, 1)])
    part = call(
        features_kernel,
        shape((final, hid), F32),
        sec, pick, rows, prerank_feat, weight,
        smem=1,
    )
    before = lax.ppermute(part, "section", [(2, 3)])
    carry, score1 = call(
        prerank_kernel,
        (shape((final, hid + 128), BF16), shape((1, 128), F32)),
        sec, packet, part, prerank_item, weight, section_head,
        smem=1,
    )
    near = lax.ppermute(carry, "section", [(1, 2)])
    far = lax.ppermute(carry, "section", [(1, 3)])
    scores = call(
        final_kernel,
        shape((1, 128), F32),
        sec, near, far, part, before, section_head, head_before, score0, score1,
        smem=1,
    )
    return scores[None, :, :final]


def solution(mesh):
    placed = (
        P("shard", None),
        P("section", "shard", None),
        P("section", "shard", None, None),
        P("section", "shard", None),
        P("shard", None),
        P("shard", None),
        P("section", None, None),
        P("section", None),
        P(),
        P(),
        P(),
        P(),
        P(),
    )
    return jax.shard_map(
        per_device,
        mesh=mesh,
        in_specs=placed,
        out_specs=P("section", "shard", None),
        check_vma=False,
    )
```

```python
import math

import jax
import jax.numpy as jnp
from jax import lax
from jax.experimental import pallas as pl
from jax.experimental.pallas import tpu as pltpu
from jax.sharding import PartitionSpec as P


F32 = jnp.float32
BF16 = jnp.bfloat16
NT = (((1,), (1,)), ((), ()))


def call(kernel, out_shape, *operands, smem=0, hbm=0, sems=0, flops=0, scratch=()):
    specs = [pl.BlockSpec(memory_space=pltpu.SMEM)] * smem
    specs += [pl.BlockSpec(memory_space=pltpu.HBM)] * hbm
    specs += [pl.BlockSpec(memory_space=pltpu.VMEM)] * (len(operands) - smem - hbm)
    return pl.pallas_call(
        kernel,
        out_shape=out_shape,
        in_specs=specs,
        scratch_shapes=[*scratch, *([pltpu.SemaphoreType.DMA((sems,))] if sems else [])],
        cost_estimate=pl.CostEstimate(flops=flops, transcendentals=0, bytes_accessed=0),
        compiler_params=pltpu.CompilerParams(vmem_limit_bytes=20 << 20),
    )(*operands)


def copies(sources, targets, sem):
    return [pltpu.make_async_copy(a, b, sem.at[i]) for i, (a, b) in enumerate(zip(sources, targets))]


def in_hbm(*arrays):
    return [pltpu.with_memory_space_constraint(a, pltpu.HBM) for a in arrays]


def iota(shape, axis):
    return lax.broadcasted_iota(jnp.int32, shape, axis)


def ones_where(mask):
    return jnp.where(mask, 1.0, 0.0).astype(BF16)


def dot(a, b):
    return jnp.dot(a, b, preferred_element_type=F32)


def dot_nt(a, b):
    return lax.dot_general(a, b, NT, preferred_element_type=F32)


def column(row):
    return jnp.broadcast_to(row, (128, 128)).T


def request_kernel(user_ref, owner_hbm, row_hbm, table_hbm, req_ref, slot_ref, table_ref, owner_ref, row_ref, sem):
    moves = copies((owner_hbm, row_hbm, table_hbm), (owner_ref, row_ref, table_ref), sem)
    for move in moves:
        move.start()
    shards = req_ref.shape[0]
    cands = owner_ref.shape[1]
    slots = 2 * cands // shards
    earlier = ones_where((iota((128, 256), 0) < iota((128, 256), 1)) | (iota((128, 256), 1) >= 128))
    seen = jnp.zeros((shards, 128), F32)
    ranks = []
    moves[0].wait()
    owner = owner_ref[...]
    hits = owner == iota((shards, cands), 0)
    hot = ones_where(hits)
    for b in range(cands // 128):
        part = slice(b * 128, b * 128 + 128)
        counts = dot(hot[:, part], earlier)
        ranks.append(jnp.sum(jnp.where(hits[:, part], counts[:, :128] + seen, 0.0), axis=0, keepdims=True))
        seen = seen + counts[:, 128:]
    rank = jnp.concatenate(ranks, axis=1).astype(jnp.int32)
    slot_ref[...] = owner * slots + rank
    moves[1].wait()
    row = row_ref[...]
    at_slot = rank + (user_ref[0] % (128 // slots)) * slots == iota((128, cands), 0)
    high = jnp.where(at_slot, (row >> 4).astype(F32), 0.0).astype(BF16)
    low = jnp.where(at_slot, (row & 15).astype(F32), 0.0).astype(BF16)
    req_ref[...] = (dot_nt(hot, high) * 16.0 + dot_nt(hot, low)).astype(jnp.int32)
    moves[2].wait()


def serve_kernel(ids_ref, table_ref, out_ref):
    users = ids_ref.shape[0]
    slots = 2048 // users
    group = 128 // slots
    rows = table_ref.shape[0]
    step = 4
    lanes = iota((128, 128), 1)
    table = table_ref[...]
    for first in range(0, users // group, step):
        tall = []
        for b in range(first, first + step):
            ids = jnp.sum(ids_ref[b * group:(b + 1) * group, :], axis=0, keepdims=True)
            col = column(ids)
            fine = ones_where((col & 127) == lanes)
            coarse = (col >> 7).astype(F32).astype(BF16)
            tall.append(jnp.concatenate(
                [jnp.where(coarse == float(r), fine, jnp.zeros_like(fine)) for r in range(rows // 128)], axis=1))
        hot = jnp.concatenate(tall, axis=0)
        out_ref[first * 128:(first + step) * 128, :] = dot(hot, table).astype(BF16)


def prepare_kernel(sec_ref, in_hbm, out_hbm, weight_hbm, head_hbm,
                   slot_ref, first_ref, second_ref, dense_ref, proj_ref,
                   spot_ref, vec_ref, in_ref, out_ref, weight_ref, head_ref, sem):
    moves = copies((in_hbm, out_hbm, weight_hbm, head_hbm),
                   (in_ref, out_ref, weight_ref, head_ref), sem)
    for move in moves:
        move.start()
    sec = sec_ref[0]
    slot = slot_ref[...].astype(F32)
    final = second_ref.shape[1]

    def second_column():
        wide = jnp.concatenate([second_ref[...].astype(F32), jnp.zeros((1, 128 - final), F32)], axis=1)
        return column(wide)[:final, :1]

    def lookup(at, row):
        lanes = iota((at.shape[0], row.shape[1]), 1).astype(F32)
        return jnp.sum(jnp.where(lanes == at, row, 0.0), axis=1, keepdims=True)

    @pl.when(sec == 0)
    def _():
        at = lookup(second_column(), first_ref[...].astype(F32))
        spot_ref[:final, :] = jnp.broadcast_to(lookup(at, slot), (final, 128))

    @pl.when(sec == 1)
    def _():
        at = second_column() * 4.0
        for f in range(4):
            spot_ref[f * final:f * final + final, :] = jnp.broadcast_to(lookup(at + float(f), slot), (final, 128))

    for move in moves:
        move.wait()

    @pl.when(sec == 0)
    def _():
        active = jax.nn.relu(dot(dense_ref[...], weight_ref[...]))
        query = (active * head_ref[...]).astype(BF16)
        vec_ref[...] = dot(query, proj_ref[...])


def picked(col, rows):
    col = col.astype(jnp.int32)
    fine = ones_where((col & 127) == iota(col.shape, 1))
    coarse = (col >> 7).astype(F32).astype(BF16)
    hot = [jnp.where(coarse == float(r), fine, jnp.zeros_like(fine)) for r in range(rows.shape[0] // 128)]
    return dot(jnp.concatenate(hot, axis=1), rows).astype(BF16)


def as_row(col, lanes):
    n = col.shape[0]
    return jnp.sum(jnp.where(iota((n, lanes), 0) == iota((n, lanes), 1), col, 0.0), axis=0, keepdims=True)


def tower_kernel(sec_ref, spot_ref, rows_ref, vec_ref, in_ref, out_ref, packet_ref, score_ref):
    @pl.when(sec_ref[0] == 0)
    def _():
        n = packet_ref.shape[0] // 2
        embed = picked(spot_ref[:n, :], rows_ref[...])
        hidden = jax.nn.relu(dot(embed, in_ref[...])).astype(BF16)
        tower = dot(hidden, out_ref[...]).astype(BF16)
        logit = jnp.sum(tower.astype(F32) * vec_ref[...], axis=1, keepdims=True)
        packet_ref[:n, :] = tower
        packet_ref[n:, :] = jnp.broadcast_to(logit, (n, 128)).astype(BF16)
        score_ref[...] = as_row(logit, n)


def features_kernel(sec_ref, feat_hbm, item_hbm, slot_ref, spot_ref, rows_ref, weight_ref, head_ref,
                    part_ref, item_ref, feat_ref, sem):
    sec = sec_ref[0]
    n = part_ref.shape[0] - 8
    cands = slot_ref.shape[1]
    width = rows_ref.shape[1]

    @pl.when(sec == 1)
    def _():
        moves = copies((feat_hbm, item_hbm), (feat_ref, item_ref), sem)
        for move in moves:
            move.start()
        embed = picked(spot_ref[:4 * n, :], rows_ref[...])
        for move in moves:
            move.wait()
        wide = jnp.concatenate([embed[f * n:(f + 1) * n, :] for f in range(4)], axis=1)
        part_ref[:n, :] = dot(wide, feat_ref[...])

    @pl.when(sec >= 2)
    def _():
        rows = rows_ref[...]
        embed = jnp.concatenate(
            [picked(jnp.concatenate([column(slot_ref[:, b:b + 128]) for b in range(h, h + 512, 128)], axis=0), rows)
             for h in range(0, cands, 512)], axis=0)
        r, c = iota((128, 128), 0), iota((128, 128), 1)
        same_item = (r // 32) == (c // 32)
        spread = ones_where((r % 32) == (c % 32))
        own_lanes = (r % 4) == (c // 32)
        grams = []
        for b in range(embed.shape[0] // 128):
            block = embed[b * 128:b * 128 + 128, :]
            gram = dot_nt(block, block) * (1.0 / math.sqrt(width))
            gram = jnp.where(same_item, gram, 0.0).astype(BF16)
            grams.append(jnp.where(own_lanes, dot(gram, spread), 0.0).astype(BF16))
        tall = jnp.concatenate(grams, axis=0)
        i, k = iota((8 * n, 32 * n), 0), iota((8 * n, 32 * n), 1)
        choose = ones_where(((k // 32) == (i % n)) & (((k % 32) // 4) == (i // n)))
        flat = dot(choose, tall).astype(BF16)
        flat = jnp.concatenate([flat[q * n:(q + 1) * n, :] for q in range(8)], axis=1)
        part_ref[:n, :] = dot(flat, weight_ref[...])
        part_ref[n:n + 1, :] = head_ref[...]


def prerank_kernel(sec_ref, packet_ref, part_ref, item_ref, weight_ref, head_ref, carry_ref, score_ref):
    @pl.when(sec_ref[0] == 1)
    def _():
        n, hid = part_ref.shape[0] - 8, part_ref.shape[1]
        pre = part_ref[:n, :] + dot(packet_ref[:n, :], item_ref[...])
        inner = jax.nn.relu(pre).astype(BF16)
        hidden = jax.nn.relu(dot(inner, weight_ref[...]))
        prior = packet_ref[n:, :].astype(F32)[:, :1]
        logit = jnp.sum(hidden * head_ref[...], axis=1, keepdims=True) / math.sqrt(hid) + prior
        carry_ref[:, :hid] = hidden.astype(BF16)
        carry_ref[:, hid:] = jnp.broadcast_to(logit, (n, 128)).astype(BF16)
        score_ref[...] = as_row(logit, n)


def final_kernel(sec_ref, near_ref, far_ref, part_ref, before_ref, score0_ref, score1_ref, score_ref):
    sec = sec_ref[0]
    n, hid = part_ref.shape[0] - 8, part_ref.shape[1]
    scale = 1.0 / math.sqrt(hid)

    def rank(from_ref, carry, prior):
        hidden = jax.nn.relu(from_ref[:n, :] + carry)
        return hidden, jnp.sum(hidden * from_ref[n:n + 1, :], axis=1, keepdims=True) * scale + prior

    @pl.when(sec == 0)
    def _():
        score_ref[...] = score0_ref[...]

    @pl.when(sec == 1)
    def _():
        score_ref[...] = score1_ref[...]

    @pl.when(sec == 2)
    def _():
        near = near_ref[...].astype(F32)
        _, logit = rank(part_ref, near[:, :hid], near[:, hid:hid + 1])
        score_ref[...] = as_row(logit, n)

    @pl.when(sec == 3)
    def _():
        far = far_ref[...].astype(F32)
        hidden, logit = rank(before_ref, far[:, :hid], far[:, hid:hid + 1])
        prior = logit.astype(BF16).astype(F32)
        _, logit = rank(part_ref, hidden.astype(BF16).astype(F32), prior)
        score_ref[...] = as_row(logit, n)


def cascade(
    user_dense,
    tables,
    feat_owner,
    feat_row,
    keep_first,
    keep_second,
    section_weight,
    section_head,
    user_proj,
    item_in,
    item_out,
    prerank_feat,
    prerank_item,
):
    shape = pltpu.VMEM
    shards = lax.axis_size("shard")
    cands = feat_row.shape[2]
    slots = 2 * cands // shards
    spots = shards * slots
    width = tables.shape[2]
    hid = section_weight.shape[1]
    final = keep_second.shape[1]
    sec = lax.axis_index("section").reshape(1).astype(jnp.int32)
    user = lax.axis_index("shard").reshape(1).astype(jnp.int32)
    like = lambda a: shape(a.shape, a.dtype)

    request, slot, table, _, _ = call(
        request_kernel,
        (shape((shards, 128), jnp.int32), shape((1, cands), jnp.int32), like(tables[0]),
         shape((1, cands), jnp.int32), shape((1, cands), jnp.int32)),
        user, *in_hbm(feat_owner.reshape(1, cands), feat_row.reshape(1, cands), tables[0]),
        smem=1, hbm=3, sems=3, flops=10**8,
    )
    asked = lax.all_to_all(request.reshape(shards, 1, 128), "shard", 0, 0, tiled=True)
    spot, user_vec, item_in, item_out, weight, head = call(
        prepare_kernel,
        (shape((128, 128), F32), shape((1, width), F32), like(item_in), like(item_out),
         like(section_weight[0]), like(section_head)),
        sec, *in_hbm(item_in, item_out, section_weight[0], section_head),
        slot, keep_first, keep_second, user_dense, user_proj,
        smem=1, hbm=4, sems=4, flops=10**9,
    )
    served = call(
        serve_kernel,
        shape((spots, width), BF16),
        asked.reshape(shards, 128), table,
        flops=10**9,
    )
    rows = lax.all_to_all(served.reshape(shards, slots, width), "shard", 0, 0, tiled=True)
    rows = rows.reshape(spots, width)
    packet, score0 = call(
        tower_kernel,
        (shape((2 * final, width), BF16), shape((1, final), F32)),
        sec, spot, rows, user_vec, item_in, item_out,
        smem=1, flops=10**6,
    )
    packet = lax.ppermute(packet, "section", [(0, 1)])
    part, prerank_item = call(
        features_kernel,
        (shape((final + 8, hid), F32), like(prerank_item)),
        sec, *in_hbm(prerank_feat, prerank_item), slot, spot, rows, weight, head,
        smem=1, hbm=2, sems=2, scratch=[pltpu.VMEM(prerank_feat.shape, BF16)], flops=10**9,
    )
    before = lax.ppermute(part, "section", [(2, 3)])
    carry, score1 = call(
        prerank_kernel,
        (shape((final, hid + 128), BF16), shape((1, final), F32)),
        sec, packet, part, prerank_item, weight, head,
        smem=1, flops=10**8,
    )
    near = lax.ppermute(carry, "section", [(1, 2)])
    far = lax.ppermute(carry, "section", [(1, 3)])
    scores = call(
        final_kernel,
        jax.ShapeDtypeStruct((1, final), F32),
        sec, near, far, part, before, score0, score1,
        smem=1, flops=10**6,
    )
    return scores[None]


def solution(mesh):
    placed = (
        P("shard", None),
        P("section", "shard", None),
        P("section", "shard", None, None),
        P("section", "shard", None),
        P("shard", None),
        P("shard", None),
        P("section", None, None),
        P("section", None),
        P(),
        P(),
        P(),
        P(),
        P(),
    )
    return jax.shard_map(
        cascade,
        mesh=mesh,
        in_specs=placed,
        out_specs=P("section", "shard", None),
        check_vma=False,
    )
```

```python
import math

import jax
import jax.numpy as jnp
from jax import lax
from jax.experimental import pallas as pl
from jax.experimental.pallas import tpu as pltpu
from jax.sharding import PartitionSpec as P


F32 = jnp.float32
BF16 = jnp.bfloat16
NT = (((1,), (1,)), ((), ()))


def call(kernel, out_shape, *operands, smem=0, hbm=0, sems=0, flops=0, scratch=()):
    specs = [pl.BlockSpec(memory_space=pltpu.SMEM)] * smem
    specs += [pl.BlockSpec(memory_space=pltpu.HBM)] * hbm
    specs += [pl.BlockSpec(memory_space=pltpu.VMEM)] * (len(operands) - smem - hbm)
    return pl.pallas_call(
        kernel,
        out_shape=out_shape,
        in_specs=specs,
        scratch_shapes=[*scratch, *([pltpu.SemaphoreType.DMA((sems,))] if sems else [])],
        cost_estimate=pl.CostEstimate(flops=flops, transcendentals=0, bytes_accessed=0),
        compiler_params=pltpu.CompilerParams(vmem_limit_bytes=20 << 20),
    )(*operands)


def copies(sources, targets, sem):
    return [pltpu.make_async_copy(a, b, sem.at[i]) for i, (a, b) in enumerate(zip(sources, targets))]


def in_hbm(*arrays):
    return [pltpu.with_memory_space_constraint(a, pltpu.HBM) for a in arrays]


def iota(shape, axis):
    return lax.broadcasted_iota(jnp.int32, shape, axis)


def ones_where(mask):
    return jnp.where(mask, 1.0, 0.0).astype(BF16)


def dot(a, b):
    return jnp.dot(a, b, preferred_element_type=F32)


def dot_nt(a, b):
    return lax.dot_general(a, b, NT, preferred_element_type=F32)


def column(row):
    return jnp.broadcast_to(row, (128, 128)).T


def request_kernel(user_ref, owner_hbm, row_hbm, table_hbm, req_ref, slot_ref, table_ref, owner_ref, row_ref, sem):
    moves = copies((owner_hbm, row_hbm, table_hbm), (owner_ref, row_ref, table_ref), sem)
    for move in moves:
        move.start()
    shards = req_ref.shape[0]
    cands = owner_ref.shape[1]
    slots = 2 * cands // shards
    earlier = ones_where((iota((128, 256), 0) < iota((128, 256), 1)) | (iota((128, 256), 1) >= 128))
    seen = jnp.zeros((shards, 128), F32)
    ranks = []
    moves[0].wait()
    owner = owner_ref[...]
    hits = owner == iota((shards, cands), 0)
    hot = ones_where(hits)
    for b in range(cands // 128):
        part = slice(b * 128, b * 128 + 128)
        counts = dot(hot[:, part], earlier)
        ranks.append(jnp.sum(jnp.where(hits[:, part], counts[:, :128] + seen, 0.0), axis=0, keepdims=True))
        seen = seen + counts[:, 128:]
    rank = jnp.concatenate(ranks, axis=1).astype(jnp.int32)
    slot_ref[...] = owner * slots + rank
    moves[1].wait()
    row = row_ref[...]
    at_slot = rank + (user_ref[0] % (128 // slots)) * slots == iota((128, cands), 0)
    high = jnp.where(at_slot, (row >> 4).astype(F32), 0.0).astype(BF16)
    low = jnp.where(at_slot, (row & 15).astype(F32), 0.0).astype(BF16)
    req_ref[...] = (dot_nt(hot, high) * 16.0 + dot_nt(hot, low)).astype(jnp.int32)
    moves[2].wait()


def halves(table):
    half = table.shape[0] // 2
    return jnp.concatenate([table[:half, :], table[half:, :]], axis=1)


def picked(col, wide):
    half, width = wide.shape[0], wide.shape[1] // 2
    fine = ones_where((col & 127) == iota(col.shape, 1))
    coarse = ((col & (half - 1)) >> 7).astype(F32).astype(BF16)
    hot = [jnp.where(coarse == float(r), fine, jnp.zeros_like(fine)) for r in range(half // 128)]
    both = dot(jnp.concatenate(hot, axis=1), wide)
    return jnp.where(col < half, both[:, :width], both[:, width:]).astype(BF16)


def serve_kernel(ids_ref, table_ref, out_ref):
    users = ids_ref.shape[0]
    rows = out_ref.shape[0]
    group = 128 * users // rows
    step = 4
    wide = halves(table_ref[...])
    for first in range(0, users // group, step):
        cols = [column(jnp.sum(ids_ref[b * group:(b + 1) * group, :], axis=0, keepdims=True))
                for b in range(first, first + step)]
        out_ref[first * 128:(first + step) * 128, :] = picked(jnp.concatenate(cols, axis=0), wide)


def prepare_kernel(sec_ref, in_hbm, out_hbm, weight_hbm, proj_hbm,
                   slot_ref, first_ref, second_ref, dense_ref, head_ref,
                   spot_ref, vec_ref, in_ref, out_ref, weight_ref, proj_ref, sem):
    sec = sec_ref[0]
    moves = copies((in_hbm, out_hbm, weight_hbm, proj_hbm), (in_ref, out_ref, weight_ref, proj_ref), sem)

    @pl.when(sec == 0)
    def _():
        for move in moves:
            move.start()

    slot = slot_ref[...].astype(F32)
    final = second_ref.shape[1]

    def second_column():
        wide = jnp.concatenate([second_ref[...].astype(F32), jnp.zeros((1, 128 - final), F32)], axis=1)
        return column(wide)[:final, :1]

    def lookup(at, row):
        lanes = iota((at.shape[0], row.shape[1]), 1).astype(F32)
        return jnp.sum(jnp.where(lanes == at, row, 0.0), axis=1, keepdims=True)

    @pl.when(sec == 0)
    def _():
        at = lookup(second_column(), first_ref[...].astype(F32))
        spot_ref[:final, :] = jnp.broadcast_to(lookup(at, slot), (final, 128)).astype(jnp.int32)

    @pl.when(sec == 1)
    def _():
        at = second_column() * 4.0
        for f in range(4):
            spot_ref[f * final:f * final + final, :] = jnp.broadcast_to(lookup(at + float(f), slot), (final, 128)).astype(jnp.int32)

    @pl.when(sec == 0)
    def _():
        for move in moves:
            move.wait()
        active = jax.nn.relu(dot(dense_ref[...], weight_ref[...]))
        query = (active * head_ref[...]).astype(BF16)
        vec_ref[...] = dot(query, proj_ref[...])


def as_row(col, lanes):
    n = col.shape[0]
    return jnp.sum(jnp.where(iota((n, lanes), 0) == iota((n, lanes), 1), col, 0.0), axis=0, keepdims=True)


def tower_kernel(sec_ref, spot_ref, rows_ref, vec_ref, in_ref, out_ref, packet_ref, score_ref):
    @pl.when(sec_ref[0] == 0)
    def _():
        n = packet_ref.shape[0] // 2
        embed = picked(spot_ref[:n, :], halves(rows_ref[...]))
        hidden = jax.nn.relu(dot(embed, in_ref[...])).astype(BF16)
        tower = dot(hidden, out_ref[...]).astype(BF16)
        logit = jnp.sum(tower.astype(F32) * vec_ref[...], axis=1, keepdims=True)
        packet_ref[:n, :] = tower
        packet_ref[n:, :] = jnp.broadcast_to(logit, (n, 128)).astype(BF16)
        score_ref[...] = as_row(logit, n)


def features_kernel(sec_ref, feat_hbm, item_hbm, weight_hbm, spot_ref, rows_ref,
                    part_ref, item_ref, weight_ref, feat_ref, sem):
    @pl.when(sec_ref[0] == 1)
    def _():
        n = part_ref.shape[0]
        moves = copies((feat_hbm, item_hbm, weight_hbm), (feat_ref, item_ref, weight_ref), sem)
        for move in moves:
            move.start()
        embed = picked(spot_ref[:4 * n, :], halves(rows_ref[...]))
        tall = jnp.concatenate([embed[f * n:(f + 1) * n, :] for f in range(4)], axis=1)
        moves[0].wait()
        part_ref[...] = dot(tall, feat_ref[...])
        for move in moves[1:]:
            move.wait()


def gram_kernel(sec_ref, weight_hbm, slot_ref, rows_ref, head_ref, part_ref, weight_ref, sem):
    @pl.when(sec_ref[0] >= 2)
    def _():
        n = part_ref.shape[0] - 8
        cands = slot_ref.shape[1]
        width = rows_ref.shape[1]
        move = pltpu.make_async_copy(weight_hbm, weight_ref, sem.at[0])
        move.start()
        wide = halves(rows_ref[...])
        embed = [
            picked(jnp.concatenate([column(slot_ref[:, b:b + 128]) for b in range(h, h + 512, 128)], axis=0), wide)
            for h in range(0, cands, 512)
        ]
        r, c = iota((128, 128), 0), iota((128, 128), 1)
        same_item = (r // 32) == (c // 32)
        spread = ones_where((r % 32) == (c % 32))
        own_lanes = (r % 4) == (c // 32)
        grams = []
        for b in range(cands // 128):
            block = embed[b // 4][b % 4 * 128:b % 4 * 128 + 128, :]
            gram = dot_nt(block, block) * (1.0 / math.sqrt(width))
            gram = jnp.where(same_item, gram, 0.0).astype(BF16)
            grams.append(jnp.where(own_lanes, dot(gram, spread), 0.0).astype(BF16))
        tall = jnp.concatenate(grams, axis=0)
        i, k = iota((8 * n, 32 * n), 0), iota((8 * n, 32 * n), 1)
        choose = ones_where(((k // 32) == (i % n)) & (((k % 32) // 4) == (i // n)))
        flat = dot(choose, tall).astype(BF16)
        flat = jnp.concatenate([flat[q * n:(q + 1) * n, :] for q in range(8)], axis=1)
        move.wait()
        part_ref[:n, :] = dot(flat, weight_ref[...])
        part_ref[n:n + 1, :] = head_ref[...]


def prerank_kernel(sec_ref, packet_ref, part_ref, item_ref, weight_ref, head_ref, carry_ref, score_ref):
    @pl.when(sec_ref[0] == 1)
    def _():
        n, hid = part_ref.shape
        pre = part_ref[...] + dot(packet_ref[:n, :], item_ref[...])
        inner = jax.nn.relu(pre).astype(BF16)
        hidden = jax.nn.relu(dot(inner, weight_ref[...]))
        prior = packet_ref[n:, :].astype(F32)[:, :1]
        logit = jnp.sum(hidden * head_ref[...], axis=1, keepdims=True) / math.sqrt(hid) + prior
        carry_ref[:, :hid] = hidden.astype(BF16)
        carry_ref[:, hid:] = jnp.broadcast_to(logit, (n, 128)).astype(BF16)
        score_ref[...] = as_row(logit, n)


def final_kernel(sec_ref, near_ref, far_ref, part_ref, before_ref, score0_ref, score1_ref, score_ref):
    sec = sec_ref[0]
    n, hid = part_ref.shape[0] - 8, part_ref.shape[1]
    scale = 1.0 / math.sqrt(hid)

    def rank(from_ref, carry, prior):
        hidden = jax.nn.relu(from_ref[:n, :] + carry)
        return hidden, jnp.sum(hidden * from_ref[n:n + 1, :], axis=1, keepdims=True) * scale + prior

    @pl.when(sec == 0)
    def _():
        score_ref[...] = score0_ref[...]

    @pl.when(sec == 1)
    def _():
        score_ref[...] = score1_ref[...]

    @pl.when(sec == 2)
    def _():
        near = near_ref[...].astype(F32)
        _, logit = rank(part_ref, near[:, :hid], near[:, hid:hid + 1])
        score_ref[...] = as_row(logit, n)

    @pl.when(sec == 3)
    def _():
        far = far_ref[...].astype(F32)
        hidden, logit = rank(before_ref, far[:, :hid], far[:, hid:hid + 1])
        prior = logit.astype(BF16).astype(F32)
        _, logit = rank(part_ref, hidden.astype(BF16).astype(F32), prior)
        score_ref[...] = as_row(logit, n)


def cascade(
    user_dense,
    tables,
    feat_owner,
    feat_row,
    keep_first,
    keep_second,
    section_weight,
    section_head,
    user_proj,
    item_in,
    item_out,
    prerank_feat,
    prerank_item,
):
    shape = pltpu.VMEM
    shards = lax.axis_size("shard")
    cands = feat_row.shape[2]
    slots = 2 * cands // shards
    spots = shards * slots
    width = tables.shape[2]
    hid = section_weight.shape[1]
    final = keep_second.shape[1]
    sec = lax.axis_index("section").reshape(1).astype(jnp.int32)
    user = lax.axis_index("shard").reshape(1).astype(jnp.int32)
    like = lambda a: shape(a.shape, a.dtype)

    request, slot, table, _, _ = call(
        request_kernel,
        (shape((shards, 128), jnp.int32), shape((1, cands), jnp.int32), like(tables[0]),
         shape((1, cands), jnp.int32), shape((1, cands), jnp.int32)),
        user, *in_hbm(feat_owner.reshape(1, cands), feat_row.reshape(1, cands), tables[0]),
        smem=1, hbm=3, sems=3, flops=10**8,
    )
    asked = lax.all_to_all(request.reshape(shards, 1, 128), "shard", 0, 0, tiled=True)
    weight = in_hbm(section_weight[0])[0]
    spot, user_vec, item_in, item_out = call(
        prepare_kernel,
        (shape((128, 128), jnp.int32), shape((1, width), F32), like(item_in), like(item_out)),
        sec, *in_hbm(item_in, item_out), weight, *in_hbm(user_proj),
        slot, keep_first, keep_second, user_dense, section_head,
        smem=1, hbm=4, sems=4, scratch=[pltpu.VMEM(weight.shape, BF16), pltpu.VMEM(user_proj.shape, BF16)], flops=10**9,
    )
    served = call(
        serve_kernel,
        shape((spots, width), BF16),
        asked.reshape(shards, 128), table,
        flops=10**9,
    )
    rows = lax.all_to_all(served.reshape(shards, slots, width), "shard", 0, 0, tiled=True)
    rows = rows.reshape(spots, width)
    packet, score0 = call(
        tower_kernel,
        (shape((2 * final, width), BF16), shape((1, final), F32)),
        sec, spot, rows, user_vec, item_in, item_out,
        smem=1, flops=10**6,
    )
    packet = lax.ppermute(packet, "section", [(0, 1)])
    pre, prerank_item, weight_near = call(
        features_kernel,
        (shape((final, hid), F32), like(prerank_item), like(weight)),
        sec, *in_hbm(prerank_feat, prerank_item), weight, spot, rows,
        smem=1, hbm=3, sems=3, scratch=[pltpu.VMEM(prerank_feat.shape, BF16)], flops=10**8,
    )
    carry, score1 = call(
        prerank_kernel,
        (shape((final, hid + 128), BF16), shape((1, final), F32)),
        sec, packet, pre, prerank_item, weight_near, section_head,
        smem=1, flops=10**8,
    )
    far = lax.ppermute(carry, "section", [(1, 3)])
    near = lax.ppermute(carry, "section", [(1, 2)])
    part = call(
        gram_kernel,
        shape((final + 8, hid), F32),
        sec, weight, slot, rows, section_head,
        smem=1, hbm=1, sems=1, scratch=[pltpu.VMEM(weight.shape, BF16)], flops=10**9,
    )
    before = lax.ppermute(part, "section", [(2, 3)])
    scores = call(
        final_kernel,
        jax.ShapeDtypeStruct((1, final), F32),
        sec, near, far, part, before, score0, score1,
        smem=1, flops=10**6,
    )
    return scores[None]


def solution(mesh):
    placed = (
        P("shard", None),
        P("section", "shard", None),
        P("section", "shard", None, None),
        P("section", "shard", None),
        P("shard", None),
        P("shard", None),
        P("section", None, None),
        P("section", None),
        P(),
        P(),
        P(),
        P(),
        P(),
    )
    return jax.shard_map(
        cascade,
        mesh=mesh,
        in_specs=placed,
        out_specs=P("section", "shard", None),
        check_vma=False,
    )
```

```python
import math

import jax
import jax.numpy as jnp
from jax import lax
from jax.experimental import pallas as pl
from jax.experimental.pallas import tpu as pltpu
from jax.sharding import PartitionSpec as P


F32 = jnp.float32
BF16 = jnp.bfloat16
NT = (((1,), (1,)), ((), ()))
MARK = 1 << 14


def call(kernel, out_shape, *operands, smem=0, hbm=0, sems=0, flops=0, scratch=(), smem_out=False):
    specs = [pl.BlockSpec(memory_space=pltpu.SMEM)] * smem
    specs += [pl.BlockSpec(memory_space=pltpu.HBM)] * hbm
    specs += [pl.BlockSpec(memory_space=pltpu.VMEM)] * (len(operands) - smem - hbm)
    vmem, scalar = pl.BlockSpec(memory_space=pltpu.VMEM), pl.BlockSpec(memory_space=pltpu.SMEM)
    many = isinstance(out_shape, (tuple, list))
    return pl.pallas_call(
        kernel,
        out_shape=out_shape,
        out_specs=(vmem, scalar) if smem_out else (vmem,) * len(out_shape) if many else vmem,
        in_specs=specs,
        scratch_shapes=[*scratch, *([pltpu.SemaphoreType.DMA((sems,))] if sems else [])],
        cost_estimate=pl.CostEstimate(flops=flops, transcendentals=0, bytes_accessed=0),
        compiler_params=pltpu.CompilerParams(vmem_limit_bytes=20 << 20),
    )(*operands)


def copies(sources, targets, sem):
    return [pltpu.make_async_copy(a, b, sem.at[i]) for i, (a, b) in enumerate(zip(sources, targets))]


def in_hbm(*arrays):
    return [pltpu.with_memory_space_constraint(a, pltpu.HBM) for a in arrays]


def iota(shape, axis):
    return lax.broadcasted_iota(jnp.int32, shape, axis)


def ones_where(mask):
    return jnp.where(mask, 1.0, 0.0).astype(BF16)


def dot(a, b):
    return jnp.dot(a, b, preferred_element_type=F32)


def dot_nt(a, b):
    return lax.dot_general(a, b, NT, preferred_element_type=F32)


def column(row):
    return jnp.broadcast_to(row, (128, 128)).T


def lookup(at, row):
    lanes = iota((at.shape[0], row.shape[1]), 1).astype(F32)
    return jnp.sum(jnp.where(lanes == at, row.astype(F32), 0.0), axis=1, keepdims=True)


def request_kernel(sec_ref, user_ref, dense_ref, owner_hbm, row_hbm, table_hbm, first_hbm, second_hbm,
                   req_ref, slot_ref, spot_ref, table_ref, owner_ref, row_ref, first_ref, second_ref, sem):
    moves = copies((owner_hbm, row_hbm, first_hbm, second_hbm, table_hbm),
                   (owner_ref, row_ref, first_ref, second_ref, table_ref), sem)
    for move in moves:
        move.start()
    shards = req_ref.shape[0]
    cands = owner_ref.shape[1]
    final = second_ref.shape[1]
    slots = 2 * cands // shards
    base = (user_ref[0] % (128 // slots)) * slots
    sec = sec_ref[0]
    for move in moves[:4]:
        move.wait()

    @pl.when(dense_ref[0] == 1)
    def _():
        earlier = ones_where((iota((128, 256), 0) < iota((128, 256), 1)) | (iota((128, 256), 1) >= 128))
        seen = jnp.zeros((shards, 128), F32)
        ranks = []
        owner = owner_ref[...]
        hits = owner == iota((shards, cands), 0)
        hot = ones_where(hits)
        for b in range(cands // 128):
            part = slice(b * 128, b * 128 + 128)
            counts = dot(hot[:, part], earlier)
            ranks.append(jnp.sum(jnp.where(hits[:, part], counts[:, :128] + seen, 0.0), axis=0, keepdims=True))
            seen = seen + counts[:, 128:]
        rank = jnp.concatenate(ranks, axis=1).astype(jnp.int32)
        slot_ref[...] = owner * slots + rank
        row = row_ref[...]
        at_slot = rank + base == iota((128, cands), 0)
        high = jnp.where(at_slot, (row >> 4).astype(F32), 0.0).astype(BF16)
        low = jnp.where(at_slot, (row & 15).astype(F32), 0.0).astype(BF16)
        req_ref[...] = (dot_nt(hot, high) * 16.0 + dot_nt(hot, low)).astype(jnp.int32)

    @pl.when(dense_ref[0] == 0)
    def _():
        second = jnp.concatenate([second_ref[...], jnp.zeros((1, 128 - final), jnp.int32)], axis=1)
        second = column(second.astype(F32))[:final, :1]
        single = lookup(second, first_ref[...])
        fours = [second * 4.0 + float(f) for f in range(4)]
        none = jnp.full((final, 1), -1.0, F32)
        at = jnp.concatenate(
            [jnp.where(sec == 0, single if f == 0 else none, fours[f]) for f in range(4)], axis=0)
        owner = lookup(at, owner_ref[...] + 1) - 1.0
        row = lookup(at, row_ref[...]).astype(jnp.int32)
        count = at.shape[0]
        lanes = iota((count, 128), 1).astype(F32)
        hot = jnp.where(owner == lanes, 1.0, 0.0)
        before = ones_where(iota((count, count), 1) < iota((count, count), 0))
        rank = jnp.sum(hot * dot(before, hot.astype(BF16)), axis=1, keepdims=True)
        spot_ref[...] = jnp.broadcast_to(owner * slots + rank, spot_ref.shape).astype(jnp.int32)
        at_slot = rank + base.astype(F32) == lanes
        high = jnp.where(at_slot, (row >> 4).astype(F32), 0.0).astype(BF16)
        low = jnp.where(at_slot, (row & 15).astype(F32), 0.0).astype(BF16)
        turned = hot.T.astype(BF16)
        mine = (iota((1, 128), 1) >= base) & (iota((1, 128), 1) < base + slots)
        over = jnp.max(rank, axis=0, keepdims=True) >= slots // 2
        mark = jnp.where(mine & over, MARK, 0)
        req_ref[...] = (dot(turned, high) * 16.0 + dot(turned, low)).astype(jnp.int32) + mark

    moves[4].wait()


def halves(table):
    half = table.shape[0] // 2
    return jnp.concatenate([table[:half, :], table[half:, :]], axis=1)


def picked(col, wide):
    half, width = wide.shape[0], wide.shape[1] // 2
    fine = ones_where((col & 127) == iota(col.shape, 1))
    coarse = ((col & (half - 1)) >> 7).astype(F32).astype(BF16)
    hot = [jnp.where(coarse == float(r), fine, jnp.zeros_like(fine)) for r in range(half // 128)]
    both = dot(jnp.concatenate(hot, axis=1), wide)
    return jnp.where(col < half, both[:, :width], both[:, width:]).astype(BF16)


def served_rows(ids_ref, table_ref, out_ref, keep):
    users = ids_ref.shape[0]
    slots = out_ref.shape[0] // users * 16 // keep
    group = 128 // slots
    wide = halves(table_ref[...])
    count = group * keep
    step = 512 // count
    for first in range(0, users // group, step):
        cols = []
        for b in range(first, first + step):
            ids = jnp.sum(ids_ref[b * group:(b + 1) * group, :], axis=0, keepdims=True)
            col = column(ids & (MARK - 1))
            cols += [col[i * slots:i * slots + keep, :] for i in range(group)] if keep < slots else [col]
        out_ref[first * count:(first + step) * count, :] = picked(jnp.concatenate(cols, axis=0), wide)


def serve_kernel(ids_ref, table_ref, out_ref):
    served_rows(ids_ref, table_ref, out_ref, 16)


def serve_short_kernel(ids_ref, table_ref, out_ref, over_ref):
    over_ref[0] = jnp.max(ids_ref[...])
    served_rows(ids_ref, table_ref, out_ref, 8)


def nothing_kernel(*refs):
    pass


def prepare_kernel(sec_ref, in_hbm, out_hbm, weight_hbm, proj_hbm, dense_ref, head_ref,
                   vec_ref, in_ref, out_ref, weight_ref, proj_ref, sem):
    @pl.when(sec_ref[0] == 0)
    def _():
        moves = copies((in_hbm, out_hbm, weight_hbm, proj_hbm), (in_ref, out_ref, weight_ref, proj_ref), sem)
        for move in moves:
            move.start()
        for move in moves:
            move.wait()
        active = jax.nn.relu(dot(dense_ref[...], weight_ref[...]))
        query = (active * head_ref[...]).astype(BF16)
        vec_ref[...] = dot(query, proj_ref[...])


def as_row(col, lanes):
    n = col.shape[0]
    return jnp.sum(jnp.where(iota((n, lanes), 0) == iota((n, lanes), 1), col, 0.0), axis=0, keepdims=True)


def tower_kernel(sec_ref, spot_ref, rows_ref, vec_ref, in_ref, out_ref, packet_ref, score_ref):
    @pl.when(sec_ref[0] == 0)
    def _():
        n = packet_ref.shape[0] // 2
        embed = picked(spot_ref[:n, :], halves(rows_ref[...]))
        hidden = jax.nn.relu(dot(embed, in_ref[...])).astype(BF16)
        tower = dot(hidden, out_ref[...]).astype(BF16)
        logit = jnp.sum(tower.astype(F32) * vec_ref[...], axis=1, keepdims=True)
        packet_ref[:n, :] = tower
        packet_ref[n:, :] = jnp.broadcast_to(logit, (n, 128)).astype(BF16)
        score_ref[...] = as_row(logit, n)


def features_kernel(sec_ref, feat_hbm, item_hbm, weight_hbm, spot_ref, rows_ref,
                    part_ref, item_ref, weight_ref, feat_ref, sem):
    @pl.when(sec_ref[0] == 1)
    def _():
        n = part_ref.shape[0]
        moves = copies((feat_hbm, item_hbm, weight_hbm), (feat_ref, item_ref, weight_ref), sem)
        for move in moves:
            move.start()
        embed = picked(spot_ref[:4 * n, :], halves(rows_ref[...]))
        tall = jnp.concatenate([embed[f * n:(f + 1) * n, :] for f in range(4)], axis=1)
        moves[0].wait()
        part_ref[...] = dot(tall, feat_ref[...])
        for move in moves[1:]:
            move.wait()


def gram_kernel(sec_ref, weight_hbm, slot_ref, rows_ref, head_ref, part_ref, weight_ref, sem):
    @pl.when(sec_ref[0] >= 2)
    def _():
        n = part_ref.shape[0] - 8
        cands = slot_ref.shape[1]
        width = rows_ref.shape[1]
        move = pltpu.make_async_copy(weight_hbm, weight_ref, sem.at[0])
        move.start()
        wide = halves(rows_ref[...])
        embed = [
            picked(jnp.concatenate([column(slot_ref[:, b:b + 128]) for b in range(h, h + 512, 128)], axis=0), wide)
            for h in range(0, cands, 512)
        ]
        r, c = iota((128, 128), 0), iota((128, 128), 1)
        same_item = (r // 32) == (c // 32)
        spread = ones_where((r % 32) == (c % 32))
        own_lanes = (r % 4) == (c // 32)
        grams = []
        for b in range(cands // 128):
            block = embed[b // 4][b % 4 * 128:b % 4 * 128 + 128, :]
            gram = dot_nt(block, block) * (1.0 / math.sqrt(width))
            gram = jnp.where(same_item, gram, 0.0).astype(BF16)
            grams.append(jnp.where(own_lanes, dot(gram, spread), 0.0).astype(BF16))
        tall = jnp.concatenate(grams, axis=0)
        i, k = iota((8 * n, 32 * n), 0), iota((8 * n, 32 * n), 1)
        choose = ones_where(((k // 32) == (i % n)) & (((k % 32) // 4) == (i // n)))
        flat = dot(choose, tall).astype(BF16)
        flat = jnp.concatenate([flat[q * n:(q + 1) * n, :] for q in range(8)], axis=1)
        move.wait()
        part_ref[:n, :] = dot(flat, weight_ref[...])
        part_ref[n:n + 1, :] = head_ref[...]


def prerank_kernel(sec_ref, packet_ref, part_ref, item_ref, weight_ref, head_ref, carry_ref, score_ref):
    @pl.when(sec_ref[0] == 1)
    def _():
        n, hid = part_ref.shape
        pre = part_ref[...] + dot(packet_ref[:n, :], item_ref[...])
        inner = jax.nn.relu(pre).astype(BF16)
        hidden = jax.nn.relu(dot(inner, weight_ref[...]))
        prior = packet_ref[n:, :].astype(F32)[:, :1]
        logit = jnp.sum(hidden * head_ref[...], axis=1, keepdims=True) / math.sqrt(hid) + prior
        carry_ref[:, :hid] = hidden.astype(BF16)
        carry_ref[:, hid:] = jnp.broadcast_to(logit, (n, 128)).astype(BF16)
        score_ref[...] = as_row(logit, n)


def rank(part_ref, carry_ref):
    n, hid = part_ref.shape[0] - 8, part_ref.shape[1]
    carry = carry_ref[...].astype(F32)
    hidden = jax.nn.relu(part_ref[:n, :] + carry[:, :hid])
    logit = jnp.sum(hidden * part_ref[n:n + 1, :], axis=1, keepdims=True) / math.sqrt(hid)
    return hidden, logit + carry[:, hid:hid + 1]


def rank_kernel(sec_ref, near_ref, part_ref, carry_ref, score_ref):
    @pl.when(sec_ref[0] == 2)
    def _():
        n, hid = part_ref.shape[0] - 8, part_ref.shape[1]
        hidden, logit = rank(part_ref, near_ref)
        carry_ref[:, :hid] = hidden.astype(BF16)
        carry_ref[:, hid:] = jnp.broadcast_to(logit, (n, 128)).astype(BF16)
        score_ref[...] = as_row(logit, n)


def final_kernel(sec_ref, last_ref, part_ref, score0_ref, score1_ref, score2_ref, score_ref):
    sec = sec_ref[0]

    for s, from_ref in enumerate((score0_ref, score1_ref, score2_ref)):
        @pl.when(sec == s)
        def _():
            score_ref[...] = from_ref[...]

    @pl.when(sec == 3)
    def _():
        _, logit = rank(part_ref, last_ref)
        score_ref[...] = as_row(logit, logit.shape[0])


def cascade(
    user_dense,
    tables,
    feat_owner,
    feat_row,
    keep_first,
    keep_second,
    section_weight,
    section_head,
    user_proj,
    item_in,
    item_out,
    prerank_feat,
    prerank_item,
):
    shape = pltpu.VMEM
    shards = lax.axis_size("shard")
    cands = feat_row.shape[2]
    slots = 2 * cands // shards
    spots = shards * slots
    width = tables.shape[2]
    hid = section_weight.shape[1]
    final = keep_second.shape[1]
    sec = lax.axis_index("section").reshape(1).astype(jnp.int32)
    user = lax.axis_index("shard").reshape(1).astype(jnp.int32)
    dense = sec[0] >= 2
    like = lambda a: shape(a.shape, a.dtype)

    weight, feat, item, into, out_of, proj = in_hbm(
        section_weight[0], prerank_feat, prerank_item, item_in, item_out, user_proj)

    request, slot, spot, table = call(
        request_kernel,
        (shape((shards, 128), jnp.int32), shape((1, cands), jnp.int32), shape((128, 128), jnp.int32), like(tables[0])),
        sec, user, dense.astype(jnp.int32).reshape(1), *in_hbm(feat_owner.reshape(1, cands), feat_row.reshape(1, cands), tables[0], keep_first, keep_second),
        smem=3, hbm=5, sems=5, flops=10**8,
        scratch=[pltpu.VMEM(s, jnp.int32) for s in ((1, cands), (1, cands), keep_first.shape, keep_second.shape)],
    )
    asked = lax.all_to_all(request.reshape(shards, 1, 128), "shard", 0, 0, tiled=True).reshape(shards, 128)

    def exchanged(served):
        rows = lax.all_to_all(served.reshape(shards, -1, width), "shard", 0, 0, tiled=True)
        rows = jnp.pad(rows, ((0, 0), (0, slots - rows.shape[1]), (0, 0)))
        return rows.reshape(spots, width)

    def serve():
        return call(serve_kernel, shape((spots, width), BF16), asked, table, flops=10**9)

    def blank(*shapes):
        return pl.pallas_call(
            nothing_kernel,
            out_shape=shapes,
            in_specs=[pl.BlockSpec(memory_space=pl.ANY)],
            out_specs=(pl.BlockSpec(memory_space=pltpu.VMEM),) * len(shapes),
            compiler_params=pltpu.CompilerParams(vmem_limit_bytes=1 << 20),
        )(asked)

    scored = shape((1, final), F32)
    carried = shape((final, hid + 128), BF16)

    def sparse_sections():
        served, over = call(
            serve_short_kernel,
            (shape((spots // 2, width), BF16), jax.ShapeDtypeStruct((1,), jnp.int32)),
            asked, table, flops=10**9, smem_out=True,
        )

        def with_query(given):
            rows = exchanged(given)
            query = call(
                prepare_kernel,
                (shape((1, width), F32), like(item_in), like(item_out)),
                sec, into, out_of, weight, proj, user_dense, section_head,
                smem=1, hbm=4, sems=4, flops=10**9,
                scratch=[pltpu.VMEM(weight.shape, BF16), pltpu.VMEM(user_proj.shape, BF16)],
            )
            return rows, *query

        rows, *query = lax.cond(over[0] >= MARK, lambda: with_query(serve()), lambda: with_query(served))
        packet, score0 = call(
            tower_kernel,
            (shape((2 * final, width), BF16), scored),
            sec, spot, rows, *query,
            smem=1, flops=10**6,
        )
        packet = lax.ppermute(packet, "section", [(0, 1)])
        pre, item_near, weight_near = call(
            features_kernel,
            (shape((final, hid), F32), like(prerank_item), like(weight)),
            sec, feat, item, weight, spot, rows,
            smem=1, hbm=3, sems=3, scratch=[pltpu.VMEM(prerank_feat.shape, BF16)], flops=10**8,
        )
        carry, score1 = call(
            prerank_kernel,
            (carried, scored),
            sec, packet, pre, item_near, weight_near, section_head,
            smem=1, flops=10**8,
        )
        return carry, score0, score1

    def dense_sections():
        return call(
            gram_kernel,
            shape((final + 8, hid), F32),
            sec, weight, slot, exchanged(serve()), section_head,
            smem=1, hbm=1, sems=1, scratch=[pltpu.VMEM(weight.shape, BF16)], flops=10**9,
        )

    carry, score0, score1 = lax.cond(dense, lambda: tuple(blank(carried, scored, scored)), sparse_sections)
    near = lax.ppermute(carry, "section", [(1, 2)])
    part = lax.cond(dense, dense_sections, lambda: blank(shape((final + 8, hid), F32))[0])
    carry, score2 = call(rank_kernel, (carried, scored), sec, near, part, smem=1, flops=10**6)
    last = lax.ppermute(carry, "section", [(2, 3)])
    scores = call(
        final_kernel,
        jax.ShapeDtypeStruct((1, final), F32),
        sec, last, part, score0, score1, score2,
        smem=1, flops=10**6,
    )
    return scores[None]


def solution(mesh):
    placed = (
        P("shard", None),
        P("section", "shard", None),
        P("section", "shard", None, None),
        P("section", "shard", None),
        P("shard", None),
        P("shard", None),
        P("section", None, None),
        P("section", None),
        P(),
        P(),
        P(),
        P(),
        P(),
    )
    return jax.shard_map(
        cascade,
        mesh=mesh,
        in_specs=placed,
        out_specs=P("section", "shard", None),
        check_vma=False,
    )
```

```python
import math

import jax
import jax.numpy as jnp
from jax import lax
from jax.experimental import pallas as pl
from jax.experimental.pallas import tpu as pltpu
from jax.sharding import PartitionSpec as P


F32 = jnp.float32
BF16 = jnp.bfloat16
NT = (((1,), (1,)), ((), ()))
MARK = 1 << 14


def call(kernel, out_shape, *operands, smem=0, hbm=0, sems=0, flops=0, scratch=(), smem_out=False):
    specs = [pl.BlockSpec(memory_space=pltpu.SMEM)] * smem
    specs += [pl.BlockSpec(memory_space=pltpu.HBM)] * hbm
    specs += [pl.BlockSpec(memory_space=pltpu.VMEM)] * (len(operands) - smem - hbm)
    vmem, scalar = pl.BlockSpec(memory_space=pltpu.VMEM), pl.BlockSpec(memory_space=pltpu.SMEM)
    many = isinstance(out_shape, (tuple, list))
    return pl.pallas_call(
        kernel,
        out_shape=out_shape,
        out_specs=(vmem,) * (len(out_shape) - 1) + (scalar,) if smem_out else (vmem,) * len(out_shape) if many else vmem,
        in_specs=specs,
        scratch_shapes=[*scratch, *([pltpu.SemaphoreType.DMA((sems,))] if sems else [])],
        cost_estimate=pl.CostEstimate(flops=flops, transcendentals=0, bytes_accessed=0),
        compiler_params=pltpu.CompilerParams(vmem_limit_bytes=20 << 20),
    )(*operands)


def copies(sources, targets, sem):
    return [pltpu.make_async_copy(a, b, sem.at[i]) for i, (a, b) in enumerate(zip(sources, targets))]


def in_hbm(*arrays):
    return [pltpu.with_memory_space_constraint(a, pltpu.HBM) for a in arrays]


def iota(shape, axis):
    return lax.broadcasted_iota(jnp.int32, shape, axis)


def ones_where(mask):
    return jnp.where(mask, 1.0, 0.0).astype(BF16)


def dot(a, b):
    return jnp.dot(a, b, preferred_element_type=F32)


def dot_nt(a, b):
    return lax.dot_general(a, b, NT, preferred_element_type=F32)


def column(row):
    return jnp.broadcast_to(row, (128, 128)).T


def lookup(at, row):
    lanes = iota((at.shape[0], row.shape[1]), 1).astype(F32)
    return jnp.sum(jnp.where(lanes == at, row.astype(F32), 0.0), axis=1, keepdims=True)


def request_kernel(sec_ref, user_ref, dense_ref, owner_hbm, row_hbm, table_hbm, first_hbm, second_hbm,
                   weight_hbm, proj_hbm, into_hbm, out_of_hbm,
                   req_ref, slot_ref, spot_ref, table_ref, weight_ref, proj_ref, into_ref, out_of_ref,
                   owner_ref, row_ref, first_ref, second_ref, sem):
    moves = copies((owner_hbm, row_hbm, first_hbm, second_hbm, table_hbm),
                   (owner_ref, row_ref, first_ref, second_ref, table_ref), sem)
    for move in moves:
        move.start()
    later = [pltpu.make_async_copy(a, b, sem.at[5 + i]) for i, (a, b) in enumerate((
        (weight_hbm, weight_ref), (proj_hbm, proj_ref), (into_hbm, into_ref), (out_of_hbm, out_of_ref)))]

    @pl.when(dense_ref[0] == 0)
    def _():
        for move in later:
            move.start()

    shards = req_ref.shape[0]
    cands = owner_ref.shape[1]
    final = second_ref.shape[1]
    slots = 2 * cands // shards
    base = (user_ref[0] % (128 // slots)) * slots
    sec = sec_ref[0]
    for move in moves[:4]:
        move.wait()

    @pl.when(dense_ref[0] == 1)
    def _():
        earlier = ones_where((iota((128, 256), 0) < iota((128, 256), 1)) | (iota((128, 256), 1) >= 128))
        seen = jnp.zeros((shards, 128), F32)
        ranks = []
        owner = owner_ref[...]
        hits = owner == iota((shards, cands), 0)
        hot = ones_where(hits)
        for b in range(cands // 128):
            part = slice(b * 128, b * 128 + 128)
            counts = dot(hot[:, part], earlier)
            ranks.append(jnp.sum(jnp.where(hits[:, part], counts[:, :128] + seen, 0.0), axis=0, keepdims=True))
            seen = seen + counts[:, 128:]
        rank = jnp.concatenate(ranks, axis=1).astype(jnp.int32)
        slot_ref[...] = owner * slots + rank
        row = row_ref[...]
        at_slot = rank + base == iota((128, cands), 0)
        high = jnp.where(at_slot, (row >> 4).astype(F32), 0.0).astype(BF16)
        low = jnp.where(at_slot, (row & 15).astype(F32), 0.0).astype(BF16)
        req_ref[...] = (dot_nt(hot, high) * 16.0 + dot_nt(hot, low)).astype(jnp.int32)

    @pl.when(dense_ref[0] == 0)
    def _():
        second = jnp.concatenate([second_ref[...], jnp.zeros((1, 128 - final), jnp.int32)], axis=1)
        second = column(second.astype(F32))[:final, :1]
        single = lookup(second, first_ref[...])
        fours = [second * 4.0 + float(f) for f in range(4)]
        none = jnp.full((final, 1), -1.0, F32)
        at = jnp.concatenate(
            [jnp.where(sec == 0, single if f == 0 else none, fours[f]) for f in range(4)], axis=0)
        owner = lookup(at, owner_ref[...] + 1) - 1.0
        row = lookup(at, row_ref[...]).astype(jnp.int32)
        count = at.shape[0]
        lanes = iota((count, 128), 1).astype(F32)
        hot = jnp.where(owner == lanes, 1.0, 0.0)
        before = ones_where(iota((count, count), 1) < iota((count, count), 0))
        rank = jnp.sum(hot * dot(before, hot.astype(BF16)), axis=1, keepdims=True)
        spot_ref[...] = jnp.broadcast_to(owner * slots + rank, spot_ref.shape).astype(jnp.int32)
        at_slot = rank + base.astype(F32) == lanes
        high = jnp.where(at_slot, (row >> 4).astype(F32), 0.0).astype(BF16)
        low = jnp.where(at_slot, (row & 15).astype(F32), 0.0).astype(BF16)
        turned = hot.T.astype(BF16)
        mine = (iota((1, 128), 1) >= base) & (iota((1, 128), 1) < base + slots)
        over = jnp.max(rank, axis=0, keepdims=True) >= slots // 2
        mark = jnp.where(mine & over, MARK, 0)
        req_ref[...] = (dot(turned, high) * 16.0 + dot(turned, low)).astype(jnp.int32) + mark
        for move in later:
            move.wait()

    moves[4].wait()


def halves(table):
    half = table.shape[0] // 2
    return jnp.concatenate([table[:half, :], table[half:, :]], axis=1)


def picked(col, wide):
    half, width = wide.shape[0], wide.shape[1] // 2
    fine = ones_where((col & 127) == iota(col.shape, 1))
    coarse = ((col & (half - 1)) >> 7).astype(F32).astype(BF16)
    hot = [jnp.where(coarse == float(r), fine, jnp.zeros_like(fine)) for r in range(half // 128)]
    both = dot(jnp.concatenate(hot, axis=1), wide)
    return jnp.where(col < half, both[:, :width], both[:, width:]).astype(BF16)


def served_rows(ids_ref, table_ref, out_ref, keep):
    users = ids_ref.shape[0]
    slots = out_ref.shape[0] // users * 16 // keep
    group = 128 // slots
    wide = halves(table_ref[...])
    count = group * keep
    step = 512 // count
    for first in range(0, users // group, step):
        cols = []
        for b in range(first, first + step):
            ids = jnp.sum(ids_ref[b * group:(b + 1) * group, :], axis=0, keepdims=True)
            col = column(ids & (MARK - 1))
            cols += [col[i * slots:i * slots + keep, :] for i in range(group)] if keep < slots else [col]
        out_ref[first * count:(first + step) * count, :] = picked(jnp.concatenate(cols, axis=0), wide)


def serve_kernel(ids_ref, table_ref, out_ref):
    served_rows(ids_ref, table_ref, out_ref, 16)


def serve_short_kernel(sec_ref, ids_ref, table_ref, dense_ref, weight_ref, head_ref, proj_ref,
                       out_ref, vec_ref, over_ref):
    over_ref[0] = jnp.max(ids_ref[...])
    served_rows(ids_ref, table_ref, out_ref, 8)

    @pl.when(sec_ref[0] == 0)
    def _():
        active = jax.nn.relu(dot(dense_ref[...], weight_ref[...]))
        query = (active * head_ref[...]).astype(BF16)
        vec_ref[...] = dot(query, proj_ref[...])


def nothing_kernel(*refs):
    pass


def as_row(col, lanes):
    n = col.shape[0]
    return jnp.sum(jnp.where(iota((n, lanes), 0) == iota((n, lanes), 1), col, 0.0), axis=0, keepdims=True)


def survivors_kernel(sec_ref, feat_hbm, item_hbm, spot_ref, rows_ref, vec_ref, into_ref, out_of_ref,
                     packet_ref, score_ref, part_ref, item_ref, feat_ref, sem):
    n = part_ref.shape[0]
    slots = rows_ref.shape[0] // 128
    spot = spot_ref[...]
    spot = (spot >> 4) * slots + (spot & 15)

    @pl.when(sec_ref[0] == 0)
    def _():
        embed = picked(spot[:n, :], halves(rows_ref[...]))
        hidden = jax.nn.relu(dot(embed, into_ref[...])).astype(BF16)
        tower = dot(hidden, out_of_ref[...]).astype(BF16)
        logit = jnp.sum(tower.astype(F32) * vec_ref[...], axis=1, keepdims=True)
        packet_ref[:n, :] = tower
        packet_ref[n:, :] = jnp.broadcast_to(logit, (n, 128)).astype(BF16)
        score_ref[...] = as_row(logit, n)

    @pl.when(sec_ref[0] == 1)
    def _():
        moves = copies((feat_hbm, item_hbm), (feat_ref, item_ref), sem)
        for move in moves:
            move.start()
        embed = picked(spot[:4 * n, :], halves(rows_ref[...]))
        tall = jnp.concatenate([embed[f * n:(f + 1) * n, :] for f in range(4)], axis=1)
        for move in moves:
            move.wait()
        part_ref[...] = dot(tall, feat_ref[...])


def gram_kernel(sec_ref, weight_hbm, slot_ref, rows_ref, head_ref, part_ref, weight_ref, sem):
    @pl.when(sec_ref[0] >= 2)
    def _():
        n = part_ref.shape[0] - 8
        cands = slot_ref.shape[1]
        width = rows_ref.shape[1]
        move = pltpu.make_async_copy(weight_hbm, weight_ref, sem.at[0])
        move.start()
        wide = halves(rows_ref[...])
        embed = [
            picked(jnp.concatenate([column(slot_ref[:, b:b + 128]) for b in range(h, h + 512, 128)], axis=0), wide)
            for h in range(0, cands, 512)
        ]
        r, c = iota((128, 128), 0), iota((128, 128), 1)
        same_item = (r // 32) == (c // 32)
        spread = ones_where((r % 32) == (c % 32))
        own_lanes = (r % 4) == (c // 32)
        grams = []
        for b in range(cands // 128):
            block = embed[b // 4][b % 4 * 128:b % 4 * 128 + 128, :]
            gram = dot_nt(block, block) * (1.0 / math.sqrt(width))
            gram = jnp.where(same_item, gram, 0.0).astype(BF16)
            grams.append(jnp.where(own_lanes, dot(gram, spread), 0.0).astype(BF16))
        tall = jnp.concatenate(grams, axis=0)
        i, k = iota((8 * n, 32 * n), 0), iota((8 * n, 32 * n), 1)
        choose = ones_where(((k // 32) == (i % n)) & (((k % 32) // 4) == (i // n)))
        flat = dot(choose, tall).astype(BF16)
        flat = jnp.concatenate([flat[q * n:(q + 1) * n, :] for q in range(8)], axis=1)
        move.wait()
        part_ref[:n, :] = dot(flat, weight_ref[...])
        part_ref[n:n + 1, :] = head_ref[...]


def prerank_kernel(sec_ref, packet_ref, part_ref, item_ref, weight_ref, head_ref, carry_ref, score_ref):
    @pl.when(sec_ref[0] == 1)
    def _():
        n, hid = part_ref.shape
        pre = part_ref[...] + dot(packet_ref[:n, :], item_ref[...])
        inner = jax.nn.relu(pre).astype(BF16)
        hidden = jax.nn.relu(dot(inner, weight_ref[...]))
        prior = packet_ref[n:, :].astype(F32)[:, :1]
        logit = jnp.sum(hidden * head_ref[...], axis=1, keepdims=True) / math.sqrt(hid) + prior
        carry_ref[:, :hid] = hidden.astype(BF16)
        carry_ref[:, hid:] = jnp.broadcast_to(logit, (n, 128)).astype(BF16)
        score_ref[...] = as_row(logit, n)


def rank(part_ref, carry_ref):
    n, hid = part_ref.shape[0] - 8, part_ref.shape[1]
    carry = carry_ref[...].astype(F32)
    hidden = jax.nn.relu(part_ref[:n, :] + carry[:, :hid])
    logit = jnp.sum(hidden * part_ref[n:n + 1, :], axis=1, keepdims=True) / math.sqrt(hid)
    return hidden, logit + carry[:, hid:hid + 1]


def rank_kernel(sec_ref, near_ref, part_ref, carry_ref, score_ref):
    @pl.when(sec_ref[0] == 2)
    def _():
        n, hid = part_ref.shape[0] - 8, part_ref.shape[1]
        hidden, logit = rank(part_ref, near_ref)
        carry_ref[:, :hid] = hidden.astype(BF16)
        carry_ref[:, hid:] = jnp.broadcast_to(logit, (n, 128)).astype(BF16)
        score_ref[...] = as_row(logit, n)


def final_kernel(sec_ref, last_ref, part_ref, score0_ref, score1_ref, score2_ref, score_ref):
    sec = sec_ref[0]

    for s, from_ref in enumerate((score0_ref, score1_ref, score2_ref)):
        @pl.when(sec == s)
        def _():
            score_ref[...] = from_ref[...]

    @pl.when(sec == 3)
    def _():
        _, logit = rank(part_ref, last_ref)
        score_ref[...] = as_row(logit, logit.shape[0])


def cascade(
    user_dense,
    tables,
    feat_owner,
    feat_row,
    keep_first,
    keep_second,
    section_weight,
    section_head,
    user_proj,
    item_in,
    item_out,
    prerank_feat,
    prerank_item,
):
    shape = pltpu.VMEM
    shards = lax.axis_size("shard")
    cands = feat_row.shape[2]
    slots = 2 * cands // shards
    spots = shards * slots
    width = tables.shape[2]
    hid = section_weight.shape[1]
    final = keep_second.shape[1]
    sec = lax.axis_index("section").reshape(1).astype(jnp.int32)
    user = lax.axis_index("shard").reshape(1).astype(jnp.int32)
    dense = sec[0] >= 2
    like = lambda a: shape(a.shape, a.dtype)

    weight, feat, item, into, out_of, proj = in_hbm(
        section_weight[0], prerank_feat, prerank_item, item_in, item_out, user_proj)

    request, slot, spot, table, weight_near, proj_near, into_near, out_of_near = call(
        request_kernel,
        (shape((shards, 128), jnp.int32), shape((1, cands), jnp.int32), shape((128, 128), jnp.int32), like(tables[0]),
         like(weight), like(proj), like(into), like(out_of)),
        sec, user, dense.astype(jnp.int32).reshape(1),
        *in_hbm(feat_owner.reshape(1, cands), feat_row.reshape(1, cands), tables[0], keep_first, keep_second),
        weight, proj, into, out_of,
        smem=3, hbm=9, sems=9, flops=10**8,
        scratch=[pltpu.VMEM(s, jnp.int32) for s in ((1, cands), (1, cands), keep_first.shape, keep_second.shape)],
    )
    asked = lax.all_to_all(request.reshape(shards, 1, 128), "shard", 0, 0, tiled=True).reshape(shards, 128)

    def exchanged(served):
        rows = lax.all_to_all(served.reshape(shards, -1, width), "shard", 0, 0, tiled=True)
        return rows.reshape(-1, width)

    def serve():
        return call(serve_kernel, shape((spots, width), BF16), asked, table, flops=10**9)

    def blank(*shapes):
        return pl.pallas_call(
            nothing_kernel,
            out_shape=shapes,
            in_specs=[pl.BlockSpec(memory_space=pl.ANY)],
            out_specs=(pl.BlockSpec(memory_space=pltpu.VMEM),) * len(shapes),
            compiler_params=pltpu.CompilerParams(vmem_limit_bytes=1 << 20),
        )(asked)

    scored = shape((1, final), F32)
    carried = shape((final, hid + 128), BF16)

    def sparse_sections():
        served, query, over = call(
            serve_short_kernel,
            (shape((spots // 2, width), BF16), shape((1, width), F32), jax.ShapeDtypeStruct((1,), jnp.int32)),
            sec, asked, table, user_dense, weight_near, section_head, proj_near,
            smem=1, flops=10**9, smem_out=True,
        )

        def survivors(given):
            return tuple(call(
                survivors_kernel,
                (shape((2 * final, width), BF16), scored, shape((final, hid), F32), like(prerank_item)),
                sec, feat, item, spot, exchanged(given), query, into_near, out_of_near,
                smem=1, hbm=2, sems=2, scratch=[pltpu.VMEM(prerank_feat.shape, BF16)], flops=10**8,
            ))

        packet, score0, pre, item_near = lax.cond(
            over[0] >= MARK, lambda: survivors(serve()), lambda: survivors(served))
        packet = lax.ppermute(packet, "section", [(0, 1)])
        carry, score1 = call(
            prerank_kernel,
            (carried, scored),
            sec, packet, pre, item_near, weight_near, section_head,
            smem=1, flops=10**8,
        )
        return carry, score0, score1

    def dense_sections():
        return call(
            gram_kernel,
            shape((final + 8, hid), F32),
            sec, weight, slot, exchanged(serve()), section_head,
            smem=1, hbm=1, sems=1, scratch=[pltpu.VMEM(weight.shape, BF16)], flops=10**9,
        )

    carry, score0, score1 = lax.cond(dense, lambda: tuple(blank(carried, scored, scored)), sparse_sections)
    near = lax.ppermute(carry, "section", [(1, 2)])
    part = lax.cond(dense, dense_sections, lambda: blank(shape((final + 8, hid), F32))[0])
    carry, score2 = call(rank_kernel, (carried, scored), sec, near, part, smem=1, flops=10**6)
    last = lax.ppermute(carry, "section", [(2, 3)])
    scores = call(
        final_kernel,
        jax.ShapeDtypeStruct((1, final), F32),
        sec, last, part, score0, score1, score2,
        smem=1, flops=10**6,
    )
    return scores[None]


def solution(mesh):
    placed = (
        P("shard", None),
        P("section", "shard", None),
        P("section", "shard", None, None),
        P("section", "shard", None),
        P("shard", None),
        P("shard", None),
        P("section", None, None),
        P("section", None),
        P(),
        P(),
        P(),
        P(),
        P(),
    )
    return jax.shard_map(
        cascade,
        mesh=mesh,
        in_specs=placed,
        out_specs=P("section", "shard", None),
        check_vma=False,
    )
```

```python
import math

import jax
import jax.numpy as jnp
from jax import lax
from jax.experimental import pallas as pl
from jax.experimental.pallas import tpu as pltpu
from jax.sharding import PartitionSpec as P


F32 = jnp.float32
BF16 = jnp.bfloat16
NT = (((1,), (1,)), ((), ()))
MARK = 1 << 14


def call(kernel, out_shape, *operands, smem=0, hbm=0, sems=0, flops=0, scratch=(), smem_out=False):
    specs = [pl.BlockSpec(memory_space=pltpu.SMEM)] * smem
    specs += [pl.BlockSpec(memory_space=pltpu.HBM)] * hbm
    specs += [pl.BlockSpec(memory_space=pltpu.VMEM)] * (len(operands) - smem - hbm)
    vmem, scalar = pl.BlockSpec(memory_space=pltpu.VMEM), pl.BlockSpec(memory_space=pltpu.SMEM)
    many = isinstance(out_shape, (tuple, list))
    return pl.pallas_call(
        kernel,
        out_shape=out_shape,
        out_specs=(vmem,) * (len(out_shape) - 1) + (scalar,) if smem_out else (vmem,) * len(out_shape) if many else vmem,
        in_specs=specs,
        scratch_shapes=[*scratch, *([pltpu.SemaphoreType.DMA((sems,))] if sems else [])],
        cost_estimate=pl.CostEstimate(flops=flops, transcendentals=0, bytes_accessed=0),
        compiler_params=pltpu.CompilerParams(vmem_limit_bytes=20 << 20),
    )(*operands)


def copies(sources, targets, sem):
    return [pltpu.make_async_copy(a, b, sem.at[i]) for i, (a, b) in enumerate(zip(sources, targets))]


def in_hbm(*arrays):
    return [pltpu.with_memory_space_constraint(a, pltpu.HBM) for a in arrays]


def iota(shape, axis):
    return lax.broadcasted_iota(jnp.int32, shape, axis)


def ones_where(mask):
    return jnp.where(mask, 1.0, 0.0).astype(BF16)


def dot(a, b):
    return jnp.dot(a, b, preferred_element_type=F32)


def dot_nt(a, b):
    return lax.dot_general(a, b, NT, preferred_element_type=F32)


def column(row):
    return jnp.broadcast_to(row, (128, 128)).T


def lookup(at, row):
    lanes = iota((at.shape[0], row.shape[1]), 1).astype(F32)
    return jnp.sum(jnp.where(lanes == at, row.astype(F32), 0.0), axis=1, keepdims=True)


def request_kernel(user_ref, zero_ref, one_ref, dense_ref, owner_hbm, row_hbm, table_hbm, first_hbm, second_hbm,
                   req_ref, slot_ref, spot_ref, table_ref, owner_ref, row_ref, first_ref, second_ref, sem):
    moves = copies((owner_hbm, row_hbm, first_hbm, second_hbm, table_hbm),
                   (owner_ref, row_ref, first_ref, second_ref, table_ref), sem)
    for move in moves:
        move.start()
    shards = req_ref.shape[0]
    cands = owner_ref.shape[1]
    final = second_ref.shape[1]
    slots = 2 * cands // shards
    base = (user_ref[0] % (128 // slots)) * slots
    for move in moves[:4]:
        move.wait()

    @pl.when(dense_ref[0] == 1)
    def _():
        earlier = ones_where((iota((128, 256), 0) < iota((128, 256), 1)) | (iota((128, 256), 1) >= 128))
        seen = jnp.zeros((shards, 128), F32)
        ranks = []
        owner = owner_ref[...]
        hits = owner == iota((shards, cands), 0)
        hot = ones_where(hits)
        for b in range(cands // 128):
            part = slice(b * 128, b * 128 + 128)
            counts = dot(hot[:, part], earlier)
            ranks.append(jnp.sum(jnp.where(hits[:, part], counts[:, :128] + seen, 0.0), axis=0, keepdims=True))
            seen = seen + counts[:, 128:]
        rank = jnp.concatenate(ranks, axis=1).astype(jnp.int32)
        slot_ref[...] = owner * slots + rank
        row = row_ref[...]
        at_slot = rank + base == iota((128, cands), 0)
        high = jnp.where(at_slot, (row >> 4).astype(F32), 0.0).astype(BF16)
        low = jnp.where(at_slot, (row & 15).astype(F32), 0.0).astype(BF16)
        req_ref[...] = (dot_nt(hot, high) * 16.0 + dot_nt(hot, low)).astype(jnp.int32)

    @pl.when(zero_ref[0] + one_ref[0] > 0)
    def _():
        second = jnp.concatenate([second_ref[...], jnp.zeros((1, 128 - final), jnp.int32)], axis=1)
        second = column(second.astype(F32))[:final, :1]
        single = lookup(second, first_ref[...])
        fours = [second * 4.0 + float(f) for f in range(4)]
        none = jnp.full((final, 1), -1.0, F32)
        at = jnp.concatenate(
            [jnp.where(zero_ref[0] == 1, single if f == 0 else none, fours[f]) for f in range(4)], axis=0)
        owner = lookup(at, owner_ref[...] + 1) - 1.0
        row = lookup(at, row_ref[...]).astype(jnp.int32)
        count = at.shape[0]
        lanes = iota((count, 128), 1).astype(F32)
        hot = jnp.where(owner == lanes, 1.0, 0.0)
        before = ones_where(iota((count, count), 1) < iota((count, count), 0))
        rank = jnp.sum(hot * dot(before, hot.astype(BF16)), axis=1, keepdims=True)
        spot_ref[...] = jnp.broadcast_to(owner * slots + rank, spot_ref.shape).astype(jnp.int32)
        at_slot = rank + base.astype(F32) == lanes
        high = jnp.where(at_slot, (row >> 4).astype(F32), 0.0).astype(BF16)
        low = jnp.where(at_slot, (row & 15).astype(F32), 0.0).astype(BF16)
        turned = hot.T.astype(BF16)
        mine = (iota((1, 128), 1) >= base) & (iota((1, 128), 1) < base + slots)
        over = jnp.max(rank, axis=0, keepdims=True) >= slots // 2
        mark = jnp.where(mine & over, MARK, 0)
        req_ref[...] = (dot(turned, high) * 16.0 + dot(turned, low)).astype(jnp.int32) + mark

    moves[4].wait()


def halves(table):
    half = table.shape[0] // 2
    return jnp.concatenate([table[:half, :], table[half:, :]], axis=1)


def picked(col, wide):
    half, width = wide.shape[0], wide.shape[1] // 2
    fine = ones_where((col & 127) == iota(col.shape, 1))
    coarse = ((col & (half - 1)) >> 7).astype(F32).astype(BF16)
    hot = [jnp.where(coarse == float(r), fine, jnp.zeros_like(fine)) for r in range(half // 128)]
    both = dot(jnp.concatenate(hot, axis=1), wide)
    return jnp.where(col < half, both[:, :width], both[:, width:]).astype(BF16)


def served_rows(ids_ref, table_ref, out_ref, keep):
    users = ids_ref.shape[0]
    slots = out_ref.shape[0] // users * 16 // keep
    group = 128 // slots
    wide = halves(table_ref[...])
    count = group * keep
    step = 512 // count
    for first in range(0, users // group, step):
        cols = []
        for b in range(first, first + step):
            ids = jnp.sum(ids_ref[b * group:(b + 1) * group, :], axis=0, keepdims=True)
            col = column(ids & (MARK - 1))
            cols += [col[i * slots:i * slots + keep, :] for i in range(group)] if keep < slots else [col]
        out_ref[first * count:(first + step) * count, :] = picked(jnp.concatenate(cols, axis=0), wide)


def serve_kernel(ids_ref, table_ref, out_ref):
    served_rows(ids_ref, table_ref, out_ref, 16)


def serve_zero_kernel(weight_hbm, proj_hbm, into_hbm, out_of_hbm, ids_ref, table_ref, dense_ref, head_ref,
                      out_ref, vec_ref, into_ref, out_of_ref, over_ref, weight_ref, proj_ref, sem):
    moves = copies((weight_hbm, proj_hbm, into_hbm, out_of_hbm), (weight_ref, proj_ref, into_ref, out_of_ref), sem)
    for move in moves:
        move.start()
    over_ref[0] = jnp.max(ids_ref[...])
    served_rows(ids_ref, table_ref, out_ref, 8)
    for move in moves:
        move.wait()
    active = jax.nn.relu(dot(dense_ref[...], weight_ref[...]))
    query = (active * head_ref[...]).astype(BF16)
    vec_ref[...] = dot(query, proj_ref[...])


def serve_one_kernel(weight_hbm, item_hbm, ids_ref, table_ref, out_ref, weight_ref, item_ref, over_ref, sem):
    moves = copies((weight_hbm, item_hbm), (weight_ref, item_ref), sem)
    for move in moves:
        move.start()
    over_ref[0] = jnp.max(ids_ref[...])
    served_rows(ids_ref, table_ref, out_ref, 8)
    for move in moves:
        move.wait()


def nothing_kernel(*refs):
    pass


def copy_kernel(*refs):
    half = len(refs) // 2
    for from_ref, to_ref in zip(refs[:half], refs[half:]):
        to_ref[...] = from_ref[...]


def as_row(col, lanes):
    n = col.shape[0]
    return jnp.sum(jnp.where(iota((n, lanes), 0) == iota((n, lanes), 1), col, 0.0), axis=0, keepdims=True)


def survivors(spot, rows):
    slots = rows.shape[0] // 128
    return picked((spot >> 4) * slots + (spot & 15), halves(rows))


def tower_kernel(spot_ref, rows_ref, vec_ref, into_ref, out_of_ref, packet_ref, score_ref):
    n = packet_ref.shape[0] // 2
    embed = survivors(spot_ref[:n, :], rows_ref[...])
    hidden = jax.nn.relu(dot(embed, into_ref[...])).astype(BF16)
    tower = dot(hidden, out_of_ref[...]).astype(BF16)
    logit = jnp.sum(tower.astype(F32) * vec_ref[...], axis=1, keepdims=True)
    packet_ref[:n, :] = tower
    packet_ref[n:, :] = jnp.broadcast_to(logit, (n, 128)).astype(BF16)
    score_ref[...] = as_row(logit, n)


def features_kernel(feat_hbm, spot_ref, rows_ref, part_ref, feat_ref, sem):
    move = pltpu.make_async_copy(feat_hbm, feat_ref, sem.at[0])
    move.start()
    n = part_ref.shape[0]
    embed = survivors(spot_ref[:4 * n, :], rows_ref[...])
    tall = jnp.concatenate([embed[f * n:(f + 1) * n, :] for f in range(4)], axis=1)
    move.wait()
    part_ref[...] = dot(tall, feat_ref[...])


def gram_kernel(sec_ref, weight_hbm, slot_ref, rows_ref, head_ref, part_ref, weight_ref, sem):
    @pl.when(sec_ref[0] >= 2)
    def _():
        n = part_ref.shape[0] - 8
        cands = slot_ref.shape[1]
        width = rows_ref.shape[1]
        move = pltpu.make_async_copy(weight_hbm, weight_ref, sem.at[0])
        move.start()
        wide = halves(rows_ref[...])
        embed = [
            picked(jnp.concatenate([column(slot_ref[:, b:b + 128]) for b in range(h, h + 512, 128)], axis=0), wide)
            for h in range(0, cands, 512)
        ]
        r, c = iota((128, 128), 0), iota((128, 128), 1)
        same_item = (r // 32) == (c // 32)
        spread = ones_where((r % 32) == (c % 32))
        own_lanes = (r % 4) == (c // 32)
        grams = []
        for b in range(cands // 128):
            block = embed[b // 4][b % 4 * 128:b % 4 * 128 + 128, :]
            gram = dot_nt(block, block) * (1.0 / math.sqrt(width))
            gram = jnp.where(same_item, gram, 0.0).astype(BF16)
            grams.append(jnp.where(own_lanes, dot(gram, spread), 0.0).astype(BF16))
        tall = jnp.concatenate(grams, axis=0)
        i, k = iota((8 * n, 32 * n), 0), iota((8 * n, 32 * n), 1)
        choose = ones_where(((k // 32) == (i % n)) & (((k % 32) // 4) == (i // n)))
        flat = dot(choose, tall).astype(BF16)
        flat = jnp.concatenate([flat[q * n:(q + 1) * n, :] for q in range(8)], axis=1)
        move.wait()
        part_ref[:n, :] = dot(flat, weight_ref[...])
        part_ref[n:n + 1, :] = head_ref[...]


def prerank_kernel(sec_ref, packet_ref, part_ref, item_ref, weight_ref, head_ref, carry_ref, score_ref):
    @pl.when(sec_ref[0] == 1)
    def _():
        n, hid = part_ref.shape
        pre = part_ref[...] + dot(packet_ref[:n, :], item_ref[...])
        inner = jax.nn.relu(pre).astype(BF16)
        hidden = jax.nn.relu(dot(inner, weight_ref[...]))
        prior = packet_ref[n:, :].astype(F32)[:, :1]
        logit = jnp.sum(hidden * head_ref[...], axis=1, keepdims=True) / math.sqrt(hid) + prior
        carry_ref[:, :hid] = hidden.astype(BF16)
        carry_ref[:, hid:] = jnp.broadcast_to(logit, (n, 128)).astype(BF16)
        score_ref[...] = as_row(logit, n)


def rank(part_ref, carry_ref):
    n, hid = part_ref.shape[0] - 8, part_ref.shape[1]
    carry = carry_ref[...].astype(F32)
    hidden = jax.nn.relu(part_ref[:n, :] + carry[:, :hid])
    logit = jnp.sum(hidden * part_ref[n:n + 1, :], axis=1, keepdims=True) / math.sqrt(hid)
    return hidden, logit + carry[:, hid:hid + 1]


def rank_kernel(sec_ref, near_ref, part_ref, carry_ref, score_ref):
    @pl.when(sec_ref[0] == 2)
    def _():
        n, hid = part_ref.shape[0] - 8, part_ref.shape[1]
        hidden, logit = rank(part_ref, near_ref)
        carry_ref[:, :hid] = hidden.astype(BF16)
        carry_ref[:, hid:] = jnp.broadcast_to(logit, (n, 128)).astype(BF16)
        score_ref[...] = as_row(logit, n)


def final_kernel(sec_ref, last_ref, part_ref, score0_ref, score1_ref, score2_ref, score_ref):
    sec = sec_ref[0]

    for s, from_ref in enumerate((score0_ref, score1_ref, score2_ref)):
        @pl.when(sec == s)
        def _():
            score_ref[...] = from_ref[...]

    @pl.when(sec == 3)
    def _():
        _, logit = rank(part_ref, last_ref)
        score_ref[...] = as_row(logit, logit.shape[0])


def cascade(
    user_dense,
    tables,
    feat_owner,
    feat_row,
    keep_first,
    keep_second,
    section_weight,
    section_head,
    user_proj,
    item_in,
    item_out,
    prerank_feat,
    prerank_item,
):
    shape = pltpu.VMEM
    shards = lax.axis_size("shard")
    cands = feat_row.shape[2]
    slots = 2 * cands // shards
    spots = shards * slots
    width = tables.shape[2]
    hid = section_weight.shape[1]
    final = keep_second.shape[1]
    sec = lax.axis_index("section").reshape(1).astype(jnp.int32)
    user = lax.axis_index("shard").reshape(1).astype(jnp.int32)
    turns = [sec[0] == 0, sec[0] == 1, sec[0] >= 2]
    like = lambda a: shape(a.shape, a.dtype)

    weight, feat, item, into, out_of, proj = in_hbm(
        section_weight[0], prerank_feat, prerank_item, item_in, item_out, user_proj)

    request, slot, spot, table = call(
        request_kernel,
        (shape((shards, 128), jnp.int32), shape((1, cands), jnp.int32), shape((128, 128), jnp.int32), like(tables[0])),
        user, *(turn.astype(jnp.int32).reshape(1) for turn in turns),
        *in_hbm(feat_owner.reshape(1, cands), feat_row.reshape(1, cands), tables[0], keep_first, keep_second),
        smem=4, hbm=5, sems=5, flops=10**8,
        scratch=[pltpu.VMEM(s, jnp.int32) for s in ((1, cands), (1, cands), keep_first.shape, keep_second.shape)],
    )
    asked = lax.all_to_all(request.reshape(shards, 1, 128), "shard", 0, 0, tiled=True).reshape(shards, 128)

    def exchanged(served):
        rows = lax.all_to_all(served.reshape(shards, -1, width), "shard", 0, 0, tiled=True)
        return rows.reshape(-1, width)

    def serve():
        return call(serve_kernel, shape((spots, width), BF16), asked, table, flops=10**9)

    def blank(*shapes):
        return pl.pallas_call(
            nothing_kernel,
            out_shape=shapes,
            in_specs=[pl.BlockSpec(memory_space=pl.ANY)],
            out_specs=(pl.BlockSpec(memory_space=pltpu.VMEM),) * len(shapes),
            compiler_params=pltpu.CompilerParams(vmem_limit_bytes=1 << 20),
        )(asked)

    scored = shape((1, final), F32)
    carried = shape((final, hid + 128), BF16)

    def either(over, served, then):
        return lax.cond(over[0] >= MARK, lambda: then(exchanged(serve())), lambda: then(exchanged(served)))

    def kept(*arrays):
        return tuple(call(copy_kernel, tuple(like(a) for a in arrays), *arrays))

    short = shape((spots // 2, width), BF16)
    scalar = jax.ShapeDtypeStruct((1,), jnp.int32)
    packed = shape((2 * final, width), BF16)
    product = shape((final, hid), F32)

    def section_zero():
        served, query, into_near, out_of_near, over = call(
            serve_zero_kernel,
            (short, shape((1, width), F32), like(into), like(out_of), scalar),
            weight, proj, into, out_of, asked, table, user_dense, section_head,
            hbm=4, sems=4, flops=10**9, smem_out=True,
            scratch=[pltpu.VMEM(weight.shape, BF16), pltpu.VMEM(proj.shape, BF16)],
        )
        return kept(*either(over, served, lambda rows: tuple(call(
            tower_kernel, (packed, scored), spot, rows, query, into_near, out_of_near, flops=10**7))))

    def section_one():
        served, weight_near, item_near, over = call(
            serve_one_kernel,
            (short, like(weight), like(item), scalar),
            weight, item, asked, table,
            hbm=2, sems=2, flops=10**9, smem_out=True,
        )
        product_near = either(over, served, lambda rows: call(
            features_kernel, product, feat, spot, rows,
            hbm=1, sems=1, scratch=[pltpu.VMEM(feat.shape, BF16)], flops=10**8))
        return *kept(product_near), weight_near, item_near

    def dense_sections():
        return call(
            gram_kernel,
            shape((final + 8, hid), F32),
            sec, weight, slot, exchanged(serve()), section_head,
            smem=1, hbm=1, sems=1, scratch=[pltpu.VMEM(weight.shape, BF16)], flops=10**9,
        )

    packet, score0 = lax.cond(turns[0], section_zero, lambda: tuple(blank(packed, scored)))
    packet = lax.ppermute(packet, "section", [(0, 1)])
    pre, weight_near, item_near = lax.cond(
        turns[1], section_one, lambda: tuple(blank(product, like(weight), like(item))))
    carry, score1 = call(
        prerank_kernel,
        (carried, scored),
        sec, packet, pre, item_near, weight_near, section_head,
        smem=1, flops=10**8,
    )
    near = lax.ppermute(carry, "section", [(1, 2)])
    part = lax.cond(turns[2], dense_sections, lambda: blank(shape((final + 8, hid), F32))[0])
    carry, score2 = call(rank_kernel, (carried, scored), sec, near, part, smem=1, flops=10**6)
    last = lax.ppermute(carry, "section", [(2, 3)])
    scores = call(
        final_kernel,
        jax.ShapeDtypeStruct((1, final), F32),
        sec, last, part, score0, score1, score2,
        smem=1, flops=10**6,
    )
    return scores[None]


def solution(mesh):
    placed = (
        P("shard", None),
        P("section", "shard", None),
        P("section", "shard", None, None),
        P("section", "shard", None),
        P("shard", None),
        P("shard", None),
        P("section", None, None),
        P("section", None),
        P(),
        P(),
        P(),
        P(),
        P(),
    )
    return jax.shard_map(
        cascade,
        mesh=mesh,
        in_specs=placed,
        out_specs=P("section", "shard", None),
        check_vma=False,
    )
```

```python
import math

import jax
import jax.numpy as jnp
from jax import lax
from jax.experimental import pallas as pl
from jax.experimental.pallas import tpu as pltpu
from jax.sharding import PartitionSpec as P


F32 = jnp.float32
BF16 = jnp.bfloat16
NT = (((1,), (1,)), ((), ()))
MARK = 1 << 14


def call(kernel, out_shape, *operands, smem=0, hbm=0, sems=0, flops=0, scratch=(), smem_out=False):
    specs = [pl.BlockSpec(memory_space=pltpu.SMEM)] * smem
    specs += [pl.BlockSpec(memory_space=pltpu.HBM)] * hbm
    specs += [pl.BlockSpec(memory_space=pltpu.VMEM)] * (len(operands) - smem - hbm)
    vmem, scalar = pl.BlockSpec(memory_space=pltpu.VMEM), pl.BlockSpec(memory_space=pltpu.SMEM)
    many = isinstance(out_shape, (tuple, list))
    return pl.pallas_call(
        kernel,
        out_shape=out_shape,
        out_specs=(vmem,) * (len(out_shape) - 1) + (scalar,) if smem_out else (vmem,) * len(out_shape) if many else vmem,
        in_specs=specs,
        scratch_shapes=[*scratch, *([pltpu.SemaphoreType.DMA((sems,))] if sems else [])],
        cost_estimate=pl.CostEstimate(flops=flops, transcendentals=0, bytes_accessed=0),
        compiler_params=pltpu.CompilerParams(vmem_limit_bytes=20 << 20),
    )(*operands)


def copies(sources, targets, sem):
    return [pltpu.make_async_copy(a, b, sem.at[i]) for i, (a, b) in enumerate(zip(sources, targets))]


def in_hbm(*arrays):
    return [pltpu.with_memory_space_constraint(a, pltpu.HBM) for a in arrays]


def iota(shape, axis):
    return lax.broadcasted_iota(jnp.int32, shape, axis)


def ones_where(mask):
    return jnp.where(mask, 1.0, 0.0).astype(BF16)


def dot(a, b):
    return jnp.dot(a, b, preferred_element_type=F32)


def dot_nt(a, b):
    return lax.dot_general(a, b, NT, preferred_element_type=F32)


def column(row):
    return jnp.broadcast_to(row, (128, 128)).T


def lookup(at, row):
    lanes = iota((at.shape[0], row.shape[1]), 1).astype(F32)
    return jnp.sum(jnp.where(lanes == at, row.astype(F32), 0.0), axis=1, keepdims=True)


def request_kernel(user_ref, zero_ref, one_ref, dense_ref, owner_hbm, row_hbm, table_hbm, first_hbm, second_hbm, head_hbm,
                   weight_hbm, req_ref, slot_ref, spot_ref, table_ref, head_ref,
                   owner_ref, row_ref, first_ref, second_ref, sem):
    moves = copies((owner_hbm, row_hbm, first_hbm, second_hbm, table_hbm, head_hbm),
                   (owner_ref, row_ref, first_ref, second_ref, table_ref, head_ref), sem)
    for move in moves:
        move.start()
    shards = req_ref.shape[0]
    cands = owner_ref.shape[1]
    final = second_ref.shape[1]
    slots = 2 * cands // shards
    base = (user_ref[0] % (128 // slots)) * slots
    for move in moves[:4]:
        move.wait()

    @pl.when(dense_ref[0] == 1)
    def _():
        earlier = ones_where((iota((128, 256), 0) < iota((128, 256), 1)) | (iota((128, 256), 1) >= 128))
        seen = jnp.zeros((shards, 128), F32)
        ranks = []
        owner = owner_ref[...]
        hits = owner == iota((shards, cands), 0)
        hot = ones_where(hits)
        for b in range(cands // 128):
            part = slice(b * 128, b * 128 + 128)
            counts = dot(hot[:, part], earlier)
            ranks.append(jnp.sum(jnp.where(hits[:, part], counts[:, :128] + seen, 0.0), axis=0, keepdims=True))
            seen = seen + counts[:, 128:]
        rank = jnp.concatenate(ranks, axis=1).astype(jnp.int32)
        slot_ref[...] = owner * slots + rank
        row = row_ref[...]
        at_slot = rank + base == iota((128, cands), 0)
        high = jnp.where(at_slot, (row >> 4).astype(F32), 0.0).astype(BF16)
        low = jnp.where(at_slot, (row & 15).astype(F32), 0.0).astype(BF16)
        req_ref[...] = (dot_nt(hot, high) * 16.0 + dot_nt(hot, low)).astype(jnp.int32)

    @pl.when(zero_ref[0] + one_ref[0] > 0)
    def _():
        second = jnp.concatenate([second_ref[...], jnp.zeros((1, 128 - final), jnp.int32)], axis=1)
        second = column(second.astype(F32))[:final, :1]
        single = lookup(second, first_ref[...])
        fours = [second * 4.0 + float(f) for f in range(4)]
        none = jnp.full((final, 1), -1.0, F32)
        at = jnp.concatenate(
            [jnp.where(zero_ref[0] == 1, single if f == 0 else none, fours[f]) for f in range(4)], axis=0)
        owner = lookup(at, owner_ref[...] + 1) - 1.0
        row = lookup(at, row_ref[...]).astype(jnp.int32)
        count = at.shape[0]
        lanes = iota((count, 128), 1).astype(F32)
        hot = jnp.where(owner == lanes, 1.0, 0.0)
        before = ones_where(iota((count, count), 1) < iota((count, count), 0))
        rank = jnp.sum(hot * dot(before, hot.astype(BF16)), axis=1, keepdims=True)
        spot_ref[...] = jnp.broadcast_to(owner * slots + rank, spot_ref.shape).astype(jnp.int32)
        at_slot = rank + base.astype(F32) == lanes
        high = jnp.where(at_slot, (row >> 4).astype(F32), 0.0).astype(BF16)
        low = jnp.where(at_slot, (row & 15).astype(F32), 0.0).astype(BF16)
        turned = hot.T.astype(BF16)
        mine = (iota((1, 128), 1) >= base) & (iota((1, 128), 1) < base + slots)
        over = jnp.max(rank, axis=0, keepdims=True) >= slots // 2
        mark = jnp.where(mine & over, MARK, 0)
        req_ref[...] = (dot(turned, high) * 16.0 + dot(turned, low)).astype(jnp.int32) + mark

    for move in moves[4:]:
        move.wait()


def halves(table):
    half = table.shape[0] // 2
    return jnp.concatenate([table[:half, :], table[half:, :]], axis=1)


def picked(col, wide):
    half, width = wide.shape[0], wide.shape[1] // 2
    fine = ones_where((col & 127) == iota(col.shape, 1))
    coarse = ((col & (half - 1)) >> 7).astype(F32).astype(BF16)
    hot = [jnp.where(coarse == float(r), fine, jnp.zeros_like(fine)) for r in range(half // 128)]
    both = dot(jnp.concatenate(hot, axis=1), wide)
    return jnp.where(col < half, both[:, :width], both[:, width:]).astype(BF16)


def served_rows(ids_ref, table_ref, out_ref, keep):
    users = ids_ref.shape[0]
    slots = out_ref.shape[0] // users * 16 // keep
    group = 128 // slots
    wide = halves(table_ref[...])
    count = group * keep
    step = 512 // count
    for first in range(0, users // group, step):
        cols = []
        for b in range(first, first + step):
            ids = jnp.sum(ids_ref[b * group:(b + 1) * group, :], axis=0, keepdims=True)
            col = column(ids & (MARK - 1))
            cols += [col[i * slots:i * slots + keep, :] for i in range(group)] if keep < slots else [col]
        out_ref[first * count:(first + step) * count, :] = picked(jnp.concatenate(cols, axis=0), wide)


def serve_kernel(ids_ref, table_ref, out_ref):
    served_rows(ids_ref, table_ref, out_ref, 16)


def serve_zero_kernel(proj_hbm, into_hbm, out_of_hbm, ids_ref, table_ref, dense_ref, head_ref, weight_ref,
                      out_ref, vec_ref, into_ref, out_of_ref, over_ref, proj_ref, sem):
    moves = copies((proj_hbm, into_hbm, out_of_hbm), (proj_ref, into_ref, out_of_ref), sem)
    for move in moves:
        move.start()
    over_ref[0] = jnp.max(ids_ref[...])
    served_rows(ids_ref, table_ref, out_ref, 8)
    for move in moves:
        move.wait()
    active = jax.nn.relu(dot(dense_ref[...], weight_ref[...]))
    query = (active * head_ref[...]).astype(BF16)
    vec_ref[...] = dot(query, proj_ref[...])


def serve_one_kernel(item_hbm, ids_ref, table_ref, out_ref, item_ref, over_ref, sem):
    move = pltpu.make_async_copy(item_hbm, item_ref, sem.at[0])
    move.start()
    over_ref[0] = jnp.max(ids_ref[...])
    served_rows(ids_ref, table_ref, out_ref, 8)
    move.wait()


def nothing_kernel(*refs):
    pass


def copy_kernel(*refs):
    half = len(refs) // 2
    for from_ref, to_ref in zip(refs[:half], refs[half:]):
        to_ref[...] = from_ref[...]


def as_row(col, lanes):
    n = col.shape[0]
    return jnp.sum(jnp.where(iota((n, lanes), 0) == iota((n, lanes), 1), col, 0.0), axis=0, keepdims=True)


def survivors(spot, rows):
    slots = rows.shape[0] // 128
    return picked((spot >> 4) * slots + (spot & 15), halves(rows))


def tower_kernel(spot_ref, rows_ref, vec_ref, into_ref, out_of_ref, packet_ref, score_ref):
    n = packet_ref.shape[0] // 2
    embed = survivors(spot_ref[:n, :], rows_ref[...])
    hidden = jax.nn.relu(dot(embed, into_ref[...])).astype(BF16)
    tower = dot(hidden, out_of_ref[...]).astype(BF16)
    logit = jnp.sum(tower.astype(F32) * vec_ref[...], axis=1, keepdims=True)
    packet_ref[:n, :] = tower
    packet_ref[n:, :] = jnp.broadcast_to(logit, (n, 128)).astype(BF16)
    score_ref[...] = as_row(logit, n)


def features_kernel(feat_hbm, spot_ref, rows_ref, part_ref, feat_ref, sem):
    move = pltpu.make_async_copy(feat_hbm, feat_ref, sem.at[0])
    move.start()
    n = part_ref.shape[0]
    embed = survivors(spot_ref[:4 * n, :], rows_ref[...])
    tall = jnp.concatenate([embed[f * n:(f + 1) * n, :] for f in range(4)], axis=1)
    move.wait()
    part_ref[...] = dot(tall, feat_ref[...])


def gram_kernel(slot_ref, rows_ref, head_ref, weight_ref, part_ref):
    n = part_ref.shape[0] - 8
    cands = slot_ref.shape[1]
    width = rows_ref.shape[1]
    wide = halves(rows_ref[...])
    embed = [
        picked(jnp.concatenate([column(slot_ref[:, b:b + 128]) for b in range(h, h + 512, 128)], axis=0), wide)
        for h in range(0, cands, 512)
    ]
    r, c = iota((128, 128), 0), iota((128, 128), 1)
    same_item = (r // 32) == (c // 32)
    spread = ones_where((r % 32) == (c % 32))
    own_lanes = (r % 4) == (c // 32)
    grams = []
    for b in range(cands // 128):
        block = embed[b // 4][b % 4 * 128:b % 4 * 128 + 128, :]
        gram = dot_nt(block, block) * (1.0 / math.sqrt(width))
        gram = jnp.where(same_item, gram, 0.0).astype(BF16)
        grams.append(jnp.where(own_lanes, dot(gram, spread), 0.0).astype(BF16))
    tall = jnp.concatenate(grams, axis=0)
    i, k = iota((8 * n, 32 * n), 0), iota((8 * n, 32 * n), 1)
    choose = ones_where(((k // 32) == (i % n)) & (((k % 32) // 4) == (i // n)))
    flat = dot(choose, tall).astype(BF16)
    flat = jnp.concatenate([flat[q * n:(q + 1) * n, :] for q in range(8)], axis=1)
    part_ref[:n, :] = dot(flat, weight_ref[...])
    part_ref[n:n + 1, :] = head_ref[...]


def prerank_kernel(sec_ref, packet_ref, part_ref, item_ref, weight_ref, head_ref, carry_ref, score_ref):
    @pl.when(sec_ref[0] == 1)
    def _():
        n, hid = part_ref.shape
        pre = part_ref[...] + dot(packet_ref[:n, :], item_ref[...])
        inner = jax.nn.relu(pre).astype(BF16)
        hidden = jax.nn.relu(dot(inner, weight_ref[...]))
        prior = packet_ref[n:, :].astype(F32)[:, :1]
        logit = jnp.sum(hidden * head_ref[...], axis=1, keepdims=True) / math.sqrt(hid) + prior
        carry_ref[:, :hid] = hidden.astype(BF16)
        carry_ref[:, hid:] = jnp.broadcast_to(logit, (n, 128)).astype(BF16)
        score_ref[...] = as_row(logit, n)


def rank(part_ref, carry_ref):
    n, hid = part_ref.shape[0] - 8, part_ref.shape[1]
    carry = carry_ref[...].astype(F32)
    hidden = jax.nn.relu(part_ref[:n, :] + carry[:, :hid])
    logit = jnp.sum(hidden * part_ref[n:n + 1, :], axis=1, keepdims=True) / math.sqrt(hid)
    return hidden, logit + carry[:, hid:hid + 1]


def rank_kernel(sec_ref, near_ref, part_ref, carry_ref, score_ref):
    @pl.when(sec_ref[0] == 2)
    def _():
        n, hid = part_ref.shape[0] - 8, part_ref.shape[1]
        hidden, logit = rank(part_ref, near_ref)
        carry_ref[:, :hid] = hidden.astype(BF16)
        carry_ref[:, hid:] = jnp.broadcast_to(logit, (n, 128)).astype(BF16)
        score_ref[...] = as_row(logit, n)


def final_kernel(sec_ref, last_ref, part_ref, score0_ref, score1_ref, score2_ref, score_ref):
    sec = sec_ref[0]

    for s, from_ref in enumerate((score0_ref, score1_ref, score2_ref)):
        @pl.when(sec == s)
        def _():
            score_ref[...] = from_ref[...]

    @pl.when(sec == 3)
    def _():
        _, logit = rank(part_ref, last_ref)
        score_ref[...] = as_row(logit, logit.shape[0])


def cascade(
    user_dense,
    tables,
    feat_owner,
    feat_row,
    keep_first,
    keep_second,
    section_weight,
    section_head,
    user_proj,
    item_in,
    item_out,
    prerank_feat,
    prerank_item,
):
    shape = pltpu.VMEM
    shards = lax.axis_size("shard")
    cands = feat_row.shape[2]
    slots = 2 * cands // shards
    spots = shards * slots
    width = tables.shape[2]
    hid = section_weight.shape[1]
    final = keep_second.shape[1]
    sec = lax.axis_index("section").reshape(1).astype(jnp.int32)
    user = lax.axis_index("shard").reshape(1).astype(jnp.int32)
    turns = [sec[0] == 0, sec[0] == 1, sec[0] >= 2]
    like = lambda a: shape(a.shape, a.dtype)

    feat, item, into, out_of, proj = in_hbm(prerank_feat, prerank_item, item_in, item_out, user_proj)
    weight = section_weight[0]

    def weight_near():
        return pltpu.with_memory_space_constraint(weight, pltpu.VMEM)


    request, slot, spot, table, head = call(
        request_kernel,
        (shape((shards, 128), jnp.int32), shape((1, cands), jnp.int32), shape((128, 128), jnp.int32), like(tables[0]),
         like(section_head)),
        user, *(turn.astype(jnp.int32).reshape(1) for turn in turns),
        *in_hbm(feat_owner.reshape(1, cands), feat_row.reshape(1, cands), tables[0], keep_first, keep_second, section_head,
                section_weight[0]),
        smem=4, hbm=7, sems=6, flops=10**8,
        scratch=[pltpu.VMEM(s, jnp.int32) for s in ((1, cands), (1, cands), keep_first.shape, keep_second.shape)],
    )
    asked = lax.all_to_all(request.reshape(shards, 1, 128), "shard", 0, 0, tiled=True).reshape(shards, 128)

    def exchanged(served):
        rows = lax.all_to_all(served.reshape(shards, -1, width), "shard", 0, 0, tiled=True)
        return rows.reshape(-1, width)

    def serve():
        return call(serve_kernel, shape((spots, width), BF16), asked, table, flops=10**9)

    def blank(*shapes):
        return pl.pallas_call(
            nothing_kernel,
            out_shape=shapes,
            in_specs=[pl.BlockSpec(memory_space=pl.ANY)],
            out_specs=(pl.BlockSpec(memory_space=pltpu.VMEM),) * len(shapes),
            compiler_params=pltpu.CompilerParams(vmem_limit_bytes=1 << 20),
        )(asked)

    scored = shape((1, final), F32)
    carried = shape((final, hid + 128), BF16)

    def either(over, served, then):
        return lax.cond(over[0] >= MARK, lambda: then(exchanged(serve())), lambda: then(exchanged(served)))

    def kept(*arrays):
        return tuple(call(copy_kernel, tuple(like(a) for a in arrays), *arrays))

    short = shape((spots // 2, width), BF16)
    scalar = pltpu.SMEM((1,), jnp.int32)
    packed = shape((2 * final, width), BF16)
    product = shape((final, hid), F32)

    def section_zero():
        served, query, into_near, out_of_near, over = call(
            serve_zero_kernel,
            (short, shape((1, width), F32), like(into), like(out_of), scalar),
            proj, into, out_of, asked, table, user_dense, head, weight_near(),
            hbm=3, sems=3, flops=10**9, smem_out=True,
            scratch=[pltpu.VMEM(proj.shape, BF16)],
        )
        return kept(*either(over, served, lambda rows: tuple(call(
            tower_kernel, (packed, scored), spot, rows, query, into_near, out_of_near, flops=10**7))))

    def section_one():
        served, item_near, over = call(
            serve_one_kernel,
            (short, like(item), scalar),
            item, asked, table,
            hbm=1, sems=1, flops=10**9, smem_out=True,
        )
        product_near = either(over, served, lambda rows: call(
            features_kernel, product, feat, spot, rows,
            hbm=1, sems=1, scratch=[pltpu.VMEM(feat.shape, BF16)], flops=10**8))
        return *kept(product_near), item_near

    def dense_sections():
        return call(
            gram_kernel, shape((final + 8, hid), F32), slot, exchanged(serve()), head, weight_near(), flops=10**9)

    def sparse_sections():
        packet, score0 = lax.cond(turns[0], section_zero, lambda: tuple(blank(packed, scored)))
        packet = lax.ppermute(packet, "section", [(0, 1)])
        pre, item_near = lax.cond(turns[1], section_one, lambda: tuple(blank(product, like(item))))
        return *call(
            prerank_kernel,
            (carried, scored),
            sec, packet, pre, item_near, weight_near(), head,
            smem=1, flops=10**8,
        ), score0

    carry, score1, score0 = lax.cond(turns[2], lambda: tuple(blank(carried, scored, scored)), sparse_sections)
    near = lax.ppermute(carry, "section", [(1, 2)])
    part = lax.cond(turns[2], dense_sections, lambda: blank(shape((final + 8, hid), F32))[0])
    carry, score2 = call(rank_kernel, (carried, scored), sec, near, part, smem=1, flops=10**6)
    last = lax.ppermute(carry, "section", [(2, 3)])
    scores = call(
        final_kernel,
        jax.ShapeDtypeStruct((1, final), F32),
        sec, last, part, score0, score1, score2,
        smem=1, flops=10**6,
    )
    return scores[None]


def solution(mesh):
    placed = (
        P("shard", None),
        P("section", "shard", None),
        P("section", "shard", None, None),
        P("section", "shard", None),
        P("shard", None),
        P("shard", None),
        P("section", None, None),
        P("section", None),
        P(),
        P(),
        P(),
        P(),
        P(),
    )
    return jax.shard_map(
        cascade,
        mesh=mesh,
        in_specs=placed,
        out_specs=P("section", "shard", None),
        check_vma=False,
    )
```

```python
import math

import jax
import jax.numpy as jnp
from jax import lax
from jax.experimental import pallas as pl
from jax.experimental.pallas import tpu as pltpu
from jax.sharding import PartitionSpec as P


F32 = jnp.float32
BF16 = jnp.bfloat16
NT = (((1,), (1,)), ((), ()))
MARK = 1 << 14


def call(kernel, out_shape, *operands, smem=0, hbm=0, sems=0, flops=0, scratch=(), smem_out=False):
    specs = [pl.BlockSpec(memory_space=pltpu.SMEM)] * smem
    specs += [pl.BlockSpec(memory_space=pltpu.HBM)] * hbm
    specs += [pl.BlockSpec(memory_space=pltpu.VMEM)] * (len(operands) - smem - hbm)
    vmem, scalar = pl.BlockSpec(memory_space=pltpu.VMEM), pl.BlockSpec(memory_space=pltpu.SMEM)
    many = isinstance(out_shape, (tuple, list))
    return pl.pallas_call(
        kernel,
        out_shape=out_shape,
        out_specs=(vmem,) * (len(out_shape) - 1) + (scalar,) if smem_out else (vmem,) * len(out_shape) if many else vmem,
        in_specs=specs,
        scratch_shapes=[*scratch, *([pltpu.SemaphoreType.DMA((sems,))] if sems else [])],
        cost_estimate=pl.CostEstimate(flops=flops, transcendentals=0, bytes_accessed=0),
        compiler_params=pltpu.CompilerParams(vmem_limit_bytes=20 << 20),
    )(*operands)


def copies(sources, targets, sem):
    return [pltpu.make_async_copy(a, b, sem.at[i]) for i, (a, b) in enumerate(zip(sources, targets))]


def in_hbm(*arrays):
    return [pltpu.with_memory_space_constraint(a, pltpu.HBM) for a in arrays]


def iota(shape, axis):
    return lax.broadcasted_iota(jnp.int32, shape, axis)


def ones_where(mask):
    return jnp.where(mask, 1.0, 0.0).astype(BF16)


def dot(a, b):
    return jnp.dot(a, b, preferred_element_type=F32)


def dot_nt(a, b):
    return lax.dot_general(a, b, NT, preferred_element_type=F32)


def column(row):
    return jnp.broadcast_to(row, (128, 128)).T


def lookup(at, row):
    lanes = iota((at.shape[0], row.shape[1]), 1).astype(F32)
    return jnp.sum(jnp.where(lanes == at, row.astype(F32), 0.0), axis=1, keepdims=True)


def request_kernel(user_ref, zero_ref, one_ref, dense_ref, owner_hbm, row_hbm, table_hbm, first_hbm, second_hbm, head_hbm,
                   weight_hbm, req_ref, slot_ref, spot_ref, table_ref, head_ref,
                   owner_ref, row_ref, first_ref, second_ref, sem):
    moves = copies((owner_hbm, row_hbm, first_hbm, second_hbm, table_hbm, head_hbm),
                   (owner_ref, row_ref, first_ref, second_ref, table_ref, head_ref), sem)
    for move in moves:
        move.start()
    shards = req_ref.shape[0]
    cands = owner_ref.shape[1]
    final = second_ref.shape[1]
    slots = 2 * cands // shards
    base = (user_ref[0] % (128 // slots)) * slots

    @pl.when(dense_ref[0] == 1)
    def _():
        moves[0].wait()
        earlier = ones_where((iota((128, 256), 0) < iota((128, 256), 1)) | (iota((128, 256), 1) >= 128))
        seen = jnp.zeros((shards, 128), F32)
        ranks = []
        owner = owner_ref[...]
        hits = owner == iota((shards, cands), 0)
        hot = ones_where(hits)
        for b in range(cands // 128):
            part = slice(b * 128, b * 128 + 128)
            counts = dot(hot[:, part], earlier)
            ranks.append(jnp.sum(jnp.where(hits[:, part], counts[:, :128] + seen, 0.0), axis=0, keepdims=True))
            seen = seen + counts[:, 128:]
        rank = jnp.concatenate(ranks, axis=1).astype(jnp.int32)
        slot_ref[...] = owner * slots + rank
        for move in moves[1:4]:
            move.wait()
        row = row_ref[...]
        at_slot = rank + base == iota((128, cands), 0)
        high = jnp.where(at_slot, (row >> 4).astype(F32), 0.0).astype(BF16)
        low = jnp.where(at_slot, (row & 15).astype(F32), 0.0).astype(BF16)
        both = dot_nt(hot, jnp.concatenate([high, low], axis=0))
        req_ref[...] = (both[:, :128] * 16.0 + both[:, 128:]).astype(jnp.int32)

    @pl.when(zero_ref[0] + one_ref[0] > 0)
    def _():
        for move in moves[:4]:
            move.wait()
        second = jnp.concatenate([second_ref[...], jnp.zeros((1, 128 - final), jnp.int32)], axis=1)
        second = column(second.astype(F32))[:final, :1]
        single = lookup(second, first_ref[...])
        fours = [second * 4.0 + float(f) for f in range(4)]
        none = jnp.full((final, 1), -1.0, F32)
        at = jnp.concatenate(
            [jnp.where(zero_ref[0] == 1, single if f == 0 else none, fours[f]) for f in range(4)], axis=0)
        owner = lookup(at, owner_ref[...] + 1) - 1.0
        row = lookup(at, row_ref[...]).astype(jnp.int32)
        count = at.shape[0]
        lanes = iota((count, 128), 1).astype(F32)
        hot = jnp.where(owner == lanes, 1.0, 0.0)
        before = ones_where(iota((count, count), 1) < iota((count, count), 0))
        rank = jnp.sum(hot * dot(before, hot.astype(BF16)), axis=1, keepdims=True)
        spot_ref[...] = jnp.broadcast_to(owner * slots + rank, spot_ref.shape).astype(jnp.int32)
        at_slot = rank + base.astype(F32) == lanes
        high = jnp.where(at_slot, (row >> 4).astype(F32), 0.0).astype(BF16)
        low = jnp.where(at_slot, (row & 15).astype(F32), 0.0).astype(BF16)
        turned = hot.T.astype(BF16)
        mine = (iota((1, 128), 1) >= base) & (iota((1, 128), 1) < base + slots)
        over = jnp.max(rank, axis=0, keepdims=True) >= slots // 2
        mark = jnp.where(mine & over, MARK, 0)
        both = dot(turned, jnp.concatenate([high, low], axis=1))
        req_ref[...] = (both[:, :128] * 16.0 + both[:, 128:]).astype(jnp.int32) + mark

    for move in moves[4:]:
        move.wait()


def halves(table):
    half = table.shape[0] // 2
    return jnp.concatenate([table[:half, :], table[half:, :]], axis=1)


def picked(col, wide):
    half, width = wide.shape[0], wide.shape[1] // 2
    fine = ones_where((col & 127) == iota(col.shape, 1))
    coarse = ((col & (half - 1)) >> 7).astype(F32).astype(BF16)
    hot = [jnp.where(coarse == float(r), fine, jnp.zeros_like(fine)) for r in range(half // 128)]
    both = dot(jnp.concatenate(hot, axis=1), wide)
    return jnp.where(col < half, both[:, :width], both[:, width:]).astype(BF16)


def served_rows(ids_ref, table_ref, out_ref, keep):
    users = ids_ref.shape[0]
    slots = out_ref.shape[0] // users * 16 // keep
    group = 128 // slots
    wide = halves(table_ref[...])
    count = group * keep
    step = 512 // count
    for first in range(0, users // group, step):
        cols = []
        for b in range(first, first + step):
            ids = jnp.sum(ids_ref[b * group:(b + 1) * group, :], axis=0, keepdims=True)
            col = column(ids & (MARK - 1))
            cols += [col[i * slots:i * slots + keep, :] for i in range(group)] if keep < slots else [col]
        out_ref[first * count:(first + step) * count, :] = picked(jnp.concatenate(cols, axis=0), wide)


def serve_kernel(ids_ref, table_ref, out_ref):
    served_rows(ids_ref, table_ref, out_ref, 16)


def serve_zero_kernel(proj_hbm, into_hbm, out_of_hbm, ids_ref, table_ref, dense_ref, head_ref, weight_ref,
                      out_ref, vec_ref, into_ref, out_of_ref, over_ref, proj_ref, sem):
    moves = copies((proj_hbm, into_hbm, out_of_hbm), (proj_ref, into_ref, out_of_ref), sem)
    for move in moves:
        move.start()
    over_ref[0] = jnp.max(ids_ref[...])
    served_rows(ids_ref, table_ref, out_ref, 8)
    for move in moves:
        move.wait()
    active = jax.nn.relu(dot(dense_ref[...], weight_ref[...]))
    query = (active * head_ref[...]).astype(BF16)
    vec_ref[...] = dot(query, proj_ref[...])


def serve_one_kernel(item_hbm, ids_ref, table_ref, out_ref, item_ref, over_ref, sem):
    move = pltpu.make_async_copy(item_hbm, item_ref, sem.at[0])
    move.start()
    over_ref[0] = jnp.max(ids_ref[...])
    served_rows(ids_ref, table_ref, out_ref, 8)
    move.wait()


def nothing_kernel(*refs):
    pass


def copy_kernel(*refs):
    half = len(refs) // 2
    for from_ref, to_ref in zip(refs[:half], refs[half:]):
        to_ref[...] = from_ref[...]


def as_row(col, lanes):
    n = col.shape[0]
    return jnp.sum(jnp.where(iota((n, lanes), 0) == iota((n, lanes), 1), col, 0.0), axis=0, keepdims=True)


def survivors(spot, rows):
    slots = rows.shape[0] // 128
    return picked((spot >> 4) * slots + (spot & 15), halves(rows))


def tower_kernel(spot_ref, rows_ref, vec_ref, into_ref, out_of_ref, packet_ref, score_ref):
    n = packet_ref.shape[0] // 2
    embed = survivors(spot_ref[:n, :], rows_ref[...])
    hidden = jax.nn.relu(dot(embed, into_ref[...])).astype(BF16)
    tower = dot(hidden, out_of_ref[...]).astype(BF16)
    logit = jnp.sum(tower.astype(F32) * vec_ref[...], axis=1, keepdims=True)
    packet_ref[:n, :] = tower
    packet_ref[n:, :] = jnp.broadcast_to(logit, (n, 128)).astype(BF16)
    score_ref[...] = as_row(logit, n)


def features_kernel(feat_hbm, spot_ref, rows_ref, part_ref, feat_ref, sem):
    move = pltpu.make_async_copy(feat_hbm, feat_ref, sem.at[0])
    move.start()
    n = part_ref.shape[0]
    embed = survivors(spot_ref[:4 * n, :], rows_ref[...])
    tall = jnp.concatenate([embed[f * n:(f + 1) * n, :] for f in range(4)], axis=1)
    move.wait()
    part_ref[...] = dot(tall, feat_ref[...])


def gram_kernel(slot_ref, rows_ref, head_ref, weight_ref, part_ref):
    n = part_ref.shape[0] - 8
    cands = slot_ref.shape[1]
    width = rows_ref.shape[1]
    wide = halves(rows_ref[...])
    embed = [
        picked(jnp.concatenate([column(slot_ref[:, b:b + 128]) for b in range(h, h + 512, 128)], axis=0), wide)
        for h in range(0, cands, 512)
    ]
    own_lanes = (iota((32, 128), 0) % 4) == (iota((32, 128), 1) // 32)
    grams = []
    for b in range(cands // 128):
        block = embed[b // 4][b % 4 * 128:b % 4 * 128 + 128, :]
        items = [block[i * 32:i * 32 + 32, :] for i in range(4)]
        four = []
        for i in (0, 2):
            wide_pair = jnp.concatenate([items[i]] * 4 + [items[i + 1]] * 4, axis=0)
            both = dot_nt(block[i * 32:i * 32 + 64, :], wide_pair) * (1.0 / math.sqrt(width))
            four += [jnp.where(own_lanes, both[:32, :128], 0.0), jnp.where(own_lanes, both[32:, 128:], 0.0)]
        grams.append(jnp.concatenate(four, axis=0).astype(BF16))
    i, k = iota((64, 256), 0), iota((64, 256), 1)
    choose = ones_where(((k // 32) == (i % 8)) & (((k % 32) // 4) == (i // 8)))
    flat = []
    for b in range(0, len(grams), 2):
        eight = dot(choose, jnp.concatenate(grams[b:b + 2], axis=0))
        flat.append(jnp.concatenate([eight[q * 8:q * 8 + 8, :] for q in range(8)], axis=1))
    flat = jnp.concatenate(flat, axis=0).astype(BF16)
    part_ref[:n, :] = dot(flat, weight_ref[...])
    part_ref[n:n + 1, :] = head_ref[...]


def prerank_kernel(sec_ref, packet_ref, part_ref, item_ref, weight_ref, head_ref, carry_ref, score_ref):
    @pl.when(sec_ref[0] == 1)
    def _():
        n, hid = part_ref.shape
        pre = part_ref[...] + dot(packet_ref[:n, :], item_ref[...])
        inner = jax.nn.relu(pre).astype(BF16)
        hidden = jax.nn.relu(dot(inner, weight_ref[...]))
        prior = packet_ref[n:, :].astype(F32)[:, :1]
        logit = jnp.sum(hidden * head_ref[...], axis=1, keepdims=True) / math.sqrt(hid) + prior
        carry_ref[:, :hid] = hidden.astype(BF16)
        carry_ref[:, hid:] = jnp.broadcast_to(logit, (n, 128)).astype(BF16)
        score_ref[...] = as_row(logit, n)


def rank(part_ref, carry_ref):
    n, hid = part_ref.shape[0] - 8, part_ref.shape[1]
    carry = carry_ref[...].astype(F32)
    hidden = jax.nn.relu(part_ref[:n, :] + carry[:, :hid])
    logit = jnp.sum(hidden * part_ref[n:n + 1, :], axis=1, keepdims=True) / math.sqrt(hid)
    return hidden, logit + carry[:, hid:hid + 1]


def rank_kernel(sec_ref, near_ref, part_ref, carry_ref, score_ref):
    @pl.when(sec_ref[0] == 2)
    def _():
        n, hid = part_ref.shape[0] - 8, part_ref.shape[1]
        hidden, logit = rank(part_ref, near_ref)
        carry_ref[:, :hid] = hidden.astype(BF16)
        carry_ref[:, hid:] = jnp.broadcast_to(logit, (n, 128)).astype(BF16)
        score_ref[...] = as_row(logit, n)


def final_kernel(sec_ref, last_ref, part_ref, score0_ref, score1_ref, score2_ref, score_ref):
    sec = sec_ref[0]

    for s, from_ref in enumerate((score0_ref, score1_ref, score2_ref)):
        @pl.when(sec == s)
        def _():
            score_ref[...] = from_ref[...]

    @pl.when(sec == 3)
    def _():
        _, logit = rank(part_ref, last_ref)
        score_ref[...] = as_row(logit, logit.shape[0])


def cascade(
    user_dense,
    tables,
    feat_owner,
    feat_row,
    keep_first,
    keep_second,
    section_weight,
    section_head,
    user_proj,
    item_in,
    item_out,
    prerank_feat,
    prerank_item,
):
    shape = pltpu.VMEM
    shards = lax.axis_size("shard")
    cands = feat_row.shape[2]
    slots = 2 * cands // shards
    spots = shards * slots
    width = tables.shape[2]
    hid = section_weight.shape[1]
    final = keep_second.shape[1]
    sec = lax.axis_index("section").reshape(1).astype(jnp.int32)
    user = lax.axis_index("shard").reshape(1).astype(jnp.int32)
    turns = [sec[0] == 0, sec[0] == 1, sec[0] >= 2]
    like = lambda a: shape(a.shape, a.dtype)

    feat, item, into, out_of, proj = in_hbm(prerank_feat, prerank_item, item_in, item_out, user_proj)
    weight = section_weight[0]

    def weight_near():
        return pltpu.with_memory_space_constraint(weight, pltpu.VMEM)


    request, slot, spot, table, head = call(
        request_kernel,
        (shape((shards, 128), jnp.int32), shape((1, cands), jnp.int32), shape((128, 128), jnp.int32), like(tables[0]),
         like(section_head)),
        user, *(turn.astype(jnp.int32).reshape(1) for turn in turns),
        *in_hbm(feat_owner.reshape(1, cands), feat_row.reshape(1, cands), tables[0], keep_first, keep_second, section_head,
                section_weight[0]),
        smem=4, hbm=7, sems=6, flops=10**8,
        scratch=[pltpu.VMEM(s, jnp.int32) for s in ((1, cands), (1, cands), keep_first.shape, keep_second.shape)],
    )
    asked = lax.all_to_all(request.reshape(shards, 1, 128), "shard", 0, 0, tiled=True).reshape(shards, 128)

    def exchanged(served):
        rows = lax.all_to_all(served.reshape(shards, -1, width), "shard", 0, 0, tiled=True)
        return rows.reshape(-1, width)

    def serve():
        return call(serve_kernel, shape((spots, width), BF16), asked, table, flops=10**9)

    def blank(*shapes):
        return pl.pallas_call(
            nothing_kernel,
            out_shape=shapes,
            in_specs=[pl.BlockSpec(memory_space=pl.ANY)],
            out_specs=(pl.BlockSpec(memory_space=pltpu.VMEM),) * len(shapes),
            compiler_params=pltpu.CompilerParams(vmem_limit_bytes=1 << 20),
        )(asked)

    scored = shape((1, final), F32)
    carried = shape((final, hid + 128), BF16)

    def either(over, served, then):
        return lax.cond(over[0] >= MARK, lambda: then(exchanged(serve())), lambda: then(exchanged(served)))

    def kept(*arrays):
        return tuple(call(copy_kernel, tuple(like(a) for a in arrays), *arrays))

    short = shape((spots // 2, width), BF16)
    scalar = pltpu.SMEM((1,), jnp.int32)
    packed = shape((2 * final, width), BF16)
    product = shape((final, hid), F32)

    def section_zero():
        served, query, into_near, out_of_near, over = call(
            serve_zero_kernel,
            (short, shape((1, width), F32), like(into), like(out_of), scalar),
            proj, into, out_of, asked, table, user_dense, head, weight_near(),
            hbm=3, sems=3, flops=10**9, smem_out=True,
            scratch=[pltpu.VMEM(proj.shape, BF16)],
        )
        return kept(*either(over, served, lambda rows: tuple(call(
            tower_kernel, (packed, scored), spot, rows, query, into_near, out_of_near, flops=10**7))))

    def section_one():
        served, item_near, over = call(
            serve_one_kernel,
            (short, like(item), scalar),
            item, asked, table,
            hbm=1, sems=1, flops=10**9, smem_out=True,
        )
        product_near = either(over, served, lambda rows: call(
            features_kernel, product, feat, spot, rows,
            hbm=1, sems=1, scratch=[pltpu.VMEM(feat.shape, BF16)], flops=10**8))
        return *kept(product_near), item_near

    def dense_sections():
        return call(
            gram_kernel, shape((final + 8, hid), F32), slot, exchanged(serve()), head, weight_near(), flops=10**9)

    def sparse_sections():
        packet, score0 = lax.cond(turns[0], section_zero, lambda: tuple(blank(packed, scored)))
        packet = lax.ppermute(packet, "section", [(0, 1)])
        pre, item_near = lax.cond(turns[1], section_one, lambda: tuple(blank(product, like(item))))
        return *call(
            prerank_kernel,
            (carried, scored),
            sec, packet, pre, item_near, weight_near(), head,
            smem=1, flops=10**8,
        ), score0

    carry, score1, score0 = lax.cond(turns[2], lambda: tuple(blank(carried, scored, scored)), sparse_sections)
    near = lax.ppermute(carry, "section", [(1, 2)])
    part = lax.cond(turns[2], dense_sections, lambda: blank(shape((final + 8, hid), F32))[0])
    carry, score2 = call(rank_kernel, (carried, scored), sec, near, part, smem=1, flops=10**6)
    last = lax.ppermute(carry, "section", [(2, 3)])
    scores = call(
        final_kernel,
        jax.ShapeDtypeStruct((1, final), F32),
        sec, last, part, score0, score1, score2,
        smem=1, flops=10**6,
    )
    return scores[None]


def solution(mesh):
    placed = (
        P("shard", None),
        P("section", "shard", None),
        P("section", "shard", None, None),
        P("section", "shard", None),
        P("shard", None),
        P("shard", None),
        P("section", None, None),
        P("section", None),
        P(),
        P(),
        P(),
        P(),
        P(),
    )
    return jax.shard_map(
        cascade,
        mesh=mesh,
        in_specs=placed,
        out_specs=P("section", "shard", None),
        check_vma=False,
    )
```

```python
import math

import jax
import jax.numpy as jnp
from jax import lax
from jax.experimental import pallas as pl
from jax.experimental.pallas import tpu as pltpu
from jax.sharding import PartitionSpec as P


F32 = jnp.float32
BF16 = jnp.bfloat16
NT = (((1,), (1,)), ((), ()))
MARK = 1 << 14


def call(kernel, out_shape, *operands, smem=0, hbm=0, sems=0, flops=0, scratch=(), smem_out=False):
    specs = [pl.BlockSpec(memory_space=pltpu.SMEM)] * smem
    specs += [pl.BlockSpec(memory_space=pltpu.HBM)] * hbm
    specs += [pl.BlockSpec(memory_space=pltpu.VMEM)] * (len(operands) - smem - hbm)
    vmem, scalar = pl.BlockSpec(memory_space=pltpu.VMEM), pl.BlockSpec(memory_space=pltpu.SMEM)
    many = isinstance(out_shape, (tuple, list))
    return pl.pallas_call(
        kernel,
        out_shape=out_shape,
        out_specs=(vmem,) * (len(out_shape) - 1) + (scalar,) if smem_out else (vmem,) * len(out_shape) if many else vmem,
        in_specs=specs,
        scratch_shapes=[*scratch, *([pltpu.SemaphoreType.DMA((sems,))] if sems else [])],
        cost_estimate=pl.CostEstimate(flops=flops, transcendentals=0, bytes_accessed=0),
        compiler_params=pltpu.CompilerParams(vmem_limit_bytes=20 << 20),
    )(*operands)


def copies(sources, targets, sem):
    return [pltpu.make_async_copy(a, b, sem.at[i]) for i, (a, b) in enumerate(zip(sources, targets))]


def in_hbm(*arrays):
    return [pltpu.with_memory_space_constraint(a, pltpu.HBM) for a in arrays]


def iota(shape, axis):
    return lax.broadcasted_iota(jnp.int32, shape, axis)


def ones_where(mask):
    return jnp.where(mask, 1.0, 0.0).astype(BF16)


def dot(a, b):
    return jnp.dot(a, b, preferred_element_type=F32)


def dot_nt(a, b):
    return lax.dot_general(a, b, NT, preferred_element_type=F32)


def column(row):
    return jnp.broadcast_to(row, (128, 128)).T


def lookup(at, row):
    lanes = iota((at.shape[0], row.shape[1]), 1).astype(F32)
    return jnp.sum(jnp.where(lanes == at, row.astype(F32), 0.0), axis=1, keepdims=True)


def request_kernel(user_ref, zero_ref, one_ref, dense_ref, owner_hbm, row_hbm, table_hbm, first_hbm, second_hbm, head_hbm,
                   weight_hbm, req_ref, slot_ref, spot_ref, table_ref, head_ref,
                   owner_ref, row_ref, first_ref, second_ref, sem):
    moves = copies((owner_hbm, row_hbm, first_hbm, second_hbm, table_hbm, head_hbm),
                   (owner_ref, row_ref, first_ref, second_ref, table_ref, head_ref), sem)
    for move in moves:
        move.start()
    shards = req_ref.shape[0]
    cands = owner_ref.shape[1]
    final = second_ref.shape[1]
    slots = 2 * cands // shards
    base = (user_ref[0] % (128 // slots)) * slots

    @pl.when(dense_ref[0] == 1)
    def _():
        moves[0].wait()
        earlier = ones_where((iota((128, 256), 0) < iota((128, 256), 1)) | (iota((128, 256), 1) >= 128))
        seen = jnp.zeros((shards, 128), F32)
        ranks = []
        owner = owner_ref[...]
        hits = owner == iota((shards, cands), 0)
        hot = ones_where(hits)
        for b in range(cands // 128):
            part = slice(b * 128, b * 128 + 128)
            counts = dot(hot[:, part], earlier)
            ranks.append(jnp.sum(jnp.where(hits[:, part], counts[:, :128] + seen, 0.0), axis=0, keepdims=True))
            seen = seen + counts[:, 128:]
        rank = jnp.concatenate(ranks, axis=1).astype(jnp.int32)
        slot_ref[...] = owner * slots + rank
        for move in moves[1:4]:
            move.wait()
        row = row_ref[...]
        at_slot = rank + base == iota((128, cands), 0)
        high = jnp.where(at_slot, (row >> 4).astype(F32), 0.0).astype(BF16)
        low = jnp.where(at_slot, (row & 15).astype(F32), 0.0).astype(BF16)
        both = dot_nt(hot, jnp.concatenate([high, low], axis=0))
        req_ref[...] = (both[:, :128] * 16.0 + both[:, 128:]).astype(jnp.int32)

    def request_rows(at):
        owner = lookup(at, owner_ref[...] + 1) - 1.0
        row = lookup(at, row_ref[...]).astype(jnp.int32)
        count = at.shape[0]
        lanes = iota((count, 128), 1).astype(F32)
        hot = jnp.where(owner == lanes, 1.0, 0.0)
        before = ones_where(iota((count, count), 1) < iota((count, count), 0))
        rank = jnp.sum(hot * dot(before, hot.astype(BF16)), axis=1, keepdims=True)
        spot_ref[:count, :] = jnp.broadcast_to(owner * slots + rank, (count, 128)).astype(jnp.int32)
        at_slot = rank + base.astype(F32) == lanes
        high = jnp.where(at_slot, (row >> 4).astype(F32), 0.0).astype(BF16)
        low = jnp.where(at_slot, (row & 15).astype(F32), 0.0).astype(BF16)
        turned = hot.T.astype(BF16)
        mine = (iota((1, 128), 1) >= base) & (iota((1, 128), 1) < base + slots)
        over = jnp.max(rank, axis=0, keepdims=True) >= slots // 2
        mark = jnp.where(mine & over, MARK, 0)
        both = dot(turned, jnp.concatenate([high, low], axis=1))
        req_ref[...] = (both[:, :128] * 16.0 + both[:, 128:]).astype(jnp.int32) + mark

    def second_column():
        second = jnp.concatenate([second_ref[...], jnp.zeros((1, 128 - final), jnp.int32)], axis=1)
        return column(second.astype(F32))[:final, :1]

    @pl.when(zero_ref[0] == 1)
    def _():
        for move in moves[:4]:
            move.wait()
        request_rows(lookup(second_column(), first_ref[...]))

    @pl.when(one_ref[0] == 1)
    def _():
        for move in moves[:4]:
            move.wait()
        second = second_column() * 4.0
        request_rows(jnp.concatenate([second + float(f) for f in range(4)], axis=0))

    for move in moves[4:]:
        move.wait()


def halves(table):
    half = table.shape[0] // 2
    return jnp.concatenate([table[:half, :], table[half:, :]], axis=1)


def picked(col, wide):
    half, width = wide.shape[0], wide.shape[1] // 2
    fine = ones_where((col & 127) == iota(col.shape, 1))
    coarse = ((col & (half - 1)) >> 7).astype(F32).astype(BF16)
    hot = [jnp.where(coarse == float(r), fine, jnp.zeros_like(fine)) for r in range(half // 128)]
    both = dot(jnp.concatenate(hot, axis=1), wide)
    return jnp.where(col < half, both[:, :width], both[:, width:]).astype(BF16)


def served_rows(ids_ref, table_ref, out_ref, keep):
    users = ids_ref.shape[0]
    slots = out_ref.shape[0] // users * 16 // keep
    group = 128 // slots
    wide = halves(table_ref[...])
    count = group * keep
    step = 512 // count
    for first in range(0, users // group, step):
        cols = []
        for b in range(first, first + step):
            ids = jnp.sum(ids_ref[b * group:(b + 1) * group, :], axis=0, keepdims=True)
            col = column(ids & (MARK - 1))
            cols += [col[i * slots:i * slots + keep, :] for i in range(group)] if keep < slots else [col]
        out_ref[first * count:(first + step) * count, :] = picked(jnp.concatenate(cols, axis=0), wide)


def serve_kernel(ids_ref, table_ref, out_ref):
    served_rows(ids_ref, table_ref, out_ref, 16)


def serve_zero_kernel(proj_hbm, into_hbm, out_of_hbm, ids_ref, table_ref, dense_ref, head_ref, weight_ref,
                      out_ref, vec_ref, into_ref, out_of_ref, over_ref, proj_ref, sem):
    moves = copies((proj_hbm, into_hbm, out_of_hbm), (proj_ref, into_ref, out_of_ref), sem)
    for move in moves:
        move.start()
    over_ref[0] = jnp.max(ids_ref[...])
    active = jax.nn.relu(dot(dense_ref[...], weight_ref[...]))
    query = (active * head_ref[...]).astype(BF16)
    served_rows(ids_ref, table_ref, out_ref, 8)
    for move in moves:
        move.wait()
    vec_ref[...] = dot(query, proj_ref[...])


def serve_one_kernel(item_hbm, ids_ref, table_ref, out_ref, item_ref, over_ref, sem):
    move = pltpu.make_async_copy(item_hbm, item_ref, sem.at[0])
    move.start()
    over_ref[0] = jnp.max(ids_ref[...])
    served_rows(ids_ref, table_ref, out_ref, 8)
    move.wait()


def nothing_kernel(*refs):
    pass


def copy_kernel(*refs):
    half = len(refs) // 2
    for from_ref, to_ref in zip(refs[:half], refs[half:]):
        to_ref[...] = from_ref[...]


def as_row(col, lanes):
    n = col.shape[0]
    return jnp.sum(jnp.where(iota((n, lanes), 0) == iota((n, lanes), 1), col, 0.0), axis=0, keepdims=True)


def survivors(spot, rows):
    slots = rows.shape[0] // 128
    return picked((spot >> 4) * slots + (spot & 15), halves(rows))


def tower_kernel(spot_ref, rows_ref, vec_ref, into_ref, out_of_ref, packet_ref, score_ref):
    n = packet_ref.shape[0] // 2
    embed = survivors(spot_ref[:n, :], rows_ref[...])
    hidden = jax.nn.relu(dot(embed, into_ref[...])).astype(BF16)
    tower = dot(hidden, out_of_ref[...]).astype(BF16)
    logit = jnp.sum(tower.astype(F32) * vec_ref[...], axis=1, keepdims=True)
    packet_ref[:n, :] = tower
    packet_ref[n:, :] = jnp.broadcast_to(logit, (n, 128)).astype(BF16)
    score_ref[...] = as_row(logit, n)


def features_kernel(feat_hbm, spot_ref, rows_ref, part_ref, feat_ref, sem):
    move = pltpu.make_async_copy(feat_hbm, feat_ref, sem.at[0])
    move.start()
    n = part_ref.shape[0]
    embed = survivors(spot_ref[:4 * n, :], rows_ref[...])
    tall = jnp.concatenate([embed[f * n:(f + 1) * n, :] for f in range(4)], axis=1)
    move.wait()
    part_ref[...] = dot(tall, feat_ref[...])


def gram_kernel(slot_ref, rows_ref, head_ref, weight_ref, part_ref):
    n = part_ref.shape[0] - 8
    cands = slot_ref.shape[1]
    width = rows_ref.shape[1]
    wide = halves(rows_ref[...])
    embed = [
        picked(jnp.concatenate([column(slot_ref[:, b:b + 128]) for b in range(h, h + 512, 128)], axis=0), wide)
        for h in range(0, cands, 512)
    ]
    own_lanes = (iota((32, 128), 0) % 4) == (iota((32, 128), 1) // 32)
    grams = []
    for b in range(cands // 128):
        block = embed[b // 4][b % 4 * 128:b % 4 * 128 + 128, :]
        items = [block[i * 32:i * 32 + 32, :] for i in range(4)]
        four = []
        for i in (0, 2):
            wide_pair = jnp.concatenate([items[i]] * 4 + [items[i + 1]] * 4, axis=0)
            both = dot_nt(block[i * 32:i * 32 + 64, :], wide_pair) * (1.0 / math.sqrt(width))
            four += [jnp.where(own_lanes, both[:32, :128], 0.0), jnp.where(own_lanes, both[32:, 128:], 0.0)]
        grams.append(jnp.concatenate(four, axis=0).astype(BF16))
    i, k = iota((64, 256), 0), iota((64, 256), 1)
    choose = ones_where(((k // 32) == (i % 8)) & (((k % 32) // 4) == (i // 8)))
    flat = []
    for b in range(0, len(grams), 2):
        eight = dot(choose, jnp.concatenate(grams[b:b + 2], axis=0))
        flat.append(jnp.concatenate([eight[q * 8:q * 8 + 8, :] for q in range(8)], axis=1))
    flat = jnp.concatenate(flat, axis=0).astype(BF16)
    part_ref[:n, :] = dot(flat, weight_ref[...])
    part_ref[n:n + 1, :] = head_ref[...]


def prerank_kernel(sec_ref, packet_ref, part_ref, item_ref, weight_ref, head_ref, carry_ref, score_ref):
    @pl.when(sec_ref[0] == 1)
    def _():
        n, hid = part_ref.shape
        pre = part_ref[...] + dot(packet_ref[:n, :], item_ref[...])
        inner = jax.nn.relu(pre).astype(BF16)
        hidden = jax.nn.relu(dot(inner, weight_ref[...]))
        prior = packet_ref[n:, :].astype(F32)[:, :1]
        logit = jnp.sum(hidden * head_ref[...], axis=1, keepdims=True) / math.sqrt(hid) + prior
        carry_ref[:, :hid] = hidden.astype(BF16)
        carry_ref[:, hid:] = jnp.broadcast_to(logit, (n, 128)).astype(BF16)
        score_ref[...] = as_row(logit, n)


def rank(part_ref, carry_ref):
    n, hid = part_ref.shape[0] - 8, part_ref.shape[1]
    carry = carry_ref[...].astype(F32)
    hidden = jax.nn.relu(part_ref[:n, :] + carry[:, :hid])
    logit = jnp.sum(hidden * part_ref[n:n + 1, :], axis=1, keepdims=True) / math.sqrt(hid)
    return hidden, logit + carry[:, hid:hid + 1]


def rank_kernel(sec_ref, near_ref, part_ref, carry_ref, score_ref):
    @pl.when(sec_ref[0] == 2)
    def _():
        n, hid = part_ref.shape[0] - 8, part_ref.shape[1]
        hidden, logit = rank(part_ref, near_ref)
        carry_ref[:, :hid] = hidden.astype(BF16)
        carry_ref[:, hid:] = jnp.broadcast_to(logit, (n, 128)).astype(BF16)
        score_ref[...] = as_row(logit, n)


def final_kernel(sec_ref, last_ref, part_ref, score0_ref, score1_ref, score2_ref, score_ref):
    sec = sec_ref[0]

    for s, from_ref in enumerate((score0_ref, score1_ref, score2_ref)):
        @pl.when(sec == s)
        def _():
            score_ref[...] = from_ref[...]

    @pl.when(sec == 3)
    def _():
        _, logit = rank(part_ref, last_ref)
        score_ref[...] = as_row(logit, logit.shape[0])


def cascade(
    user_dense,
    tables,
    feat_owner,
    feat_row,
    keep_first,
    keep_second,
    section_weight,
    section_head,
    user_proj,
    item_in,
    item_out,
    prerank_feat,
    prerank_item,
):
    shape = pltpu.VMEM
    shards = lax.axis_size("shard")
    cands = feat_row.shape[2]
    slots = 2 * cands // shards
    spots = shards * slots
    width = tables.shape[2]
    hid = section_weight.shape[1]
    final = keep_second.shape[1]
    sec = lax.axis_index("section").reshape(1).astype(jnp.int32)
    user = lax.axis_index("shard").reshape(1).astype(jnp.int32)
    turns = [sec[0] == 0, sec[0] == 1, sec[0] >= 2]
    like = lambda a: shape(a.shape, a.dtype)

    feat, item, into, out_of, proj = in_hbm(prerank_feat, prerank_item, item_in, item_out, user_proj)
    weight = section_weight[0]

    def weight_near():
        return pltpu.with_memory_space_constraint(weight, pltpu.VMEM)


    request, slot, spot, table, head = call(
        request_kernel,
        (shape((shards, 128), jnp.int32), shape((1, cands), jnp.int32), shape((128, 128), jnp.int32), like(tables[0]),
         like(section_head)),
        user, *(turn.astype(jnp.int32).reshape(1) for turn in turns),
        *in_hbm(feat_owner.reshape(1, cands), feat_row.reshape(1, cands), tables[0], keep_first, keep_second, section_head,
                section_weight[0]),
        smem=4, hbm=7, sems=6, flops=10**8,
        scratch=[pltpu.VMEM(s, jnp.int32) for s in ((1, cands), (1, cands), keep_first.shape, keep_second.shape)],
    )
    asked = lax.all_to_all(request.reshape(shards, 1, 128), "shard", 0, 0, tiled=True).reshape(shards, 128)

    def exchanged(served):
        rows = lax.all_to_all(served.reshape(shards, -1, width), "shard", 0, 0, tiled=True)
        return rows.reshape(-1, width)

    def serve():
        return call(serve_kernel, shape((spots, width), BF16), asked, table, flops=10**9)

    def blank(*shapes):
        return pl.pallas_call(
            nothing_kernel,
            out_shape=shapes,
            in_specs=[pl.BlockSpec(memory_space=pl.ANY)],
            out_specs=(pl.BlockSpec(memory_space=pltpu.VMEM),) * len(shapes),
            compiler_params=pltpu.CompilerParams(vmem_limit_bytes=1 << 20),
        )(asked)

    scored = shape((1, final), F32)
    carried = shape((final, hid + 128), BF16)

    def either(over, served, then):
        return lax.cond(over[0] >= MARK, lambda: then(exchanged(serve())), lambda: then(exchanged(served)))

    def kept(*arrays):
        return tuple(call(copy_kernel, tuple(like(a) for a in arrays), *arrays))

    short = shape((spots // 2, width), BF16)
    scalar = pltpu.SMEM((1,), jnp.int32)
    packed = shape((2 * final, width), BF16)
    product = shape((final, hid), F32)

    def section_zero():
        served, query, into_near, out_of_near, over = call(
            serve_zero_kernel,
            (short, shape((1, width), F32), like(into), like(out_of), scalar),
            proj, into, out_of, asked, table, user_dense, head, weight_near(),
            hbm=3, sems=3, flops=10**9, smem_out=True,
            scratch=[pltpu.VMEM(proj.shape, BF16)],
        )
        return kept(*either(over, served, lambda rows: tuple(call(
            tower_kernel, (packed, scored), spot, rows, query, into_near, out_of_near, flops=10**7))))

    def section_one():
        served, item_near, over = call(
            serve_one_kernel,
            (short, like(item), scalar),
            item, asked, table,
            hbm=1, sems=1, flops=10**9, smem_out=True,
        )
        product_near = either(over, served, lambda rows: call(
            features_kernel, product, feat, spot, rows,
            hbm=1, sems=1, scratch=[pltpu.VMEM(feat.shape, BF16)], flops=10**8))
        return *kept(product_near), item_near

    def dense_sections():
        return call(
            gram_kernel, shape((final + 8, hid), F32), slot, exchanged(serve()), head, weight_near(), flops=10**9)

    def sparse_sections():
        packet, score0 = lax.cond(turns[0], section_zero, lambda: tuple(blank(packed, scored)))
        packet = lax.ppermute(packet, "section", [(0, 1)])
        pre, item_near = lax.cond(turns[1], section_one, lambda: tuple(blank(product, like(item))))
        return *call(
            prerank_kernel,
            (carried, scored),
            sec, packet, pre, item_near, weight_near(), head,
            smem=1, flops=10**8,
        ), score0

    carry, score1, score0 = lax.cond(turns[2], lambda: tuple(blank(carried, scored, scored)), sparse_sections)
    near = lax.ppermute(carry, "section", [(1, 2)])
    part = lax.cond(turns[2], dense_sections, lambda: blank(shape((final + 8, hid), F32))[0])
    carry, score2 = call(rank_kernel, (carried, scored), sec, near, part, smem=1, flops=10**6)
    last = lax.ppermute(carry, "section", [(2, 3)])
    scores = call(
        final_kernel,
        jax.ShapeDtypeStruct((1, final), F32),
        sec, last, part, score0, score1, score2,
        smem=1, flops=10**6,
    )
    return scores[None]


def solution(mesh):
    placed = (
        P("shard", None),
        P("section", "shard", None),
        P("section", "shard", None, None),
        P("section", "shard", None),
        P("shard", None),
        P("shard", None),
        P("section", None, None),
        P("section", None),
        P(),
        P(),
        P(),
        P(),
        P(),
    )
    return jax.shard_map(
        cascade,
        mesh=mesh,
        in_specs=placed,
        out_specs=P("section", "shard", None),
        check_vma=False,
    )
```

```python
import math

import jax
import jax.numpy as jnp
from jax import lax
from jax.experimental import pallas as pl
from jax.experimental.pallas import tpu as pltpu
from jax.sharding import PartitionSpec as P


F32 = jnp.float32
BF16 = jnp.bfloat16
NT = (((1,), (1,)), ((), ()))
MARK = 1 << 14


def call(kernel, out_shape, *operands, smem=0, hbm=0, sems=0, flops=0, scratch=(), smem_out=False):
    specs = [pl.BlockSpec(memory_space=pltpu.SMEM)] * smem
    specs += [pl.BlockSpec(memory_space=pltpu.HBM)] * hbm
    specs += [pl.BlockSpec(memory_space=pltpu.VMEM)] * (len(operands) - smem - hbm)
    vmem, scalar = pl.BlockSpec(memory_space=pltpu.VMEM), pl.BlockSpec(memory_space=pltpu.SMEM)
    many = isinstance(out_shape, (tuple, list))
    return pl.pallas_call(
        kernel,
        out_shape=out_shape,
        out_specs=(vmem,) * (len(out_shape) - 1) + (scalar,) if smem_out else (vmem,) * len(out_shape) if many else vmem,
        in_specs=specs,
        scratch_shapes=[*scratch, *([pltpu.SemaphoreType.DMA((sems,))] if sems else [])],
        cost_estimate=pl.CostEstimate(flops=flops, transcendentals=0, bytes_accessed=0),
        compiler_params=pltpu.CompilerParams(vmem_limit_bytes=20 << 20),
    )(*operands)


def copies(sources, targets, sem):
    return [pltpu.make_async_copy(a, b, sem.at[i]) for i, (a, b) in enumerate(zip(sources, targets))]


def in_hbm(*arrays):
    return [pltpu.with_memory_space_constraint(a, pltpu.HBM) for a in arrays]


def iota(shape, axis):
    return lax.broadcasted_iota(jnp.int32, shape, axis)


def ones_where(mask):
    return jnp.where(mask, 1.0, 0.0).astype(BF16)


def dot(a, b):
    return jnp.dot(a, b, preferred_element_type=F32)


def dot_nt(a, b):
    return lax.dot_general(a, b, NT, preferred_element_type=F32)


def column(row):
    return jnp.broadcast_to(row, (128, 128)).T


def lookup(at, row):
    lanes = iota((at.shape[0], row.shape[1]), 1).astype(F32)
    return jnp.sum(jnp.where(lanes == at, row.astype(F32), 0.0), axis=1, keepdims=True)


def request_kernel(user_ref, zero_ref, one_ref, dense_ref, owner_hbm, row_hbm, table_hbm, first_hbm, second_hbm, head_hbm,
                   weight_hbm, req_ref, slot_ref, spot_ref, table_ref, head_ref,
                   owner_ref, row_ref, first_ref, second_ref, sem):
    moves = copies((owner_hbm, row_hbm, first_hbm, second_hbm, table_hbm, head_hbm),
                   (owner_ref, row_ref, first_ref, second_ref, table_ref, head_ref), sem)
    for move in moves:
        move.start()
    shards = req_ref.shape[0]
    cands = owner_ref.shape[1]
    final = second_ref.shape[1]
    slots = 2 * cands // shards
    base = (user_ref[0] % (128 // slots)) * slots

    @pl.when(dense_ref[0] == 1)
    def _():
        moves[0].wait()
        earlier = ones_where((iota((128, 256), 0) < iota((128, 256), 1)) | (iota((128, 256), 1) >= 128))
        seen = jnp.zeros((shards, 128), F32)
        ranks = []
        owner = owner_ref[...]
        hits = owner == iota((shards, cands), 0)
        hot = ones_where(hits)
        for b in range(cands // 128):
            part = slice(b * 128, b * 128 + 128)
            counts = dot(hot[:, part], earlier)
            ranks.append(jnp.sum(jnp.where(hits[:, part], counts[:, :128] + seen, 0.0), axis=0, keepdims=True))
            seen = seen + counts[:, 128:]
        rank = jnp.concatenate(ranks, axis=1).astype(jnp.int32)
        slot_ref[...] = owner * slots + rank
        for move in moves[1:4]:
            move.wait()
        row = row_ref[...]
        at_slot = rank + base == iota((128, cands), 0)
        high = jnp.where(at_slot, (row >> 4).astype(F32), 0.0).astype(BF16)
        low = jnp.where(at_slot, (row & 15).astype(F32), 0.0).astype(BF16)
        both = dot_nt(hot, jnp.concatenate([high, low], axis=0))
        req_ref[...] = (both[:, :128] * 16.0 + both[:, 128:]).astype(jnp.int32)

    def request_rows(at):
        owner = lookup(at, owner_ref[...] + 1) - 1.0
        row = lookup(at, row_ref[...]).astype(jnp.int32)
        count = at.shape[0]
        lanes = iota((count, 128), 1).astype(F32)
        hot = jnp.where(owner == lanes, 1.0, 0.0)
        before = ones_where(iota((count, count), 1) < iota((count, count), 0))
        rank = jnp.sum(hot * dot(before, hot.astype(BF16)), axis=1, keepdims=True)
        spot_ref[:count, :] = jnp.broadcast_to(owner * slots + rank, (count, 128)).astype(jnp.int32)
        at_slot = rank + base.astype(F32) == lanes
        high = jnp.where(at_slot, (row >> 4).astype(F32), 0.0).astype(BF16)
        low = jnp.where(at_slot, (row & 15).astype(F32), 0.0).astype(BF16)
        turned = hot.T.astype(BF16)
        mine = (iota((1, 128), 1) >= base) & (iota((1, 128), 1) < base + slots)
        over = jnp.max(rank, axis=0, keepdims=True) >= slots // 2
        mark = jnp.where(mine & over, MARK, 0)
        both = dot(turned, jnp.concatenate([high, low], axis=1))
        req_ref[...] = (both[:, :128] * 16.0 + both[:, 128:]).astype(jnp.int32) + mark

    def second_column():
        second = jnp.concatenate([second_ref[...], jnp.zeros((1, 128 - final), jnp.int32)], axis=1)
        return column(second.astype(F32))[:final, :1]

    @pl.when(zero_ref[0] == 1)
    def _():
        for move in moves[:4]:
            move.wait()
        request_rows(lookup(second_column(), first_ref[...]))

    @pl.when(one_ref[0] == 1)
    def _():
        for move in moves[:4]:
            move.wait()
        second = second_column() * 4.0
        request_rows(jnp.concatenate([second + float(f) for f in range(4)], axis=0))

    for move in moves[4:]:
        move.wait()


def halves(table):
    half = table.shape[0] // 2
    return jnp.concatenate([table[:half, :], table[half:, :]], axis=1)


def picked(col, wide):
    half, width = wide.shape[0], wide.shape[1] // 2
    fine = ones_where((col & 127) == iota(col.shape, 1))
    coarse = ((col & (half - 1)) >> 7).astype(F32).astype(BF16)
    hot = [jnp.where(coarse == float(r), fine, jnp.zeros_like(fine)) for r in range(half // 128)]
    both = dot(jnp.concatenate(hot, axis=1), wide)
    return jnp.where(col < half, both[:, :width], both[:, width:]).astype(BF16)


def served_rows(ids_ref, table_ref, out_ref, keep):
    users = ids_ref.shape[0]
    slots = out_ref.shape[0] // users * 16 // keep
    group = 128 // slots
    wide = halves(table_ref[...])
    count = group * keep
    step = 512 // count
    for first in range(0, users // group, step):
        cols = []
        for b in range(first, first + step):
            ids = jnp.sum(ids_ref[b * group:(b + 1) * group, :], axis=0, keepdims=True)
            col = column(ids & (MARK - 1))
            cols += [col[i * slots:i * slots + keep, :] for i in range(group)] if keep < slots else [col]
        out_ref[first * count:(first + step) * count, :] = picked(jnp.concatenate(cols, axis=0), wide)


def serve_kernel(ids_ref, table_ref, out_ref):
    served_rows(ids_ref, table_ref, out_ref, 16)


def serve_zero_kernel(proj_hbm, into_hbm, out_of_hbm, ids_ref, table_ref, dense_ref, head_ref, weight_ref,
                      out_ref, query_ref, into_ref, out_of_ref, proj_ref, over_ref, sem):
    moves = copies((proj_hbm, into_hbm, out_of_hbm), (proj_ref, into_ref, out_of_ref), sem)
    for move in moves:
        move.start()
    over_ref[0] = jnp.max(ids_ref[...])
    active = jax.nn.relu(dot(dense_ref[...], weight_ref[...]))
    query_ref[...] = (active * head_ref[...]).astype(BF16)
    served_rows(ids_ref, table_ref, out_ref, 8)
    for move in moves:
        move.wait()


def serve_one_kernel(item_hbm, ids_ref, table_ref, out_ref, item_ref, over_ref, sem):
    move = pltpu.make_async_copy(item_hbm, item_ref, sem.at[0])
    move.start()
    over_ref[0] = jnp.max(ids_ref[...])
    served_rows(ids_ref, table_ref, out_ref, 8)
    move.wait()


def nothing_kernel(*refs):
    pass


def copy_kernel(*refs):
    half = len(refs) // 2
    for from_ref, to_ref in zip(refs[:half], refs[half:]):
        to_ref[...] = from_ref[...]


def as_row(col, lanes):
    n = col.shape[0]
    return jnp.sum(jnp.where(iota((n, lanes), 0) == iota((n, lanes), 1), col, 0.0), axis=0, keepdims=True)


def survivors(spot, rows):
    slots = rows.shape[0] // 128
    return picked((spot >> 4) * slots + (spot & 15), halves(rows))


def tower_kernel(spot_ref, rows_ref, query_ref, proj_ref, into_ref, out_of_ref, packet_ref, score_ref):
    n = packet_ref.shape[0] // 2
    vec = dot(query_ref[...], proj_ref[...])
    embed = survivors(spot_ref[:n, :], rows_ref[...])
    hidden = jax.nn.relu(dot(embed, into_ref[...])).astype(BF16)
    tower = dot(hidden, out_of_ref[...]).astype(BF16)
    logit = jnp.sum(tower.astype(F32) * vec, axis=1, keepdims=True)
    packet_ref[:n, :] = tower
    packet_ref[n:, :] = jnp.broadcast_to(logit, (n, 128)).astype(BF16)
    score_ref[...] = as_row(logit, n)


def features_kernel(feat_hbm, spot_ref, rows_ref, part_ref, feat_ref, sem):
    move = pltpu.make_async_copy(feat_hbm, feat_ref, sem.at[0])
    move.start()
    n = part_ref.shape[0]
    embed = survivors(spot_ref[:4 * n, :], rows_ref[...])
    tall = jnp.concatenate([embed[f * n:(f + 1) * n, :] for f in range(4)], axis=1)
    move.wait()
    part_ref[...] = dot(tall, feat_ref[...])


def gram_kernel(slot_ref, rows_ref, head_ref, weight_ref, part_ref):
    n = part_ref.shape[0] - 8
    cands = slot_ref.shape[1]
    width = rows_ref.shape[1]
    wide = halves(rows_ref[...])
    embed = [
        picked(jnp.concatenate([column(slot_ref[:, b:b + 128]) for b in range(h, h + 512, 128)], axis=0), wide)
        for h in range(0, cands, 512)
    ]
    own_lanes = (iota((32, 128), 0) % 4) == (iota((32, 128), 1) // 32)
    grams = []
    for b in range(cands // 128):
        block = embed[b // 4][b % 4 * 128:b % 4 * 128 + 128, :]
        items = [block[i * 32:i * 32 + 32, :] for i in range(4)]
        four = []
        for i in (0, 2):
            wide_pair = jnp.concatenate([items[i]] * 4 + [items[i + 1]] * 4, axis=0)
            both = dot_nt(block[i * 32:i * 32 + 64, :], wide_pair) * (1.0 / math.sqrt(width))
            four += [jnp.where(own_lanes, both[:32, :128], 0.0), jnp.where(own_lanes, both[32:, 128:], 0.0)]
        grams.append(jnp.concatenate(four, axis=0).astype(BF16))
    i, k = iota((64, 256), 0), iota((64, 256), 1)
    choose = ones_where(((k // 32) == (i % 8)) & (((k % 32) // 4) == (i // 8)))
    flat = []
    for b in range(0, len(grams), 2):
        eight = dot(choose, jnp.concatenate(grams[b:b + 2], axis=0))
        flat.append(jnp.concatenate([eight[q * 8:q * 8 + 8, :] for q in range(8)], axis=1))
    flat = jnp.concatenate(flat, axis=0).astype(BF16)
    part_ref[:n, :] = dot(flat, weight_ref[...])
    part_ref[n:n + 1, :] = head_ref[...]


def prerank_kernel(sec_ref, packet_ref, part_ref, item_ref, weight_ref, head_ref, carry_ref, score_ref):
    @pl.when(sec_ref[0] == 1)
    def _():
        n, hid = part_ref.shape
        pre = part_ref[...] + dot(packet_ref[:n, :], item_ref[...])
        inner = jax.nn.relu(pre).astype(BF16)
        hidden = jax.nn.relu(dot(inner, weight_ref[...]))
        prior = packet_ref[n:, :].astype(F32)[:, :1]
        logit = jnp.sum(hidden * head_ref[...], axis=1, keepdims=True) / math.sqrt(hid) + prior
        carry_ref[:, :hid] = hidden.astype(BF16)
        carry_ref[:, hid:] = jnp.broadcast_to(logit, (n, 128)).astype(BF16)
        score_ref[...] = as_row(logit, n)


def rank(part_ref, carry_ref):
    n, hid = part_ref.shape[0] - 8, part_ref.shape[1]
    carry = carry_ref[...].astype(F32)
    hidden = jax.nn.relu(part_ref[:n, :] + carry[:, :hid])
    logit = jnp.sum(hidden * part_ref[n:n + 1, :], axis=1, keepdims=True) / math.sqrt(hid)
    return hidden, logit + carry[:, hid:hid + 1]


def rank_kernel(sec_ref, near_ref, part_ref, carry_ref, score_ref):
    @pl.when(sec_ref[0] == 2)
    def _():
        n, hid = part_ref.shape[0] - 8, part_ref.shape[1]
        hidden, logit = rank(part_ref, near_ref)
        carry_ref[:, :hid] = hidden.astype(BF16)
        carry_ref[:, hid:] = jnp.broadcast_to(logit, (n, 128)).astype(BF16)
        score_ref[...] = as_row(logit, n)


def final_kernel(sec_ref, last_ref, part_ref, score0_ref, score1_ref, score2_ref, score_ref):
    sec = sec_ref[0]

    for s, from_ref in enumerate((score0_ref, score1_ref, score2_ref)):
        @pl.when(sec == s)
        def _():
            score_ref[...] = from_ref[...]

    @pl.when(sec == 3)
    def _():
        _, logit = rank(part_ref, last_ref)
        score_ref[...] = as_row(logit, logit.shape[0])


def cascade(
    user_dense,
    tables,
    feat_owner,
    feat_row,
    keep_first,
    keep_second,
    section_weight,
    section_head,
    user_proj,
    item_in,
    item_out,
    prerank_feat,
    prerank_item,
):
    shape = pltpu.VMEM
    shards = lax.axis_size("shard")
    cands = feat_row.shape[2]
    slots = 2 * cands // shards
    spots = shards * slots
    width = tables.shape[2]
    hid = section_weight.shape[1]
    final = keep_second.shape[1]
    sec = lax.axis_index("section").reshape(1).astype(jnp.int32)
    user = lax.axis_index("shard").reshape(1).astype(jnp.int32)
    turns = [sec[0] == 0, sec[0] == 1, sec[0] >= 2]
    like = lambda a: shape(a.shape, a.dtype)

    feat, item, into, out_of, proj = in_hbm(prerank_feat, prerank_item, item_in, item_out, user_proj)
    weight = section_weight[0]

    def weight_near():
        return pltpu.with_memory_space_constraint(weight, pltpu.VMEM)


    request, slot, spot, table, head = call(
        request_kernel,
        (shape((shards, 128), jnp.int32), shape((1, cands), jnp.int32), shape((128, 128), jnp.int32), like(tables[0]),
         like(section_head)),
        user, *(turn.astype(jnp.int32).reshape(1) for turn in turns),
        *in_hbm(feat_owner.reshape(1, cands), feat_row.reshape(1, cands), tables[0], keep_first, keep_second, section_head,
                section_weight[0]),
        smem=4, hbm=7, sems=6, flops=10**8,
        scratch=[pltpu.VMEM(s, jnp.int32) for s in ((1, cands), (1, cands), keep_first.shape, keep_second.shape)],
    )
    asked = lax.all_to_all(request.reshape(shards, 1, 128), "shard", 0, 0, tiled=True).reshape(shards, 128)

    def exchanged(served):
        rows = lax.all_to_all(served.reshape(shards, -1, width), "shard", 0, 0, tiled=True)
        return rows.reshape(-1, width)

    def serve():
        return call(serve_kernel, shape((spots, width), BF16), asked, table, flops=10**9)

    def blank(*shapes):
        return pl.pallas_call(
            nothing_kernel,
            out_shape=shapes,
            in_specs=[pl.BlockSpec(memory_space=pl.ANY)],
            out_specs=(pl.BlockSpec(memory_space=pltpu.VMEM),) * len(shapes),
            compiler_params=pltpu.CompilerParams(vmem_limit_bytes=1 << 20),
        )(asked)

    scored = shape((1, final), F32)
    carried = shape((final, hid + 128), BF16)

    def either(over, served, then):
        return lax.cond(over[0] >= MARK, lambda: then(exchanged(serve())), lambda: then(exchanged(served)))

    def kept(*arrays):
        return tuple(call(copy_kernel, tuple(like(a) for a in arrays), *arrays))

    short = shape((spots // 2, width), BF16)
    scalar = pltpu.SMEM((1,), jnp.int32)
    packed = shape((2 * final, width), BF16)
    product = shape((final, hid), F32)

    def section_zero():
        served, query, into_near, out_of_near, proj_near, over = call(
            serve_zero_kernel,
            (short, like(user_dense), like(into), like(out_of), like(proj), scalar),
            proj, into, out_of, asked, table, user_dense, head, weight_near(),
            hbm=3, sems=3, flops=10**9, smem_out=True,
        )
        return kept(*either(over, served, lambda rows: tuple(call(
            tower_kernel, (packed, scored), spot, rows, query, proj_near, into_near, out_of_near, flops=10**7))))

    def section_one():
        served, item_near, over = call(
            serve_one_kernel,
            (short, like(item), scalar),
            item, asked, table,
            hbm=1, sems=1, flops=10**9, smem_out=True,
        )
        product_near = either(over, served, lambda rows: call(
            features_kernel, product, feat, spot, rows,
            hbm=1, sems=1, scratch=[pltpu.VMEM(feat.shape, BF16)], flops=10**8))
        return *kept(product_near), item_near

    def dense_sections():
        return call(
            gram_kernel, shape((final + 8, hid), F32), slot, exchanged(serve()), head, weight_near(), flops=10**9)

    def sparse_sections():
        packet, score0 = lax.cond(turns[0], section_zero, lambda: tuple(blank(packed, scored)))
        packet = lax.ppermute(packet, "section", [(0, 1)])
        pre, item_near = lax.cond(turns[1], section_one, lambda: tuple(blank(product, like(item))))
        return *call(
            prerank_kernel,
            (carried, scored),
            sec, packet, pre, item_near, weight_near(), head,
            smem=1, flops=10**8,
        ), score0

    carry, score1, score0 = lax.cond(turns[2], lambda: tuple(blank(carried, scored, scored)), sparse_sections)
    near = lax.ppermute(carry, "section", [(1, 2)])
    part = lax.cond(turns[2], dense_sections, lambda: blank(shape((final + 8, hid), F32))[0])
    carry, score2 = call(rank_kernel, (carried, scored), sec, near, part, smem=1, flops=10**6)
    last = lax.ppermute(carry, "section", [(2, 3)])
    scores = call(
        final_kernel,
        jax.ShapeDtypeStruct((1, final), F32),
        sec, last, part, score0, score1, score2,
        smem=1, flops=10**6,
    )
    return scores[None]


def solution(mesh):
    placed = (
        P("shard", None),
        P("section", "shard", None),
        P("section", "shard", None, None),
        P("section", "shard", None),
        P("shard", None),
        P("shard", None),
        P("section", None, None),
        P("section", None),
        P(),
        P(),
        P(),
        P(),
        P(),
    )
    return jax.shard_map(
        cascade,
        mesh=mesh,
        in_specs=placed,
        out_specs=P("section", "shard", None),
        check_vma=False,
    )
```

```python
import math

import jax
import jax.numpy as jnp
from jax import lax
from jax.experimental import pallas as pl
from jax.experimental.pallas import tpu as pltpu
from jax.sharding import PartitionSpec as P


F32 = jnp.float32
BF16 = jnp.bfloat16
NT = (((1,), (1,)), ((), ()))
MARK = 1 << 14


def call(kernel, out_shape, *operands, smem=0, hbm=0, sems=0, flops=0, scratch=(), smem_out=False):
    specs = [pl.BlockSpec(memory_space=pltpu.SMEM)] * smem
    specs += [pl.BlockSpec(memory_space=pltpu.HBM)] * hbm
    specs += [pl.BlockSpec(memory_space=pltpu.VMEM)] * (len(operands) - smem - hbm)
    vmem, scalar = pl.BlockSpec(memory_space=pltpu.VMEM), pl.BlockSpec(memory_space=pltpu.SMEM)
    many = isinstance(out_shape, (tuple, list))
    return pl.pallas_call(
        kernel,
        out_shape=out_shape,
        out_specs=(vmem,) * (len(out_shape) - 1) + (scalar,) if smem_out else (vmem,) * len(out_shape) if many else vmem,
        in_specs=specs,
        scratch_shapes=[*scratch, *([pltpu.SemaphoreType.DMA((sems,))] if sems else [])],
        cost_estimate=pl.CostEstimate(flops=flops, transcendentals=0, bytes_accessed=0),
        compiler_params=pltpu.CompilerParams(vmem_limit_bytes=20 << 20),
    )(*operands)


def copies(sources, targets, sem):
    return [pltpu.make_async_copy(a, b, sem.at[i]) for i, (a, b) in enumerate(zip(sources, targets))]


def in_hbm(*arrays):
    return [pltpu.with_memory_space_constraint(a, pltpu.HBM) for a in arrays]


def iota(shape, axis):
    return lax.broadcasted_iota(jnp.int32, shape, axis)


def ones_where(mask):
    return jnp.where(mask, 1.0, 0.0).astype(BF16)


def dot(a, b):
    return jnp.dot(a, b, preferred_element_type=F32)


def dot_nt(a, b):
    return lax.dot_general(a, b, NT, preferred_element_type=F32)


def column(row):
    return jnp.broadcast_to(row, (128, 128)).T


def lookup(at, row):
    lanes = iota((at.shape[0], row.shape[1]), 1).astype(F32)
    return jnp.sum(jnp.where(lanes == at, row.astype(F32), 0.0), axis=1, keepdims=True)


def request_kernel(user_ref, zero_ref, one_ref, dense_ref, owner_hbm, row_hbm, table_hbm, first_hbm, second_hbm, head_hbm,
                   weight_hbm, req_ref, slot_ref, spot_ref, head_ref,
                   owner_ref, row_ref, first_ref, second_ref, sem):
    moves = copies((owner_hbm, row_hbm, first_hbm, second_hbm, head_hbm),
                   (owner_ref, row_ref, first_ref, second_ref, head_ref), sem)
    for move in moves:
        move.start()
    shards = req_ref.shape[0]
    cands = owner_ref.shape[1]
    final = second_ref.shape[1]
    slots = 2 * cands // shards
    base = (user_ref[0] % (128 // slots)) * slots

    @pl.when(dense_ref[0] == 1)
    def _():
        moves[0].wait()
        earlier = ones_where((iota((128, 256), 0) < iota((128, 256), 1)) | (iota((128, 256), 1) >= 128))
        seen = jnp.zeros((shards, 128), F32)
        ranks = []
        owner = owner_ref[...]
        hits = owner == iota((shards, cands), 0)
        hot = ones_where(hits)
        for b in range(cands // 128):
            part = slice(b * 128, b * 128 + 128)
            counts = dot(hot[:, part], earlier)
            ranks.append(jnp.sum(jnp.where(hits[:, part], counts[:, :128] + seen, 0.0), axis=0, keepdims=True))
            seen = seen + counts[:, 128:]
        rank = jnp.concatenate(ranks, axis=1).astype(jnp.int32)
        slot_ref[...] = owner * slots + rank
        for move in moves[1:4]:
            move.wait()
        row = row_ref[...]
        at_slot = rank + base == iota((128, cands), 0)
        high = jnp.where(at_slot, (row >> 4).astype(F32), 0.0).astype(BF16)
        low = jnp.where(at_slot, (row & 15).astype(F32), 0.0).astype(BF16)
        both = dot_nt(hot, jnp.concatenate([high, low], axis=0))
        req_ref[...] = (both[:, :128] * 16.0 + both[:, 128:]).astype(jnp.int32)

    def request_rows(at):
        owner = lookup(at, owner_ref[...] + 1) - 1.0
        row = lookup(at, row_ref[...]).astype(jnp.int32)
        count = at.shape[0]
        lanes = iota((count, 128), 1).astype(F32)
        hot = jnp.where(owner == lanes, 1.0, 0.0)
        before = ones_where(iota((count, count), 1) < iota((count, count), 0))
        rank = jnp.sum(hot * dot(before, hot.astype(BF16)), axis=1, keepdims=True)
        spot_ref[:count, :] = jnp.broadcast_to(owner * slots + rank, (count, 128)).astype(jnp.int32)
        at_slot = rank + base.astype(F32) == lanes
        high = jnp.where(at_slot, (row >> 4).astype(F32), 0.0).astype(BF16)
        low = jnp.where(at_slot, (row & 15).astype(F32), 0.0).astype(BF16)
        turned = hot.T.astype(BF16)
        mine = (iota((1, 128), 1) >= base) & (iota((1, 128), 1) < base + slots)
        over = jnp.max(rank, axis=0, keepdims=True) >= slots // 2
        mark = jnp.where(mine & over, MARK, 0)
        both = dot(turned, jnp.concatenate([high, low], axis=1))
        req_ref[...] = (both[:, :128] * 16.0 + both[:, 128:]).astype(jnp.int32) + mark

    def second_column():
        second = jnp.concatenate([second_ref[...], jnp.zeros((1, 128 - final), jnp.int32)], axis=1)
        return column(second.astype(F32))[:final, :1]

    @pl.when(zero_ref[0] == 1)
    def _():
        for move in moves[:4]:
            move.wait()
        request_rows(lookup(second_column(), first_ref[...]))

    @pl.when(one_ref[0] == 1)
    def _():
        for move in moves[:4]:
            move.wait()
        second = second_column() * 4.0
        request_rows(jnp.concatenate([second + float(f) for f in range(4)], axis=0))

    for move in moves[4:]:
        move.wait()


def halves(table):
    half = table.shape[0] // 2
    return jnp.concatenate([table[:half, :], table[half:, :]], axis=1)


def picked(col, wide):
    half, width = wide.shape[0], wide.shape[1] // 2
    fine = ones_where((col & 127) == iota(col.shape, 1))
    coarse = ((col & (half - 1)) >> 7).astype(F32).astype(BF16)
    hot = [jnp.where(coarse == float(r), fine, jnp.zeros_like(fine)) for r in range(half // 128)]
    both = dot(jnp.concatenate(hot, axis=1), wide)
    return jnp.where(col < half, both[:, :width], both[:, width:]).astype(BF16)


def served_rows(ids_ref, table_ref, out_ref, keep):
    users = ids_ref.shape[0]
    slots = out_ref.shape[0] // users * 16 // keep
    group = 128 // slots
    wide = halves(table_ref[...])
    count = group * keep
    step = 512 // count
    for first in range(0, users // group, step):
        cols = []
        for b in range(first, first + step):
            ids = jnp.sum(ids_ref[b * group:(b + 1) * group, :], axis=0, keepdims=True)
            col = column(ids & (MARK - 1))
            cols += [col[i * slots:i * slots + keep, :] for i in range(group)] if keep < slots else [col]
        out_ref[first * count:(first + step) * count, :] = picked(jnp.concatenate(cols, axis=0), wide)


def serve_kernel(ids_ref, table_ref, out_ref):
    served_rows(ids_ref, table_ref, out_ref, 16)


def serve_zero_kernel(proj_hbm, into_hbm, out_of_hbm, ids_ref, table_ref, dense_ref, head_ref, weight_ref,
                      out_ref, vec_ref, into_ref, out_of_ref, over_ref, proj_ref, sem):
    moves = copies((proj_hbm, into_hbm, out_of_hbm), (proj_ref, into_ref, out_of_ref), sem)
    for move in moves:
        move.start()
    over_ref[0] = jnp.max(ids_ref[...])
    active = jax.nn.relu(dot(dense_ref[...], weight_ref[...]))
    query = (active * head_ref[...]).astype(BF16)
    served_rows(ids_ref, table_ref, out_ref, 8)
    for move in moves:
        move.wait()
    vec_ref[...] = dot(query, proj_ref[...])


def serve_one_kernel(item_hbm, ids_ref, table_ref, out_ref, item_ref, over_ref, sem):
    move = pltpu.make_async_copy(item_hbm, item_ref, sem.at[0])
    move.start()
    over_ref[0] = jnp.max(ids_ref[...])
    served_rows(ids_ref, table_ref, out_ref, 8)
    move.wait()


def nothing_kernel(*refs):
    pass


def copy_kernel(*refs):
    half = len(refs) // 2
    for from_ref, to_ref in zip(refs[:half], refs[half:]):
        to_ref[...] = from_ref[...]


def as_row(col, lanes):
    n = col.shape[0]
    return jnp.sum(jnp.where(iota((n, lanes), 0) == iota((n, lanes), 1), col, 0.0), axis=0, keepdims=True)


def survivors(spot, rows):
    slots = rows.shape[0] // 128
    return picked((spot >> 4) * slots + (spot & 15), halves(rows))


def tower_kernel(spot_ref, rows_ref, vec_ref, into_ref, out_of_ref, packet_ref, score_ref):
    n = packet_ref.shape[0] // 2
    embed = survivors(spot_ref[:n, :], rows_ref[...])
    hidden = jax.nn.relu(dot(embed, into_ref[...])).astype(BF16)
    tower = dot(hidden, out_of_ref[...]).astype(BF16)
    logit = jnp.sum(tower.astype(F32) * vec_ref[...], axis=1, keepdims=True)
    packet_ref[:n, :] = tower
    packet_ref[n:, :] = jnp.broadcast_to(logit, (n, 128)).astype(BF16)
    score_ref[...] = as_row(logit, n)


def features_kernel(feat_hbm, spot_ref, rows_ref, part_ref, feat_ref, sem):
    move = pltpu.make_async_copy(feat_hbm, feat_ref, sem.at[0])
    move.start()
    n = part_ref.shape[0]
    embed = survivors(spot_ref[:4 * n, :], rows_ref[...])
    tall = jnp.concatenate([embed[f * n:(f + 1) * n, :] for f in range(4)], axis=1)
    move.wait()
    part_ref[...] = dot(tall, feat_ref[...])


def gram_kernel(slot_ref, rows_ref, head_ref, weight_ref, part_ref):
    n = part_ref.shape[0] - 8
    cands = slot_ref.shape[1]
    width = rows_ref.shape[1]
    wide = halves(rows_ref[...])
    embed = [
        picked(jnp.concatenate([column(slot_ref[:, b:b + 128]) for b in range(h, h + 512, 128)], axis=0), wide)
        for h in range(0, cands, 512)
    ]
    own_lanes = (iota((32, 128), 0) % 4) == (iota((32, 128), 1) // 32)
    grams = []
    for b in range(cands // 128):
        block = embed[b // 4][b % 4 * 128:b % 4 * 128 + 128, :]
        items = [block[i * 32:i * 32 + 32, :] for i in range(4)]
        four = []
        for i in (0, 2):
            wide_pair = jnp.concatenate([items[i]] * 4 + [items[i + 1]] * 4, axis=0)
            both = dot_nt(block[i * 32:i * 32 + 64, :], wide_pair) * (1.0 / math.sqrt(width))
            four += [jnp.where(own_lanes, both[:32, :128], 0.0), jnp.where(own_lanes, both[32:, 128:], 0.0)]
        grams.append(jnp.concatenate(four, axis=0).astype(BF16))
    i, k = iota((64, 256), 0), iota((64, 256), 1)
    choose = ones_where(((k // 32) == (i % 8)) & (((k % 32) // 4) == (i // 8)))
    flat = []
    for b in range(0, len(grams), 2):
        eight = dot(choose, jnp.concatenate(grams[b:b + 2], axis=0))
        flat.append(jnp.concatenate([eight[q * 8:q * 8 + 8, :] for q in range(8)], axis=1))
    flat = jnp.concatenate(flat, axis=0).astype(BF16)
    part_ref[:n, :] = dot(flat, weight_ref[...])
    part_ref[n:n + 1, :] = head_ref[...]


def prerank_kernel(sec_ref, packet_ref, part_ref, item_ref, weight_ref, head_ref, carry_ref, score_ref):
    @pl.when(sec_ref[0] == 1)
    def _():
        n, hid = part_ref.shape
        pre = part_ref[...] + dot(packet_ref[:n, :], item_ref[...])
        inner = jax.nn.relu(pre).astype(BF16)
        hidden = jax.nn.relu(dot(inner, weight_ref[...]))
        prior = packet_ref[n:, :].astype(F32)[:, :1]
        logit = jnp.sum(hidden * head_ref[...], axis=1, keepdims=True) / math.sqrt(hid) + prior
        carry_ref[:, :hid] = hidden.astype(BF16)
        carry_ref[:, hid:] = jnp.broadcast_to(logit, (n, 128)).astype(BF16)
        score_ref[...] = as_row(logit, n)


def rank(part_ref, carry_ref):
    n, hid = part_ref.shape[0] - 8, part_ref.shape[1]
    carry = carry_ref[...].astype(F32)
    hidden = jax.nn.relu(part_ref[:n, :] + carry[:, :hid])
    logit = jnp.sum(hidden * part_ref[n:n + 1, :], axis=1, keepdims=True) / math.sqrt(hid)
    return hidden, logit + carry[:, hid:hid + 1]


def rank_kernel(sec_ref, near_ref, part_ref, carry_ref, score_ref):
    @pl.when(sec_ref[0] == 2)
    def _():
        n, hid = part_ref.shape[0] - 8, part_ref.shape[1]
        hidden, logit = rank(part_ref, near_ref)
        carry_ref[:, :hid] = hidden.astype(BF16)
        carry_ref[:, hid:] = jnp.broadcast_to(logit, (n, 128)).astype(BF16)
        score_ref[...] = as_row(logit, n)


def final_kernel(sec_ref, last_ref, part_ref, score0_ref, score1_ref, score2_ref, score_ref):
    sec = sec_ref[0]

    for s, from_ref in enumerate((score0_ref, score1_ref, score2_ref)):
        @pl.when(sec == s)
        def _():
            score_ref[...] = from_ref[...]

    @pl.when(sec == 3)
    def _():
        _, logit = rank(part_ref, last_ref)
        score_ref[...] = as_row(logit, logit.shape[0])


def cascade(
    user_dense,
    tables,
    feat_owner,
    feat_row,
    keep_first,
    keep_second,
    section_weight,
    section_head,
    user_proj,
    item_in,
    item_out,
    prerank_feat,
    prerank_item,
):
    shape = pltpu.VMEM
    shards = lax.axis_size("shard")
    cands = feat_row.shape[2]
    slots = 2 * cands // shards
    spots = shards * slots
    width = tables.shape[2]
    hid = section_weight.shape[1]
    final = keep_second.shape[1]
    sec = lax.axis_index("section").reshape(1).astype(jnp.int32)
    user = lax.axis_index("shard").reshape(1).astype(jnp.int32)
    turns = [sec[0] == 0, sec[0] == 1, sec[0] >= 2]
    like = lambda a: shape(a.shape, a.dtype)

    feat, item, into, out_of, proj = in_hbm(prerank_feat, prerank_item, item_in, item_out, user_proj)
    weight = section_weight[0]

    def weight_near():
        return pltpu.with_memory_space_constraint(weight, pltpu.VMEM)


    table = pltpu.with_memory_space_constraint(tables[0], pltpu.VMEM)
    request, slot, spot, head = call(
        request_kernel,
        (shape((shards, 128), jnp.int32), shape((1, cands), jnp.int32), shape((128, 128), jnp.int32),
         like(section_head)),
        user, *(turn.astype(jnp.int32).reshape(1) for turn in turns),
        *in_hbm(feat_owner.reshape(1, cands), feat_row.reshape(1, cands), tables[0], keep_first, keep_second, section_head,
                section_weight[0]),
        smem=4, hbm=7, sems=5, flops=10**8,
        scratch=[pltpu.VMEM(s, jnp.int32) for s in ((1, cands), (1, cands), keep_first.shape, keep_second.shape)],
    )
    asked = lax.all_to_all(request.reshape(shards, 1, 128), "shard", 0, 0, tiled=True).reshape(shards, 128)

    def exchanged(served):
        rows = lax.all_to_all(served.reshape(shards, -1, width), "shard", 0, 0, tiled=True)
        return rows.reshape(-1, width)

    def serve():
        return call(serve_kernel, shape((spots, width), BF16), asked, table, flops=10**9)

    def blank(*shapes):
        return pl.pallas_call(
            nothing_kernel,
            out_shape=shapes,
            in_specs=[pl.BlockSpec(memory_space=pl.ANY)],
            out_specs=(pl.BlockSpec(memory_space=pltpu.VMEM),) * len(shapes),
            compiler_params=pltpu.CompilerParams(vmem_limit_bytes=1 << 20),
        )(asked)

    scored = shape((1, final), F32)
    carried = shape((final, hid + 128), BF16)

    def either(over, served, then):
        return lax.cond(over[0] >= MARK, lambda: then(exchanged(serve())), lambda: then(exchanged(served)))

    def kept(*arrays):
        return tuple(call(copy_kernel, tuple(like(a) for a in arrays), *arrays))

    short = shape((spots // 2, width), BF16)
    scalar = pltpu.SMEM((1,), jnp.int32)
    packed = shape((2 * final, width), BF16)
    product = shape((final, hid), F32)

    def section_zero():
        served, query, into_near, out_of_near, over = call(
            serve_zero_kernel,
            (short, shape((1, width), F32), like(into), like(out_of), scalar),
            proj, into, out_of, asked, table, user_dense, head, weight_near(),
            hbm=3, sems=3, flops=10**9, smem_out=True,
            scratch=[pltpu.VMEM(proj.shape, BF16)],
        )
        return kept(*either(over, served, lambda rows: tuple(call(
            tower_kernel, (packed, scored), spot, rows, query, into_near, out_of_near, flops=10**7))))

    def section_one():
        served, item_near, over = call(
            serve_one_kernel,
            (short, like(item), scalar),
            item, asked, table,
            hbm=1, sems=1, flops=10**9, smem_out=True,
        )
        product_near = either(over, served, lambda rows: call(
            features_kernel, product, feat, spot, rows,
            hbm=1, sems=1, scratch=[pltpu.VMEM(feat.shape, BF16)], flops=10**8))
        return *kept(product_near), item_near

    def dense_sections():
        return call(
            gram_kernel, shape((final + 8, hid), F32), slot, exchanged(serve()), head, weight_near(), flops=10**9)

    def sparse_sections():
        packet, score0 = lax.cond(turns[0], section_zero, lambda: tuple(blank(packed, scored)))
        packet = lax.ppermute(packet, "section", [(0, 1)])
        pre, item_near = lax.cond(turns[1], section_one, lambda: tuple(blank(product, like(item))))
        return *call(
            prerank_kernel,
            (carried, scored),
            sec, packet, pre, item_near, weight_near(), head,
            smem=1, flops=10**8,
        ), score0

    carry, score1, score0 = lax.cond(turns[2], lambda: tuple(blank(carried, scored, scored)), sparse_sections)
    near = lax.ppermute(carry, "section", [(1, 2)])
    part = lax.cond(turns[2], dense_sections, lambda: blank(shape((final + 8, hid), F32))[0])
    carry, score2 = call(rank_kernel, (carried, scored), sec, near, part, smem=1, flops=10**6)
    last = lax.ppermute(carry, "section", [(2, 3)])
    scores = call(
        final_kernel,
        jax.ShapeDtypeStruct((1, final), F32),
        sec, last, part, score0, score1, score2,
        smem=1, flops=10**6,
    )
    return scores[None]


def solution(mesh):
    placed = (
        P("shard", None),
        P("section", "shard", None),
        P("section", "shard", None, None),
        P("section", "shard", None),
        P("shard", None),
        P("shard", None),
        P("section", None, None),
        P("section", None),
        P(),
        P(),
        P(),
        P(),
        P(),
    )
    return jax.shard_map(
        cascade,
        mesh=mesh,
        in_specs=placed,
        out_specs=P("section", "shard", None),
        check_vma=False,
    )
```
